32 devices in a mesh: gz: 32 (over z, y, x, core).
Axes of the slice: x: 2, y: 2, z: 4, core: 2. Of those that a mesh axis runs over, the one named last changes fastest.
Arguments:
- right_side: float32 [64, 512, 512], P('gz'), may hold values from -20 to 20
- cell_flags: int32 [64, 512, 512], P('gz'), may hold values from 0 to 2
Outputs:
- solution: float32 [64, 512, 512], P('gz')
- residual: float32 [64, 512, 512], P('gz')
The draws below stay inside these ranges and needn't reach their ends.
All inputs are finite; a program needn't handle non-finite values.
Results may differ from the reference program's by a relative error of at most 0.00011.
Values sent between devices are 32-bit elements; how exact they have to be, the bound alone decides.
A program may use at most 128 MiB of HBM per device.

```python
import math
import jax
import jax.numpy as jnp

NX = 512
NY = 512
ITERS = 2
NZ = 64


def draw_right_side(key, part):
    noise_key, phase_key = jax.random.split(key)
    depth = jnp.arange(NZ, dtype=jnp.float32) / max(NZ - 1, 1)
    across = (jnp.arange(NX, dtype=jnp.float32) + 0.5) / NX
    along = (jnp.arange(NY, dtype=jnp.float32) + 0.5) / NY
    phases = jax.random.uniform(phase_key, (2,), jnp.float32, 0.0, 2.0 * math.pi)
    base = jnp.clip(jax.random.normal(noise_key, (NZ, NX, NY), jnp.float32), -6.0, 6.0)
    wave = jnp.cos(2.0 * math.pi * across + phases[0])[:, None] * jnp.cos(2.0 * math.pi * along + phases[1])[None, :]
    upper_weight = 3.0 * depth * depth
    return base + upper_weight[:, None, None] * wave[None, :, :]


def draw_cell_flags(key, part):
    keys = jax.random.split(key, 9)
    block_z = max(NZ // 16, 2)
    block_x = max(NX // 8, 4)
    block_y = max(NY // 8, 4)
    count_z = (NZ + block_z - 1) // block_z
    count_x = (NX + block_x - 1) // block_x
    count_y = (NY + block_y - 1) // block_y
    blocks = (count_z, count_x, count_y)
    level = jnp.arange(count_z, dtype=jnp.int32)[:, None, None]
    present = jax.random.randint(keys[0], blocks, 0, count_z) >= level

    def extent(length_key, start_key, width):
        shortest = max(width // 3, 1)
        longest = max(2 * width // 3, shortest)
        length = jax.random.randint(length_key, blocks, shortest, longest + 1)
        start = jax.random.randint(start_key, blocks, 0, width - length + 1)
        return (start, length)
    start_z, length_z = extent(keys[1], keys[2], block_z)
    start_x, length_x = extent(keys[3], keys[4], block_x)
    start_y, length_y = extent(keys[5], keys[6], block_y)
    zcells = jnp.arange(NZ, dtype=jnp.int32)
    xcells = jnp.arange(NX, dtype=jnp.int32)
    ycells = jnp.arange(NY, dtype=jnp.int32)
    z_index = (zcells // block_z)[:, None, None]
    x_index = (xcells // block_x)[None, :, None]
    y_index = (ycells // block_y)[None, None, :]
    z_offset = (zcells % block_z)[:, None, None]
    x_offset = (xcells % block_x)[None, :, None]
    y_offset = (ycells % block_y)[None, None, :]

    def inside(start, length, offset):
        first = start[z_index, x_index, y_index]
        return (offset >= first) & (offset < first + length[z_index, x_index, y_index])
    solid = present[z_index, x_index, y_index] & inside(start_z, length_z, z_offset) & inside(start_x, length_x, x_offset) & inside(start_y, length_y, y_offset)
    scattered = jax.random.randint(keys[8], (NZ, NX, NY), 0, 8) == 0
    solid = solid | scattered
    edge_draw = jax.random.randint(keys[7], (NZ, 2, NY), 0, 4) == 0
    open_edge = jnp.pad(edge_draw, ((0, 0), (0, NX - 2), (0, 0)))
    open_side = (ycells >= NY - 2)[None, None, :]
    empty = open_edge | open_side
    return jnp.where(solid, 2, jnp.where(empty, 0, 1)).astype(jnp.int32)


def setup_inputs(seed: int = 0) -> dict:
    key_of = jax.random.split(jax.random.key(seed), 3)
    right_side = draw_right_side(jax.random.fold_in(key_of[2], 71), 0)
    cell_flags = draw_cell_flags(jax.random.fold_in(key_of[2], 71), 0)
    return dict(right_side=right_side, cell_flags=cell_flags)


def neighbour_total(field):
    padded = jnp.pad(field, 1)
    total = padded[2:, 1:-1, 1:-1] + padded[:-2, 1:-1, 1:-1]
    total = total + padded[1:-1, 2:, 1:-1] + padded[1:-1, :-2, 1:-1]
    total = total + padded[1:-1, 1:-1, 2:] + padded[1:-1, 1:-1, :-2]
    return total


def reference(right_side, cell_flags):
    fluid_mask = (cell_flags == 1).astype(jnp.float32)
    solid = (cell_flags == 2).astype(jnp.float32)
    diagonal = jnp.maximum(6.0 - neighbour_total(solid), 1.0)

    def operate(field):
        return fluid_mask * (diagonal * field - neighbour_total(field))

    solution = jnp.zeros_like(right_side)
    residual = fluid_mask * right_side
    precond = residual / diagonal
    direction = precond
    rz_now = jnp.sum(residual * precond)
    for iteration in range(ITERS):
        image = operate(direction)
        step_size = rz_now / jnp.sum(direction * image)
        solution = solution + step_size * direction
        residual = residual - step_size * image
        if iteration + 1 < ITERS:
            precond = residual / diagonal
            rz_new = jnp.sum(residual * precond)
            direction = precond + (rz_new / rz_now) * direction
            rz_now = rz_new
    return solution, residual
```

```python
import functools
import math

import jax
import jax.numpy as jnp
from jax import lax
from jax.experimental import pallas as pl
from jax.experimental.pallas import tpu as pltpu
from jax.sharding import PartitionSpec as P

MESH = pl.DeviceIdType.MESH
TILE = 16
PAD = 8
VMEM_BYTES = 67_043_328


def kernel(
    count, chunk, stages,
    side_hbm, flag_hbm, sol_ref, res_ref,
    rhs, flags, r0, inv, solid, u0, u1, w0, w1, halo_r, halo_u, bits_out, bits_in,
    pair, totals, mine, got,
    in_sem, bit_send, bit_recv, halo_send, halo_recv,
    pair_send, pair_recv, total_send, total_recv, sum_send, sum_recv,
):
    depth, rows, cols = rhs.shape
    words = rows // 32
    chunks = rows // chunk
    tiles = chunk // TILE
    me = lax.axis_index("gz")
    chip, odd = me // 2, lax.rem(me, 2)
    near_side, far_side = 1 - odd, odd
    partner = me + 1 - 2 * odd

    def load(plane, which):
        source, target = ((flag_hbm, flags), (side_hbm, rhs))[which]
        return pltpu.make_async_copy(source.at[plane], target.at[plane], in_sem.at[which, plane])

    def present(side):
        return jnp.where(side == 0, me > 0, me < count - 1)

    def neighbour(side):
        return me - 1 + 2 * side

    def peer(stage, j):
        size, stride = stages[stage]
        digit = lax.rem(chip // stride, size)
        return digit, (chip + (lax.rem(digit + j, size) - digit) * stride) * 2 + 1

    barrier = pltpu.get_barrier_semaphore()

    def greet(other):
        pl.semaphore_signal(barrier, inc=1, device_id=(other,), device_id_type=MESH)

    for side in range(2):
        @pl.when(present(side))
        def _():
            greet(neighbour(side))

    @pl.when(odd == 1)
    def _():
        for stage, (size, _) in enumerate(stages):
            for j in range(1, size):
                greet(peer(stage, j)[1])

    for plane in range(depth):
        for which in range(2):
            load(plane, which).start()

    blank = jnp.zeros((PAD, cols), jnp.float32)
    for ref in (u0, u1, solid):
        for plane in range(ref.shape[0]):
            ref[plane, 0:PAD, :] = blank
            ref[plane, rows + PAD:rows + 2 * PAD, :] = blank
    for side in range(2):
        @pl.when(jnp.logical_not(present(side)))
        def _():
            bits_in[side] = jnp.zeros((2, words, cols), jnp.int32)

            def clear(t, carry):
                at = pl.ds(pl.multiple_of(t * TILE, TILE), TILE)
                halo_r[side, at, :] = jnp.zeros((TILE, cols), jnp.float32)
                halo_u[side, at, :] = jnp.zeros((TILE, cols), jnp.float32)
                return carry

            lax.fori_loop(0, rows // TILE, clear, 0)

    def halo_copy(phase, side, k):
        at = pl.multiple_of(k * chunk, chunk)
        plane = side * (depth - 1)
        if phase == 0:
            source, target = r0.at[plane, pl.ds(at, chunk)], halo_r
        else:
            source, target = u1.at[plane, pl.ds(pl.multiple_of(at + PAD, PAD), chunk)], halo_u
        return pltpu.make_async_remote_copy(
            src_ref=source,
            dst_ref=target.at[1 - side, pl.ds(at, chunk)],
            send_sem=halo_send.at[phase, side, k],
            recv_sem=halo_recv.at[phase, 1 - side, k],
            device_id=(neighbour(side),),
            device_id_type=MESH,
        )

    def halo_arrival(phase, side, k):
        at = pl.multiple_of(k * chunk, chunk)
        target = halo_r if phase == 0 else halo_u
        return pltpu.make_async_remote_copy(
            src_ref=target.at[side, pl.ds(at, chunk)],
            dst_ref=target.at[side, pl.ds(at, chunk)],
            send_sem=halo_send.at[phase, side, k],
            recv_sem=halo_recv.at[phase, side, k],
            device_id=(neighbour(side),),
            device_id_type=MESH,
        )

    def send_halo(phase, side, k):
        @pl.when(present(side))
        def _():
            halo_copy(phase, side, k).start()

    def send_plane(phase, side):
        def one(k, carry):
            send_halo(phase, side, k)
            return carry

        lax.fori_loop(0, chunks, one, 0)

    def wait_halo(phase, side, k):
        @pl.when(present(side))
        def _():
            halo_arrival(phase, side, k).wait_recv()

    def row(k, t):
        return pl.multiple_of(k * chunk + t * TILE, TILE)

    outer = sorted({0, 1, depth - 2, depth - 1})
    steps = rows // TILE
    for plane in range(depth):
        load(plane, 0).wait()
        load(plane, 1).wait()

        def mask_tile(t, carry, plane=plane):
            at = pl.ds(pl.multiple_of(t * TILE, TILE), TILE)
            r0[plane, at, :] = jnp.where(flags[plane, at, :] == 1, rhs[plane, at, :], 0.0)
            return carry

        lax.fori_loop(0, steps, mask_tile, 0)

        def pack(j, word, plane=plane):
            at = pl.ds(pl.multiple_of(j * words, words), words)
            is_solid = flags[plane, at, :] == 2
            padded = pl.ds(pl.multiple_of(j * words + PAD, PAD), words)
            solid[plane + 2, padded, :] = jnp.where(is_solid, 1.0, 0.0)
            return word | jnp.left_shift(jnp.where(is_solid, 1, 0), j)

        word = lax.fori_loop(0, 32, pack, jnp.zeros((words, cols), jnp.int32))
        if plane in outer:
            bits_out[outer.index(plane)] = word

    def bit_copy(side):
        lead = 0 if side == 0 else len(outer) - 2
        return pltpu.make_async_remote_copy(
            src_ref=bits_out.at[pl.ds(lead, 2)],
            dst_ref=bits_in.at[1 - side],
            send_sem=bit_send.at[side],
            recv_sem=bit_recv.at[1 - side],
            device_id=(neighbour(side),),
            device_id_type=MESH,
        )

    greeted = sum(size - 1 for size, _ in stages)
    callers = present(0).astype(jnp.int32) + present(1).astype(jnp.int32) + odd * greeted
    pl.semaphore_wait(barrier, callers)

    for side in range(2):
        @pl.when(present(side))
        def _():
            bit_copy(side).start()
    send_plane(0, far_side)
    send_plane(0, near_side)

    for side in range(2):
        @pl.when(present(side))
        def _():
            bit_copy(1 - side).wait_recv()
        for i in range(2):
            def unpack(j, carry, side=side, i=i):
                padded = pl.ds(pl.multiple_of(j * words + PAD, PAD), words)
                bit = jnp.bitwise_and(jnp.right_shift(bits_in[side, i], j), 1)
                solid[side * (depth + 2) + i, padded, :] = bit.astype(jnp.float32)
                return carry

            lax.fori_loop(0, 32, unpack, 0)

    column = lax.broadcasted_iota(jnp.int32, (TILE, cols), 1)

    def inplane(ref, plane, start):
        block = ref[plane, pl.ds(start, TILE + 2 * PAD), :]
        centre = block[PAD:PAD + TILE]
        total = block[PAD - 1:PAD - 1 + TILE] + block[PAD + 1:PAD + 1 + TILE]
        total = total + jnp.where(column == 0, 0.0, pltpu.roll(centre, 1, 1))
        total = total + jnp.where(column == cols - 1, 0.0, pltpu.roll(centre, cols - 1, 1))
        return centre, total

    def centre_of(ref, plane, start):
        return ref[plane, pl.ds(pl.multiple_of(start + PAD, PAD), TILE), :]

    def put(ref, plane, start, value):
        ref[plane, pl.ds(pl.multiple_of(start + PAD, PAD), TILE), :] = value

    def fold(value):
        total = value[0:8]
        for i in range(8, TILE, 8):
            total = total + value[i:i + 8]
        return total

    none = jnp.zeros((8, cols), jnp.float32)

    def inverse(plane, start):
        _, total = inplane(solid, plane + 1, start)
        total = total + centre_of(solid, plane, start) + centre_of(solid, plane + 2, start)
        return 1.0 / jnp.maximum(6.0 - total, 1.0)

    def first(t, moment):
        start = pl.multiple_of(t * TILE, TILE)
        at = pl.ds(start, TILE)
        for plane in range(depth):
            value = jnp.where(flags[plane, at, :] == 1, inverse(plane + 1, start), 0.0)
            inv[plane + 1, at, :] = value
            residual = r0[plane, at, :]
            precond = residual * value
            put(u0, plane, start, precond)
            moment = moment + fold(residual * precond)
        for plane in (0, depth + 1):
            inv[plane, at, :] = inverse(plane, start)
        return moment

    moment0 = lax.fori_loop(0, steps, first, none)

    def local_part(field, scaled, out, plane, start):
        at = pl.ds(start, TILE)
        _, total = inplane(field, plane, start)
        if plane > 0:
            total = total + centre_of(field, plane - 1, start)
        if plane < depth - 1:
            total = total + centre_of(field, plane + 1, start)
        image = jnp.where(inv[plane + 1, at, :] > 0.0, scaled[plane, at, :] - total, 0.0)
        out[plane, at, :] = image
        return image

    def apply_once(plane, start, image, value, moments):
        precond = image * value
        put(u1, plane, start, precond)
        return (
            moments[0] + fold(image * centre_of(u0, plane, start)),
            moments[1] + fold(image * precond),
        )

    def second(t, moments):
        start = pl.multiple_of(t * TILE, TILE)
        for plane in range(depth):
            image = local_part(u0, r0, w0, plane, start)
            if 0 < plane < depth - 1:
                value = inv[plane + 1, pl.ds(start, TILE), :]
                moments = apply_once(plane, start, image, value, moments)
        return moments

    moments = lax.fori_loop(0, steps, second, (none, none))

    def edge_one(side, moments, forward):
        plane = side * (depth - 1)

        def step(k, moments):
            wait_halo(0, side, k)

            def tile(t, moments):
                start = row(k, t)
                at = pl.ds(start, TILE)
                value = inv[plane + 1, at, :]
                beyond = halo_r[side, at, :] * inv[side * (depth + 1), at, :]
                image = jnp.where(value > 0.0, w0[plane, at, :] - beyond, 0.0)
                w0[plane, at, :] = image
                return apply_once(plane, start, image, value, moments)

            moments = lax.fori_loop(0, tiles, tile, moments)

            @pl.when(forward)
            def _():
                send_halo(1, side, k)

            return moments

        return lax.fori_loop(0, chunks, step, moments)

    moments = edge_one(near_side, moments, odd >= 0)
    moment1, moment2 = edge_one(far_side, moments, odd == 1)

    def third(t, moment):
        start = pl.multiple_of(t * TILE, TILE)
        for plane in range(depth):
            image = local_part(u1, w0, w1, plane, start)
            moment = moment + fold(image * centre_of(u1, plane, start))
        return moment

    moment3 = lax.fori_loop(0, steps, third, none)

    def edge_two(side, moment, weight, after):
        plane = side * (depth - 1)

        def step(k, moment):
            wait_halo(1, side, k)
            after(k)

            def tile(t, moment):
                start = row(k, t)
                at = pl.ds(start, TILE)
                beyond = halo_u[side, at, :]
                image = jnp.where(inv[plane + 1, at, :] > 0.0, w1[plane, at, :] - beyond, 0.0)
                w1[plane, at, :] = image
                return moment - weight * fold(beyond * centre_of(u1, plane, start))

            return lax.fori_loop(0, tiles, tile, moment)

        return lax.fori_loop(0, chunks, step, moment)

    def lanes(value):
        total = value[:, 0:128]
        for i in range(128, cols, 128):
            total = total + value[:, i:i + 128]
        return jnp.sum(total, axis=0, keepdims=True)

    def settle(moment):
        pair[0, 0:1, :] = lanes(moment0)
        pair[0, 1:2, :] = lanes(moment1)
        pair[0, 2:3, :] = lanes(moment2)
        pair[0, 3:4, :] = lanes(moment)
        pair[0, 4:8, :] = jnp.zeros((4, 128), jnp.float32)

    moment3 = edge_two(near_side, moment3, 1.0, lambda k: None)

    def pair_copy():
        return pltpu.make_async_remote_copy(
            src_ref=pair.at[0], dst_ref=pair.at[1], send_sem=pair_send, recv_sem=pair_recv,
            device_id=(partner,), device_id_type=MESH,
        )

    def total_copy():
        return pltpu.make_async_remote_copy(
            src_ref=totals, dst_ref=totals, send_sem=total_send, recv_sem=total_recv,
            device_id=(partner,), device_id_type=MESH,
        )

    def sum_copy(stage, j):
        digit, other = peer(stage, j)
        return pltpu.make_async_remote_copy(
            src_ref=mine.at[stage],
            dst_ref=got.at[stage, digit],
            send_sem=sum_send.at[stage, j],
            recv_sem=sum_recv.at[stage, digit],
            device_id=(other,),
            device_id_type=MESH,
        )

    def sum_arrival(stage, j):
        digit, other = peer(stage, j)
        slot = lax.rem(digit + j, stages[stage][0])
        return pltpu.make_async_remote_copy(
            src_ref=got.at[stage, slot],
            dst_ref=got.at[stage, slot],
            send_sem=sum_send.at[stage, j],
            recv_sem=sum_recv.at[stage, slot],
            device_id=(other,),
            device_id_type=MESH,
        )

    @pl.when(odd == 0)
    def _():
        def send_late(k):
            @pl.when(k == max(chunks - 2, 0))
            def _():
                send_plane(1, 0)

        settle(edge_two(0, moment3, 2.0, send_late))
        pair_copy().start()
        total_copy().wait_recv()

    @pl.when(odd == 1)
    def _():
        settle(moment3)
        pair_copy().wait_recv()
        total = pair[0] + pair[1]
        for stage, (size, _) in enumerate(stages):
            mine[stage] = total
            for j in range(1, size):
                sum_copy(stage, j).start()
            got[stage, peer(stage, 0)[0]] = total
            for j in range(1, size):
                sum_arrival(stage, j).wait_recv()
            total = got[stage, 0]
            for i in range(1, size):
                total = total + got[stage, i]
        totals[...] = total
        total_copy().start()

    everyone = totals[...]
    s0, s1, s2, s3 = (everyone[i:i + 1] for i in range(4))

    def whole(value):
        return jnp.sum(value, axis=1, keepdims=True)

    rz_old = whole(s0)
    step_old = rz_old / whole(s1)
    rz_now = whole(s0 - 2.0 * step_old * s1 + step_old * step_old * s2)
    grown = 1.0 + rz_now / rz_old
    product = whole(grown * grown * s1 - 2.0 * step_old * grown * s2 + step_old * step_old * s3)
    step_size = rz_now / product
    lead = step_old + step_size * grown
    trail = step_size * step_old

    for plane in range(depth):
        def last(t, carry, plane=plane):
            start = pl.multiple_of(t * TILE, TILE)
            at = pl.ds(start, TILE)
            base = r0[plane, at, :]
            along = w0[plane, at, :]
            sol_ref[plane, at, :] = inv[plane + 1, at, :] * (lead * base - trail * along)
            res_ref[plane, at, :] = base - lead * along + trail * w1[plane, at, :]
            return carry

        lax.fori_loop(0, steps, last, 0)

    @pl.when(jnp.logical_and(odd == 1, present(1)))
    def _():
        plane = depth - 1

        def late(k, carry):
            halo_arrival(1, 1, k).wait_recv()

            def tile(t, carry):
                at = pl.ds(row(k, t), TILE)
                beyond = jnp.where(inv[plane + 1, at, :] > 0.0, halo_u[1, at, :], 0.0)
                res_ref[plane, at, :] = res_ref[plane, at, :] - trail * beyond
                return carry

            return lax.fori_loop(0, tiles, tile, carry)

        lax.fori_loop(0, chunks, late, 0)

    for side in range(2):
        @pl.when(present(side))
        def _():
            bit_copy(side).wait_send()
            for phase in range(2):
                for k in range(chunks):
                    halo_copy(phase, side, k).wait_send()

    @pl.when(odd == 0)
    def _():
        pair_copy().wait_send()

    @pl.when(odd == 1)
    def _():
        total_copy().wait_send()
        for stage, (size, _) in enumerate(stages):
            for j in range(1, size):
                sum_copy(stage, j).wait_send()


def groups(chips):
    size = math.gcd(chips, 4)
    stages, stride = [(size, 1)], size
    while stride < chips:
        rest = chips // stride
        size = 2 if rest % 2 == 0 else rest
        stages.append((size, stride))
        stride *= size
    return stages


def body(count, right_side, cell_flags):
    depth, rows, cols = right_side.shape
    stages = groups(count // 2)
    widest = max(size for size, _ in stages)
    chunk = math.gcd(rows, 64)
    chunks = rows // chunk
    f32 = jnp.float32
    field = pltpu.VMEM((depth, rows, cols), f32)
    padded = pltpu.VMEM((depth, rows + 2 * PAD, cols), f32)
    outer = len({0, 1, depth - 2, depth - 1})
    dma = pltpu.SemaphoreType.DMA
    grant = VMEM_BYTES - 8 * right_side.size - 2**19
    return pl.pallas_call(
        functools.partial(kernel, count, chunk, stages),
        out_shape=(field, field),
        in_specs=[pl.BlockSpec(memory_space=pltpu.HBM)] * 2,
        out_specs=(pl.BlockSpec(memory_space=pltpu.VMEM),) * 2,
        scratch_shapes=[
            field,
            pltpu.VMEM((depth, rows, cols), jnp.int32),
            field,
            pltpu.VMEM((depth + 2, rows, cols), f32),
            pltpu.VMEM((depth + 4, rows + 2 * PAD, cols), f32),
            padded, padded, field, field,
            pltpu.VMEM((2, rows, cols), f32),
            pltpu.VMEM((2, rows, cols), f32),
            pltpu.VMEM((outer, rows // 32, cols), jnp.int32),
            pltpu.VMEM((2, 2, rows // 32, cols), jnp.int32),
            pltpu.VMEM((2, 8, 128), f32),
            pltpu.VMEM((8, 128), f32),
            pltpu.VMEM((len(stages), 8, 128), f32),
            pltpu.VMEM((len(stages), widest, 8, 128), f32),
            dma((2, depth)),
            dma((2,)), dma((2,)),
            dma((2, 2, chunks)), dma((2, 2, chunks)),
            dma, dma, dma, dma,
            dma((len(stages), widest)), dma((len(stages), widest)),
        ],
        compiler_params=pltpu.CompilerParams(
            collective_id=0, has_side_effects=True, vmem_limit_bytes=grant
        ),
    )(right_side, cell_flags)


def solution(mesh):
    placed = (P("gz", None, None), P("gz", None, None))
    return jax.shard_map(
        functools.partial(body, mesh.shape["gz"]),
        mesh=mesh,
        in_specs=placed,
        out_specs=placed,
        check_vma=False,
    )
```

```python
import functools
import math

import jax
import jax.numpy as jnp
from jax import lax
from jax.experimental import pallas as pl
from jax.experimental.pallas import tpu as pltpu
from jax.sharding import PartitionSpec as P

MESH = pl.DeviceIdType.MESH
TILE = 16
PAD = 8
VMEM_BYTES = 67_043_328


def kernel(
    count, chunk, stages,
    side_hbm, flag_hbm, sol_ref, res_ref,
    rhs, flags, r0, inv, solid, u0, u1, w0, w1, halo_r, halo_u, bits_out, bits_in,
    pair, totals, mine, got,
    in_sem, bit_send, bit_recv, halo_send, halo_recv,
    pair_send, pair_recv, total_send, total_recv, sum_send, sum_recv,
):
    depth, rows, cols = rhs.shape
    words = rows // 32
    chunks = rows // chunk
    tiles = chunk // TILE
    me = lax.axis_index("gz")
    chip, odd = me // 2, lax.rem(me, 2)
    near_side, far_side = 1 - odd, odd
    partner = me + 1 - 2 * odd

    def load(plane, which):
        source, target = ((flag_hbm, flags), (side_hbm, rhs))[which]
        return pltpu.make_async_copy(source.at[plane], target.at[plane], in_sem.at[which, plane])

    def present(side):
        return jnp.where(side == 0, me > 0, me < count - 1)

    def neighbour(side):
        return me - 1 + 2 * side

    def peer(stage, j):
        size, stride = stages[stage]
        digit = lax.rem(chip // stride, size)
        return digit, (chip + (lax.rem(digit + j, size) - digit) * stride) * 2 + 1

    barrier = pltpu.get_barrier_semaphore()

    def greet(other):
        pl.semaphore_signal(barrier, inc=1, device_id=(other,), device_id_type=MESH)

    for side in range(2):
        @pl.when(present(side))
        def _():
            greet(neighbour(side))

    @pl.when(odd == 1)
    def _():
        for stage, (size, _) in enumerate(stages):
            for j in range(1, size):
                greet(peer(stage, j)[1])

    for plane in range(depth):
        for which in range(2):
            load(plane, which).start()

    blank = jnp.zeros((PAD, cols), jnp.float32)
    for ref in (u0, u1, solid):
        for plane in range(ref.shape[0]):
            ref[plane, 0:PAD, :] = blank
            ref[plane, rows + PAD:rows + 2 * PAD, :] = blank
    for side in range(2):
        @pl.when(jnp.logical_not(present(side)))
        def _():
            bits_in[side] = jnp.zeros((2, words, cols), jnp.int32)

            def clear(t, carry):
                at = pl.ds(pl.multiple_of(t * TILE, TILE), TILE)
                halo_r[side, at, :] = jnp.zeros((TILE, cols), jnp.float32)
                halo_u[side, at, :] = jnp.zeros((TILE, cols), jnp.float32)
                return carry

            lax.fori_loop(0, rows // TILE, clear, 0)

    def halo_copy(phase, side, k):
        at = pl.multiple_of(k * chunk, chunk)
        plane = side * (depth - 1)
        if phase == 0:
            source, target = r0.at[plane, pl.ds(at, chunk)], halo_r
        else:
            source, target = u1.at[plane, pl.ds(pl.multiple_of(at + PAD, PAD), chunk)], halo_u
        return pltpu.make_async_remote_copy(
            src_ref=source,
            dst_ref=target.at[1 - side, pl.ds(at, chunk)],
            send_sem=halo_send.at[phase, side, k],
            recv_sem=halo_recv.at[phase, 1 - side, k],
            device_id=(neighbour(side),),
            device_id_type=MESH,
        )

    def halo_arrival(phase, side, k):
        at = pl.multiple_of(k * chunk, chunk)
        target = halo_r if phase == 0 else halo_u
        return pltpu.make_async_remote_copy(
            src_ref=target.at[side, pl.ds(at, chunk)],
            dst_ref=target.at[side, pl.ds(at, chunk)],
            send_sem=halo_send.at[phase, side, k],
            recv_sem=halo_recv.at[phase, side, k],
            device_id=(neighbour(side),),
            device_id_type=MESH,
        )

    def send_halo(phase, side, k):
        @pl.when(present(side))
        def _():
            halo_copy(phase, side, k).start()

    def send_plane(phase, side):
        def one(k, carry):
            send_halo(phase, side, k)
            return carry

        lax.fori_loop(0, chunks, one, 0)

    def wait_halo(phase, side, k):
        @pl.when(present(side))
        def _():
            halo_arrival(phase, side, k).wait_recv()

    def row(k, t):
        return pl.multiple_of(k * chunk + t * TILE, TILE)

    outer = sorted({0, 1, depth - 2, depth - 1})
    steps = rows // TILE
    for plane in range(depth):
        load(plane, 0).wait()
        load(plane, 1).wait()

        def mask_tile(t, carry, plane=plane):
            at = pl.ds(pl.multiple_of(t * TILE, TILE), TILE)
            r0[plane, at, :] = jnp.where(flags[plane, at, :] == 1, rhs[plane, at, :], 0.0)
            return carry

        lax.fori_loop(0, steps, mask_tile, 0)

        def pack(j, word, plane=plane):
            at = pl.ds(pl.multiple_of(j * words, words), words)
            is_solid = flags[plane, at, :] == 2
            padded = pl.ds(pl.multiple_of(j * words + PAD, PAD), words)
            solid[plane + 2, padded, :] = jnp.where(is_solid, 1.0, 0.0)
            return word | jnp.left_shift(jnp.where(is_solid, 1, 0), j)

        word = lax.fori_loop(0, 32, pack, jnp.zeros((words, cols), jnp.int32))
        if plane in outer:
            bits_out[outer.index(plane)] = word

    def bit_copy(side):
        lead = 0 if side == 0 else len(outer) - 2
        return pltpu.make_async_remote_copy(
            src_ref=bits_out.at[pl.ds(lead, 2)],
            dst_ref=bits_in.at[1 - side],
            send_sem=bit_send.at[side],
            recv_sem=bit_recv.at[1 - side],
            device_id=(neighbour(side),),
            device_id_type=MESH,
        )

    greeted = sum(size - 1 for size, _ in stages)
    callers = present(0).astype(jnp.int32) + present(1).astype(jnp.int32) + odd * greeted
    pl.semaphore_wait(barrier, callers)

    for side in range(2):
        @pl.when(present(side))
        def _():
            bit_copy(side).start()
    @pl.when(odd == 0)
    def _():
        send_plane(0, 0)

    send_plane(0, near_side)

    for side in range(2):
        @pl.when(present(side))
        def _():
            bit_copy(1 - side).wait_recv()
        for i in range(2):
            def unpack(j, carry, side=side, i=i):
                padded = pl.ds(pl.multiple_of(j * words + PAD, PAD), words)
                bit = jnp.bitwise_and(jnp.right_shift(bits_in[side, i], j), 1)
                solid[side * (depth + 2) + i, padded, :] = bit.astype(jnp.float32)
                return carry

            lax.fori_loop(0, 32, unpack, 0)

    column = lax.broadcasted_iota(jnp.int32, (TILE, cols), 1)

    def inplane(ref, plane, start):
        block = ref[plane, pl.ds(start, TILE + 2 * PAD), :]
        centre = block[PAD:PAD + TILE]
        total = block[PAD - 1:PAD - 1 + TILE] + block[PAD + 1:PAD + 1 + TILE]
        total = total + jnp.where(column == 0, 0.0, pltpu.roll(centre, 1, 1))
        total = total + jnp.where(column == cols - 1, 0.0, pltpu.roll(centre, cols - 1, 1))
        return centre, total

    def centre_of(ref, plane, start):
        return ref[plane, pl.ds(pl.multiple_of(start + PAD, PAD), TILE), :]

    def put(ref, plane, start, value):
        ref[plane, pl.ds(pl.multiple_of(start + PAD, PAD), TILE), :] = value

    def fold(value):
        total = value[0:8]
        for i in range(8, TILE, 8):
            total = total + value[i:i + 8]
        return total

    none = jnp.zeros((8, cols), jnp.float32)

    def inverse(plane, start):
        _, total = inplane(solid, plane + 1, start)
        total = total + centre_of(solid, plane, start) + centre_of(solid, plane + 2, start)
        return 1.0 / jnp.maximum(6.0 - total, 1.0)

    def first(t, moment):
        start = pl.multiple_of(t * TILE, TILE)
        at = pl.ds(start, TILE)
        for plane in range(depth):
            value = jnp.where(flags[plane, at, :] == 1, inverse(plane + 1, start), 0.0)
            inv[plane + 1, at, :] = value
            residual = r0[plane, at, :]
            precond = residual * value
            put(u0, plane, start, precond)
            moment = moment + fold(residual * precond)
        for plane in (0, depth + 1):
            inv[plane, at, :] = inverse(plane, start)
        return moment

    moment0 = lax.fori_loop(0, steps, first, none)

    def local_part(field, scaled, out, plane, start):
        at = pl.ds(start, TILE)
        _, total = inplane(field, plane, start)
        if plane > 0:
            total = total + centre_of(field, plane - 1, start)
        if plane < depth - 1:
            total = total + centre_of(field, plane + 1, start)
        image = jnp.where(inv[plane + 1, at, :] > 0.0, scaled[plane, at, :] - total, 0.0)
        out[plane, at, :] = image
        return image

    def apply_once(plane, start, image, value, moments):
        precond = image * value
        put(u1, plane, start, precond)
        return (
            moments[0] + fold(image * centre_of(u0, plane, start)),
            moments[1] + fold(image * precond),
        )

    def second(t, moments):
        start = pl.multiple_of(t * TILE, TILE)
        for plane in range(depth):
            image = local_part(u0, r0, w0, plane, start)
            if 0 < plane < depth - 1:
                value = inv[plane + 1, pl.ds(start, TILE), :]
                moments = apply_once(plane, start, image, value, moments)
        return moments

    moments = lax.fori_loop(0, steps, second, (none, none))

    @pl.when(odd == 1)
    def _():
        send_plane(0, 1)

    def edge_one(side, moments, forward):
        plane = side * (depth - 1)

        def step(k, moments):
            wait_halo(0, side, k)

            def tile(t, moments):
                start = row(k, t)
                at = pl.ds(start, TILE)
                value = inv[plane + 1, at, :]
                beyond = halo_r[side, at, :] * inv[side * (depth + 1), at, :]
                image = jnp.where(value > 0.0, w0[plane, at, :] - beyond, 0.0)
                w0[plane, at, :] = image
                return apply_once(plane, start, image, value, moments)

            moments = lax.fori_loop(0, tiles, tile, moments)

            @pl.when(forward)
            def _():
                send_halo(1, side, k)

            return moments

        return lax.fori_loop(0, chunks, step, moments)

    moments = edge_one(near_side, moments, odd >= 0)
    moment1, moment2 = edge_one(far_side, moments, odd == 1)

    def third(t, moment):
        start = pl.multiple_of(t * TILE, TILE)
        for plane in range(depth):
            image = local_part(u1, w0, w1, plane, start)
            moment = moment + fold(image * centre_of(u1, plane, start))
        return moment

    moment3 = lax.fori_loop(0, steps, third, none)

    def edge_two(side, moment, weight, after):
        plane = side * (depth - 1)

        def step(k, moment):
            wait_halo(1, side, k)
            after(k)

            def tile(t, moment):
                start = row(k, t)
                at = pl.ds(start, TILE)
                beyond = halo_u[side, at, :]
                image = jnp.where(inv[plane + 1, at, :] > 0.0, w1[plane, at, :] - beyond, 0.0)
                w1[plane, at, :] = image
                return moment - weight * fold(beyond * centre_of(u1, plane, start))

            return lax.fori_loop(0, tiles, tile, moment)

        return lax.fori_loop(0, chunks, step, moment)

    def lanes(value):
        total = value[:, 0:128]
        for i in range(128, cols, 128):
            total = total + value[:, i:i + 128]
        return jnp.sum(total, axis=0, keepdims=True)

    def settle(moment):
        for i, value in enumerate((moment0, moment1, moment2, moment)):
            mine[0, i:i + 1, :] = lanes(value)
        mine[0, 4:8, :] = jnp.zeros((4, 128), jnp.float32)

    moment3 = edge_two(near_side, moment3, 1.0, lambda k: None)

    def pair_copy():
        return pltpu.make_async_remote_copy(
            src_ref=mine.at[0], dst_ref=pair, send_sem=pair_send, recv_sem=pair_recv,
            device_id=(partner,), device_id_type=MESH,
        )

    def total_copy():
        return pltpu.make_async_remote_copy(
            src_ref=totals, dst_ref=totals, send_sem=total_send, recv_sem=total_recv,
            device_id=(partner,), device_id_type=MESH,
        )

    def sum_copy(stage, j):
        digit, other = peer(stage, j)
        return pltpu.make_async_remote_copy(
            src_ref=mine.at[stage],
            dst_ref=got.at[stage, digit],
            send_sem=sum_send.at[stage, j],
            recv_sem=sum_recv.at[stage, digit],
            device_id=(other,),
            device_id_type=MESH,
        )

    def sum_arrival(stage, slot):
        return pltpu.make_async_remote_copy(
            src_ref=got.at[stage, slot],
            dst_ref=got.at[stage, slot],
            send_sem=sum_send.at[stage, 0],
            recv_sem=sum_recv.at[stage, slot],
            device_id=(partner,),
            device_id_type=MESH,
        )

    near_size = stages[0][0]
    ahead = min(2, chunks)

    @pl.when(odd == 0)
    def _():
        def early(k):
            @pl.when(k == max(chunks - 3, 0))
            def _():
                for i in range(ahead):
                    send_halo(1, 0, i)

        settle(edge_two(0, moment3, 2.0, early))
        pair_copy().wait_recv()
        mine[0] = mine[0] + pair[...]
        for j in range(near_size):
            sum_copy(0, j).start()

        @pl.when(present(0))
        def _():
            def pace(k, carry):
                halo_copy(1, 0, k - ahead).wait_send()
                halo_copy(1, 0, k).start()
                return carry

            lax.fori_loop(ahead, chunks, pace, 0)

        total_copy().wait_recv()

    @pl.when(odd == 1)
    def _():
        settle(moment3)
        pair_copy().start()
        for i in range(near_size):
            sum_arrival(0, i).wait_recv()
        total = got[0, 0]
        for i in range(1, near_size):
            total = total + got[0, i]
        for stage, (size, _) in enumerate(stages):
            if stage == 0:
                continue
            mine[stage] = total
            for j in range(1, size):
                sum_copy(stage, j).start()
            digit = peer(stage, 0)[0]
            got[stage, digit] = total
            for j in range(1, size):
                sum_arrival(stage, lax.rem(digit + j, size)).wait_recv()
            total = got[stage, 0]
            for i in range(1, size):
                total = total + got[stage, i]
        totals[...] = total
        total_copy().start()

    everyone = totals[...]
    s0, s1, s2, s3 = (everyone[i:i + 1] for i in range(4))

    def whole(value):
        return jnp.sum(value, axis=1, keepdims=True)

    rz_old = whole(s0)
    step_old = rz_old / whole(s1)
    rz_now = whole(s0 - 2.0 * step_old * s1 + step_old * step_old * s2)
    grown = 1.0 + rz_now / rz_old
    product = whole(grown * grown * s1 - 2.0 * step_old * grown * s2 + step_old * step_old * s3)
    step_size = rz_now / product
    lead = step_old + step_size * grown
    trail = step_size * step_old

    for plane in range(depth):
        def last(t, carry, plane=plane):
            start = pl.multiple_of(t * TILE, TILE)
            at = pl.ds(start, TILE)
            base = r0[plane, at, :]
            along = w0[plane, at, :]
            sol_ref[plane, at, :] = inv[plane + 1, at, :] * (lead * base - trail * along)
            res_ref[plane, at, :] = base - lead * along + trail * w1[plane, at, :]
            return carry

        lax.fori_loop(0, steps, last, 0)

    @pl.when(jnp.logical_and(odd == 1, present(1)))
    def _():
        plane = depth - 1

        def late(k, carry):
            halo_arrival(1, 1, k).wait_recv()

            def tile(t, carry):
                at = pl.ds(row(k, t), TILE)
                beyond = jnp.where(inv[plane + 1, at, :] > 0.0, halo_u[1, at, :], 0.0)
                res_ref[plane, at, :] = res_ref[plane, at, :] - trail * beyond
                return carry

            return lax.fori_loop(0, tiles, tile, carry)

        lax.fori_loop(0, chunks, late, 0)

    for side in range(2):
        @pl.when(present(side))
        def _():
            bit_copy(side).wait_send()
            for phase in range(2):
                for k in range(chunks):
                    if phase == 1 and side == 0 and k < chunks - min(2, chunks):
                        @pl.when(odd == 1)
                        def _():
                            halo_copy(phase, side, k).wait_send()
                    else:
                        halo_copy(phase, side, k).wait_send()

    @pl.when(odd == 0)
    def _():
        for j in range(near_size):
            sum_copy(0, j).wait_send()

    @pl.when(odd == 1)
    def _():
        pair_copy().wait_send()
        total_copy().wait_send()
        for stage, (size, _) in enumerate(stages):
            if stage == 0:
                continue
            for j in range(1, size):
                sum_copy(stage, j).wait_send()


def groups(chips):
    size = math.gcd(chips, 4)
    stages, stride = [(size, 1)], size
    while stride < chips:
        rest = chips // stride
        size = 2 if rest % 2 == 0 else rest
        stages.append((size, stride))
        stride *= size
    return stages


def body(count, right_side, cell_flags):
    depth, rows, cols = right_side.shape
    stages = groups(count // 2)
    widest = max(size for size, _ in stages)
    chunk = math.gcd(rows, 64)
    chunks = rows // chunk
    f32 = jnp.float32
    field = pltpu.VMEM((depth, rows, cols), f32)
    padded = pltpu.VMEM((depth, rows + 2 * PAD, cols), f32)
    outer = len({0, 1, depth - 2, depth - 1})
    dma = pltpu.SemaphoreType.DMA
    grant = VMEM_BYTES - 8 * right_side.size - 2**19
    return pl.pallas_call(
        functools.partial(kernel, count, chunk, stages),
        out_shape=(field, field),
        in_specs=[pl.BlockSpec(memory_space=pltpu.HBM)] * 2,
        out_specs=(pl.BlockSpec(memory_space=pltpu.VMEM),) * 2,
        scratch_shapes=[
            field,
            pltpu.VMEM((depth, rows, cols), jnp.int32),
            field,
            pltpu.VMEM((depth + 2, rows, cols), f32),
            pltpu.VMEM((depth + 4, rows + 2 * PAD, cols), f32),
            padded, padded, field, field,
            pltpu.VMEM((2, rows, cols), f32),
            pltpu.VMEM((2, rows, cols), f32),
            pltpu.VMEM((outer, rows // 32, cols), jnp.int32),
            pltpu.VMEM((2, 2, rows // 32, cols), jnp.int32),
            pltpu.VMEM((8, 128), f32),
            pltpu.VMEM((8, 128), f32),
            pltpu.VMEM((len(stages), 8, 128), f32),
            pltpu.VMEM((len(stages), widest, 8, 128), f32),
            dma((2, depth)),
            dma((2,)), dma((2,)),
            dma((2, 2, chunks)), dma((2, 2, chunks)),
            dma, dma, dma, dma,
            dma((len(stages), widest)), dma((len(stages), widest)),
        ],
        compiler_params=pltpu.CompilerParams(
            collective_id=0, has_side_effects=True, vmem_limit_bytes=grant
        ),
    )(right_side, cell_flags)


def solution(mesh):
    placed = (P("gz", None, None), P("gz", None, None))
    return jax.shard_map(
        functools.partial(body, mesh.shape["gz"]),
        mesh=mesh,
        in_specs=placed,
        out_specs=placed,
        check_vma=False,
    )
```

```python
import functools
import math

import jax
import jax.numpy as jnp
from jax import lax
from jax.experimental import pallas as pl
from jax.experimental.pallas import tpu as pltpu
from jax.sharding import PartitionSpec as P

MESH = pl.DeviceIdType.MESH
TILE = 16
LAST = 64
CHUNK = 64
AFTER = 128
LAGS = (192, 256)
BURSTS = (128, 192)
HOLDS = (64, 192)
WINDOW = 256
PAD = 8
VMEM_BYTES = 67_043_328


def kernel(
    count, chunk, stages,
    side_hbm, flag_hbm, sol_ref, res_ref,
    rhs, flags, r0, inv, shadow, u0, u1, w0, w1, halo_r, halo_u, solid, fluid, code,
    pair, mine, got,
    in_sem, go, known, bit_send, bit_recv, halo_send, halo_recv,
    pair_send, pair_recv, sum_send, sum_recv,
):
    depth, rows, cols = rhs.shape
    words = rows // 32
    chunks = rows // chunk
    tiles = chunk // TILE
    steps = rows // TILE

    def pieces(length):
        return min(max(length // chunk, 1), chunks)

    deep = pieces(WINDOW)
    final = math.gcd(rows, LAST)
    near_size, far_size = stages[0][0], stages[1][0]
    me = lax.axis_index("gz")
    chip, odd = me // 2, lax.rem(me, 2)
    is_even, is_odd = odd == 0, odd == 1
    near_side, far_side = 1 - odd, odd
    near_plane, far_plane = near_side * (depth - 1), far_side * (depth - 1)
    partner = me + 1 - 2 * odd
    has_far = jnp.where(is_even, me > 0, me < count - 1)

    digit = lax.rem(chip, near_size)
    relief = near_size // 2 if near_size > 2 else 0
    is_first, is_relief = digit == 0, digit == relief

    def by_place(lengths):
        return jnp.where(is_first, pieces(lengths[1]), pieces(lengths[0]))

    lag, burst, hold = by_place(LAGS), by_place(BURSTS), by_place(HOLDS)

    def load(plane, which):
        source, target = ((flag_hbm, flags), (side_hbm, rhs))[which]
        return pltpu.make_async_copy(source.at[plane], target.at[plane], in_sem.at[which, plane])

    def peer(stage, j):
        size, stride = stages[stage]
        digit = lax.rem(chip // stride, size)
        return digit, chip + (lax.rem(digit + j, size) - digit) * stride

    barrier = pltpu.get_barrier_semaphore()

    def greet(other):
        pl.semaphore_signal(barrier, inc=1, device_id=(other,), device_id_type=MESH)

    @pl.when(has_far)
    def _():
        greet(me - 1 + 2 * odd)

    greet(partner)
    inner_planes = list(range(1, depth - 1))
    load(far_plane, 0).start()
    for plane in [near_plane] + inner_planes:
        load(plane, 0).start()
    load(far_plane, 1).start()
    for plane in [near_plane] + inner_planes:
        load(plane, 1).start()
    pairs = far_size & (far_size - 1) == 0
    if pairs:
        rounds = [(far_size >> i,) for i in range(1, far_size.bit_length())]
    else:
        rounds = [tuple(range(1, far_size))]

    def far_peer(distance):
        digit = chip // near_size
        if pairs:
            step = distance * (1 - 2 * lax.rem(digit // distance, 2))
        else:
            step = lax.rem(digit + distance, far_size) - digit
        return 2 * (chip + step * near_size) + 1

    if relief:
        @pl.when(is_even)
        def _():
            greet(2 * (chip - digit + lax.rem(digit + relief, near_size)) + 1)

    @pl.when(is_odd)
    def _():
        for group in rounds:
            for distance in group:
                greet(far_peer(distance))
        for j in range(1, near_size):
            greet(2 * peer(0, j)[1] + 1)

    def tell(which):
        for distance in rounds[which]:
            pl.semaphore_signal(
                known.at[which], inc=1, device_id=(far_peer(distance),), device_id_type=MESH
            )

    def hear(which):
        pl.semaphore_wait(known.at[which], len(rounds[which]))
        if which + 1 < len(rounds):
            tell(which + 1)

    blank = jnp.zeros((PAD, cols), jnp.float32)
    for ref in (u0, u1):
        for plane in range(ref.shape[0]):
            ref[plane, 0:PAD, :] = blank
            ref[plane, rows + PAD:rows + 2 * PAD, :] = blank

    @pl.when(jnp.logical_not(has_far))
    def _():
        solid[far_side * (depth + 2)] = jnp.zeros((words, cols), jnp.int32)
        solid[far_side * (depth + 2) + 1] = jnp.zeros((words, cols), jnp.int32)

        def clear(t, carry):
            at = pl.ds(pl.multiple_of(t * TILE, TILE), TILE)
            halo_r[far_side, at, :] = jnp.zeros((TILE, cols), jnp.float32)
            halo_u[far_side, at, :] = jnp.zeros((TILE, cols), jnp.float32)
            return carry

        lax.fori_loop(0, steps, clear, 0)

    def on(side, there):
        if side is far_side:
            pl.when(has_far)(there)
        else:
            there()

    def halo_copy(phase, side, k, raw=False):
        at = pl.multiple_of(k * chunk, chunk)
        plane = side * (depth - 1)
        if raw:
            source = r0.at[plane, pl.ds(at, chunk)]
        else:
            field = (u0, u1)[phase]
            source = field.at[plane, pl.ds(pl.multiple_of(at + PAD, PAD), chunk)]
        return pltpu.make_async_remote_copy(
            src_ref=source,
            dst_ref=(halo_r, halo_u)[phase].at[1 - side, pl.ds(at, chunk)],
            send_sem=halo_send.at[phase, side, k],
            recv_sem=halo_recv.at[phase, 1 - side, k],
            device_id=(me - 1 + 2 * side,),
            device_id_type=MESH,
        )

    def halo_arrival(phase, side, k):
        at = pl.multiple_of(k * chunk, chunk)
        target = (halo_r, halo_u)[phase].at[side, pl.ds(at, chunk)]
        return pltpu.make_async_remote_copy(
            src_ref=target,
            dst_ref=target,
            send_sem=halo_send.at[phase, side, k],
            recv_sem=halo_recv.at[phase, side, k],
            device_id=(me - 1 + 2 * side,),
            device_id_type=MESH,
        )

    def wait_halo(phase, side, k):
        on(side, lambda: halo_arrival(phase, side, k).wait_recv())

    def send_plane(phase, side, first=0, raw=False, last=chunks):
        def all_chunks():
            def one(k, carry):
                halo_copy(phase, side, k, raw).start()
                return carry

            lax.fori_loop(first, last, one, 0)

        on(side, all_chunks)

    def sent_plane(phase, side, first=0, last=chunks):
        def all_chunks():
            def one(k, carry):
                halo_copy(phase, side, k).wait_send()
                return carry

            lax.fori_loop(first, last, one, 0)

        on(side, all_chunks)

    def bit_copy(side, planes, arrival=False):
        mine_at, theirs_at = 2 + side * (depth - 1), 1 + (1 - side) * (depth + 1)
        halo_at = 1 + side * (depth + 1)
        return pltpu.make_async_remote_copy(
            src_ref=solid.at[pl.ds(halo_at if arrival else mine_at, planes)],
            dst_ref=solid.at[pl.ds(halo_at if arrival else theirs_at, planes)],
            send_sem=bit_send.at[side],
            recv_sem=bit_recv.at[side if arrival else 1 - side],
            device_id=(me - 1 + 2 * side,),
            device_id_type=MESH,
        )

    def row(k, t):
        return pl.multiple_of(k * chunk + t * TILE, TILE)

    def mask(plane, first, last):
        def tile(t, carry):
            at = pl.ds(pl.multiple_of(t * TILE, TILE), TILE)
            r0[plane, at, :] = jnp.where(flags[plane, at, :] == 1, rhs[plane, at, :], 0.0)
            return carry

        lax.fori_loop(first, last, tile, 0)

    def pack(plane):
        def one(j, found):
            at = pl.ds(pl.multiple_of(j * words, words), words)
            kinds = flags[plane, at, :]
            return tuple(
                word | jnp.left_shift(jnp.where(kinds == kind, 1, 0), j)
                for word, kind in zip(found, (2, 1))
            )

        empty = jnp.zeros((words, cols), jnp.int32)
        solid[plane + 2], fluid[plane] = lax.fori_loop(0, 32, one, (empty, empty))

    for plane in [far_plane, near_plane] + inner_planes:
        load(plane, 0).wait()
        pack(plane)
    greeted = sum(len(group) for group in rounds) + near_size - 1 + (relief > 0)
    pl.semaphore_wait(barrier, 1 + has_far.astype(jnp.int32) + odd * greeted)

    @pl.when(is_even)
    def _():
        on(far_side, lambda: bit_copy(0, 2).start())

    @pl.when(is_odd)
    def _():
        on(far_side, lambda: bit_copy(1, 1).start())
        if rounds:
            tell(0)

    bit_copy(near_side, 1).start()
    load(far_plane, 1).wait()
    mask(far_plane, 0, steps)

    @pl.when(is_even)
    def _():
        send_plane(0, far_side, 0, True)

    for plane in [near_plane] + inner_planes:
        load(plane, 1).wait()
        mask(plane, 0, steps)

    bit_copy(near_side, 1, True).wait_recv()

    @pl.when(is_even)
    def _():
        on(far_side, lambda: bit_copy(0, 1, True).wait_recv())

    @pl.when(is_odd)
    def _():
        on(far_side, lambda: bit_copy(1, 2, True).wait_recv())

    def classify(at, slot, known_fluid):
        word = solid[at]
        line = lax.broadcasted_iota(jnp.int32, (words, cols), 0)
        across = lax.broadcasted_iota(jnp.int32, (words, cols), 1)
        before, after = pltpu.roll(word, 1, 0), pltpu.roll(word, words - 1, 0)
        before = jnp.where(line == 0, jnp.left_shift(before, 1), before)
        after = jnp.where(line == words - 1, lax.shift_right_logical(after, 1), after)
        left = jnp.where(across == 0, 0, pltpu.roll(word, 1, 1))
        right = jnp.where(across == cols - 1, 0, pltpu.roll(word, cols - 1, 1))

        def add(a, b, c):
            return a ^ b ^ c, (a & b) | (c & (a ^ b))

        ones, twos = add(before, after, left)
        more_ones, more_twos = add(right, solid[at - 1], solid[at + 1])
        digits = [ones ^ more_ones, *add(twos, more_twos, ones & more_ones)]
        for i, digit in enumerate(digits):
            if known_fluid is not None:
                digit = digit | ~known_fluid
            code[slot, i] = digit

    def inverse(slot, j):
        bit = jnp.left_shift(1, j)
        ones, twos, fours = ((code[slot, i] & bit) != 0 for i in range(3))
        none, one, two, three, four, five, six, out = (
            jnp.float32(value) for value in (1 / 6, 1 / 5, 1 / 4, 1 / 3, 1 / 2, 1.0, 1.0, 0.0)
        )
        low = jnp.where(twos, jnp.where(ones, three, two), jnp.where(ones, one, none))
        high = jnp.where(twos, jnp.where(ones, out, six), jnp.where(ones, five, four))
        return jnp.where(fours, high, low)

    column = lax.broadcasted_iota(jnp.int32, (TILE, cols), 1)

    def inplane(ref, plane, start):
        block = ref[plane, pl.ds(start, TILE + 2 * PAD), :]
        centre = block[PAD:PAD + TILE]
        total = block[PAD - 1:PAD - 1 + TILE] + block[PAD + 1:PAD + 1 + TILE]
        total = total + jnp.where(column == 0, 0.0, pltpu.roll(centre, 1, 1))
        total = total + jnp.where(column == cols - 1, 0.0, pltpu.roll(centre, cols - 1, 1))
        return centre, total

    def centre_of(ref, plane, start):
        return ref[plane, pl.ds(pl.multiple_of(start + PAD, PAD), TILE), :]

    def put(ref, plane, start, value):
        ref[plane, pl.ds(pl.multiple_of(start + PAD, PAD), TILE), :] = value

    def fold(value):
        total = value[0:8]
        for i in range(8, value.shape[0], 8):
            total = total + value[i:i + 8]
        return total

    none = jnp.zeros((8, cols), jnp.float32)

    for plane in range(depth):
        classify(plane + 2, plane, fluid[plane])

    def first(j, moment):
        start = pl.multiple_of(j * words, words)
        at = pl.ds(start, words)
        padded = pl.ds(pl.multiple_of(start + PAD, PAD), words)
        for plane in range(depth):
            value = inverse(plane, j)
            inv[plane, at, :] = value
            residual = r0[plane, at, :]
            precond = residual * value
            u0[plane, padded, :] = precond
            moment = moment + fold(residual * precond)
        return moment

    moment0 = lax.fori_loop(0, 32, first, none)
    send_plane(0, near_side)

    @pl.when(is_even)
    def _():
        def plain(t, carry):
            at = pl.ds(pl.multiple_of(t * TILE, TILE), TILE)
            shadow[at, :] = jnp.ones((TILE, cols), jnp.float32)
            return carry

        lax.fori_loop(0, steps, plain, 0)

    @pl.when(is_odd)
    def _():
        classify(depth + 2, depth, None)

        def beyond(j, carry):
            shadow[pl.ds(pl.multiple_of(j * words, words), words), :] = inverse(depth, j)
            return carry

        lax.fori_loop(0, 32, beyond, 0)
        if rounds:
            hear(0)

    def local_part(field, scaled, out, plane, start):
        at = pl.ds(start, TILE)
        _, total = inplane(field, plane, start)
        if plane > 0:
            total = total + centre_of(field, plane - 1, start)
        if plane < depth - 1:
            total = total + centre_of(field, plane + 1, start)
        image = jnp.where(inv[plane, at, :] > 0.0, scaled[plane, at, :] - total, 0.0)
        out[plane, at, :] = image
        return image

    def apply_once(plane, start, image, value, moments):
        precond = image * value
        put(u1, plane, start, precond)
        return (
            moments[0] + fold(image * centre_of(u0, plane, start)),
            moments[1] + fold(image * precond),
        )

    def second(t, moments):
        start = pl.multiple_of(t * TILE, TILE)
        for plane in range(depth):
            image = local_part(u0, r0, w0, plane, start)
            if 0 < plane < depth - 1:
                value = inv[plane, pl.ds(start, TILE), :]
                moments = apply_once(plane, start, image, value, moments)
        return moments

    moments = lax.fori_loop(0, steps, second, (none, none))

    def edge_one(side, moments):
        plane = side * (depth - 1)

        def step(k, moments):
            wait_halo(0, side, k)

            def tile(t, moments):
                start = row(k, t)
                at = pl.ds(start, TILE)
                value = inv[plane, at, :]
                beyond = halo_r[side, at, :]
                if side is far_side:
                    beyond = beyond * shadow[at, :]
                image = jnp.where(value > 0.0, w0[plane, at, :] - beyond, 0.0)
                w0[plane, at, :] = image
                return apply_once(plane, start, image, value, moments)

            moments = lax.fori_loop(0, tiles, tile, moments)
            if side is near_side:
                halo_copy(1, side, k).start()
            else:
                @pl.when(jnp.logical_and(is_odd, has_far))
                def _():
                    halo_copy(1, side, k).start()

            return moments

        return lax.fori_loop(0, chunks, step, moments)

    started = chunks - pieces(AFTER)
    passing = digit == near_size - 1

    @pl.when(is_even)
    def _():
        sent_plane(0, far_side, 0, started)

        @pl.when(passing)
        def _():
            sent_plane(0, far_side, started)

        pl.semaphore_signal(go, inc=1, device_id=(partner,), device_id_type=MESH)

    @pl.when(is_odd)
    def _():
        pl.semaphore_wait(go, 1)
        send_plane(0, far_side)

    moments = edge_one(near_side, moments)
    moment1, moment2 = edge_one(far_side, moments)

    def third(t, moment):
        start = pl.multiple_of(t * TILE, TILE)
        for plane in range(depth):
            image = local_part(u1, w0, w1, plane, start)
            moment = moment + fold(image * centre_of(u1, plane, start))
        return moment

    moment3 = lax.fori_loop(0, steps, third, none)

    def edge_two(side, moment, weight, after):
        plane = side * (depth - 1)

        def step(k, moment):
            wait_halo(1, side, k)
            after(k)

            def tile(t, moment):
                start = row(k, t)
                at = pl.ds(start, TILE)
                beyond = halo_u[side, at, :]
                image = jnp.where(inv[plane, at, :] > 0.0, w1[plane, at, :] - beyond, 0.0)
                w1[plane, at, :] = image
                return moment - weight * fold(beyond * centre_of(u1, plane, start))

            return lax.fori_loop(0, tiles, tile, moment)

        return lax.fori_loop(0, chunks, step, moment)

    def lanes(value):
        total = value[:, 0:128]
        for i in range(128, cols, 128):
            total = total + value[:, i:i + 128]
        return jnp.sum(total, axis=0, keepdims=True)

    def settle(moment):
        for i, value in enumerate((moment0, moment1, moment2, moment)):
            mine[0, i:i + 1, :] = lanes(value)
        mine[0, 4:8, :] = jnp.zeros((4, 128), jnp.float32)

    moment3 = edge_two(near_side, moment3, 1.0, lambda k: None)

    def pair_copy():
        return pltpu.make_async_remote_copy(
            src_ref=mine.at[0], dst_ref=pair, send_sem=pair_send, recv_sem=pair_recv,
            device_id=(partner,), device_id_type=MESH,
        )

    def sum_copy(stage, j, core, shift=0):
        slot, other = peer(stage, j)
        return pltpu.make_async_remote_copy(
            src_ref=mine.at[stage],
            dst_ref=got.at[stage, slot],
            send_sem=sum_send.at[core, stage + (shift > 0), j],
            recv_sem=sum_recv.at[stage, slot],
            device_id=(2 * (other - shift) + core,),
            device_id_type=MESH,
        )

    def across(act):
        act(sum_copy(1, 0, 0))

        def to_all(shift):
            for j in range(1, far_size):
                for core in (1, 0):
                    act(sum_copy(1, j, core, shift))

        if relief:
            pl.when(is_relief)(lambda: to_all(relief))
            pl.when(jnp.logical_not(is_first))(lambda: to_all(0))
        else:
            to_all(0)

    def sum_arrival(stage, slot):
        return pltpu.make_async_remote_copy(
            src_ref=got.at[stage, slot],
            dst_ref=got.at[stage, slot],
            send_sem=sum_send.at[0, stage, 0],
            recv_sem=sum_recv.at[stage, slot],
            device_id=(partner,),
            device_id_type=MESH,
        )

    def gathered(stage):
        total = got[stage, 0]
        for i in range(1, stages[stage][0]):
            total = total + got[stage, i]
        return total

    @pl.when(is_even)
    def _():
        def early(k):
            @pl.when(k == chunks - lag)
            def _():
                pl.semaphore_wait(go, 1)
                send_plane(1, far_side, 0, False, burst)

        settle(edge_two(far_side, moment3, 2.0, early))
        pair_copy().wait_recv()
        mine[0] = mine[0] + pair[...]
        for j in range(near_size):
            sum_copy(0, j, 1).start()

        @pl.when(has_far)
        def _():
            def pace(k, carry):
                halo_copy(1, 0, k - deep).wait_send()
                halo_copy(1, 0, k).start()
                return carry

            send_plane(1, far_side, burst, False, deep)
            lax.fori_loop(deep, chunks, pace, 0)

    @pl.when(is_odd)
    def _():
        settle(moment3)
        pair_copy().start()
        sent_plane(1, far_side, 0, chunks - hold)
        pl.semaphore_signal(go, inc=1, device_id=(partner,), device_id_type=MESH)
        for which in range(1, len(rounds)):
            hear(which)
        for i in range(near_size):
            sum_arrival(0, i).wait_recv()
        total = gathered(0)
        mine[1] = total
        across(lambda copy: copy.start())
        got[1, peer(1, 0)[0]] = total

    bit_copy(near_side, 1).wait_send()
    for phase in range(2):
        sent_plane(phase, near_side)

    @pl.when(is_even)
    def _():
        on(far_side, lambda: bit_copy(0, 2).wait_send())
        @pl.when(jnp.logical_not(passing))
        def _():
            sent_plane(0, far_side, started)

        for j in range(near_size):
            sum_copy(0, j, 1).wait_send()

    @pl.when(is_odd)
    def _():
        on(far_side, lambda: bit_copy(1, 1).wait_send())
        sent_plane(0, far_side)
        sent_plane(1, far_side, chunks - hold)
        pair_copy().wait_send()
        across(lambda copy: copy.wait_send())

    for j in range(1, far_size):
        sum_arrival(1, lax.rem(peer(1, 0)[0] + j, far_size)).wait_recv()
    @pl.when(is_even)
    def _():
        sum_arrival(1, peer(1, 0)[0]).wait_recv()

    everyone = gathered(1)
    s0, s1, s2, s3 = (everyone[i:i + 1] for i in range(4))

    def whole(value):
        return jnp.sum(value, axis=1, keepdims=True)

    rz_old = whole(s0)
    step_old = rz_old / whole(s1)
    rz_now = whole(s0 - 2.0 * step_old * s1 + step_old * step_old * s2)
    grown = 1.0 + rz_now / rz_old
    product = whole(grown * grown * s1 - 2.0 * step_old * grown * s2 + step_old * step_old * s3)
    step_size = rz_now / product
    lead = step_old + step_size * grown
    trail = step_size * step_old

    for plane in range(depth):
        def last(t, carry, plane=plane):
            at = pl.ds(pl.multiple_of(t * final, final), final)
            base = r0[plane, at, :]
            along = w0[plane, at, :]
            sol_ref[plane, at, :] = inv[plane, at, :] * (lead * base - trail * along)
            res_ref[plane, at, :] = base - lead * along + trail * w1[plane, at, :]
            return carry

        lax.fori_loop(0, rows // final, last, 0)

    @pl.when(jnp.logical_and(is_odd, has_far))
    def _():
        plane = depth - 1

        def late(k, carry):
            halo_arrival(1, 1, k).wait_recv()

            def tile(t, carry):
                at = pl.ds(row(k, t), TILE)
                beyond = jnp.where(inv[plane, at, :] > 0.0, halo_u[1, at, :], 0.0)
                res_ref[plane, at, :] = res_ref[plane, at, :] - trail * beyond
                return carry

            return lax.fori_loop(0, tiles, tile, carry)

        lax.fori_loop(0, chunks, late, 0)

    @pl.when(is_even)
    def _():
        sent_plane(1, far_side, chunks - deep)


def store(sol_ref, res_ref, sol_out, res_out, sem):
    copies = []
    for which, (source, target) in enumerate(((sol_ref, sol_out), (res_ref, res_out))):
        for plane in range(sol_ref.shape[0]):
            copies.append(
                pltpu.make_async_copy(source.at[plane], target.at[plane], sem.at[which, plane])
            )
    for copy in copies:
        copy.start()
    for copy in copies:
        copy.wait()


def groups(chips):
    near = math.gcd(chips, 4)
    return (near, 1), (chips // near, near)


def body(count, right_side, cell_flags):
    depth, rows, cols = right_side.shape
    assert count % 2 == 0 and depth > 1
    stages = groups(count // 2)
    widest = max(size for size, _ in stages)
    chunk = math.gcd(rows, CHUNK)
    chunks = rows // chunk
    f32 = jnp.float32
    field = pltpu.VMEM((depth, rows, cols), f32)
    padded = pltpu.VMEM((depth, rows + 2 * PAD, cols), f32)
    dma = pltpu.SemaphoreType.DMA
    grant = VMEM_BYTES - 8 * right_side.size - 2**19
    fields = pl.pallas_call(
        functools.partial(kernel, count, chunk, stages),
        out_shape=(field, field),
        in_specs=[pl.BlockSpec(memory_space=pltpu.HBM)] * 2,
        out_specs=(pl.BlockSpec(memory_space=pltpu.VMEM),) * 2,
        scratch_shapes=[
            field,
            pltpu.VMEM((depth, rows, cols), jnp.int32),
            field, field,
            pltpu.VMEM((rows, cols), f32),
            padded, padded, field, field,
            pltpu.VMEM((2, rows, cols), f32),
            pltpu.VMEM((2, rows, cols), f32),
            pltpu.VMEM((depth + 4, rows // 32, cols), jnp.int32),
            pltpu.VMEM((depth, rows // 32, cols), jnp.int32),
            pltpu.VMEM((depth + 1, 3, rows // 32, cols), jnp.int32),
            pltpu.VMEM((8, 128), f32),
            pltpu.VMEM((2, 8, 128), f32),
            pltpu.VMEM((2, widest, 8, 128), f32),
            dma((2, depth)),
            pltpu.SemaphoreType.REGULAR,
            pltpu.SemaphoreType.REGULAR((max(stages[1][0] - 1, 1),)),
            dma((2,)), dma((2,)),
            dma((2, 2, chunks)), dma((2, 2, chunks)),
            dma, dma,
            dma((2, 3, widest)), dma((2, widest)),
        ],
        compiler_params=pltpu.CompilerParams(
            collective_id=0, has_side_effects=True, vmem_limit_bytes=grant
        ),
    )(right_side, cell_flags)
    result = jax.ShapeDtypeStruct((depth, rows, cols), f32)
    return pl.pallas_call(
        store,
        out_shape=(result, result),
        in_specs=[pl.BlockSpec(memory_space=pltpu.VMEM)] * 2,
        out_specs=(pl.BlockSpec(memory_space=pltpu.HBM),) * 2,
        scratch_shapes=[dma((2, depth))],
        compiler_params=pltpu.CompilerParams(vmem_limit_bytes=2**19),
    )(*fields)


def solution(mesh):
    placed = (P("gz", None, None), P("gz", None, None))
    return jax.shard_map(
        functools.partial(body, mesh.shape["gz"]),
        mesh=mesh,
        in_specs=placed,
        out_specs=placed,
        check_vma=False,
    )
```

```python
import functools
import math

import jax
import jax.numpy as jnp
from jax import lax
from jax.experimental import pallas as pl
from jax.experimental.pallas import tpu as pltpu
from jax.sharding import PartitionSpec as P

MESH = pl.DeviceIdType.MESH
TILE = 16
LAST = 64
CHUNK = 64
AFTER = 128
LAGS = (192, 256)
BURSTS = (128, 192)
HOLDS = (64, 64)
WINDOW = 256
PAD = 8
VMEM_BYTES = 67_043_328


def kernel(
    count, chunk, stages,
    side_hbm, flag_hbm, sol_ref, res_ref,
    rhs, flags, r0, inv, shadow, u0, u1, w0, w1, halo_r, halo_u, solid, fluid, code,
    pair, mine, got,
    in_sem, go, clear, known, bit_send, bit_recv, halo_send, halo_recv,
    pair_send, pair_recv, sum_send, sum_recv,
):
    depth, rows, cols = rhs.shape
    words = rows // 32
    chunks = rows // chunk
    tiles = chunk // TILE
    steps = rows // TILE

    def pieces(length):
        return min(max(length // chunk, 1), chunks)

    deep = pieces(WINDOW)
    final = math.gcd(rows, LAST)
    near_size, far_size = stages[0][0], stages[1][0]
    me = lax.axis_index("gz")
    chip, odd = me // 2, lax.rem(me, 2)
    is_even, is_odd = odd == 0, odd == 1
    near_side, far_side = 1 - odd, odd
    near_plane, far_plane = near_side * (depth - 1), far_side * (depth - 1)
    partner = me + 1 - 2 * odd
    has_far = jnp.where(is_even, me > 0, me < count - 1)

    digit = lax.rem(chip, near_size)
    relief = near_size // 2 if near_size > 2 else 0
    is_first, is_relief = digit == 0, digit == relief

    def by_place(lengths):
        return jnp.where(is_first, pieces(lengths[1]), pieces(lengths[0]))

    lag, burst, hold = by_place(LAGS), by_place(BURSTS), by_place(HOLDS)

    def load(plane, which):
        source, target = ((flag_hbm, flags), (side_hbm, rhs))[which]
        return pltpu.make_async_copy(source.at[plane], target.at[plane], in_sem.at[which, plane])

    def peer(stage, j):
        size, stride = stages[stage]
        digit = lax.rem(chip // stride, size)
        return digit, chip + (lax.rem(digit + j, size) - digit) * stride

    barrier = pltpu.get_barrier_semaphore()

    def greet(other):
        pl.semaphore_signal(barrier, inc=1, device_id=(other,), device_id_type=MESH)

    @pl.when(has_far)
    def _():
        greet(me - 1 + 2 * odd)

    greet(partner)
    inner_planes = list(range(1, depth - 1))
    load(far_plane, 0).start()
    load(far_plane, 1).start()
    for plane in [near_plane] + inner_planes:
        load(plane, 0).start()
    for plane in [near_plane] + inner_planes:
        load(plane, 1).start()
    pairs = far_size & (far_size - 1) == 0
    if pairs:
        rounds = [(far_size >> i,) for i in range(1, far_size.bit_length())]
    else:
        rounds = [tuple(range(1, far_size))]

    def far_peer(distance):
        digit = chip // near_size
        if pairs:
            step = distance * (1 - 2 * lax.rem(digit // distance, 2))
        else:
            step = lax.rem(digit + distance, far_size) - digit
        return 2 * (chip + step * near_size) + 1

    if relief:
        @pl.when(is_even)
        def _():
            greet(2 * (chip - digit + lax.rem(digit + relief, near_size)) + 1)

    @pl.when(is_odd)
    def _():
        for group in rounds:
            for distance in group:
                greet(far_peer(distance))
        for j in range(1, near_size):
            greet(2 * peer(0, j)[1] + 1)

    def tell(which):
        for distance in rounds[which]:
            pl.semaphore_signal(
                known.at[which], inc=1, device_id=(far_peer(distance),), device_id_type=MESH
            )

    def hear(which):
        pl.semaphore_wait(known.at[which], len(rounds[which]))
        if which + 1 < len(rounds):
            tell(which + 1)

    blank = jnp.zeros((PAD, cols), jnp.float32)
    for ref in (u0, u1):
        for plane in range(ref.shape[0]):
            ref[plane, 0:PAD, :] = blank
            ref[plane, rows + PAD:rows + 2 * PAD, :] = blank

    @pl.when(jnp.logical_not(has_far))
    def _():
        solid[far_side * (depth + 2)] = jnp.zeros((words, cols), jnp.int32)
        solid[far_side * (depth + 2) + 1] = jnp.zeros((words, cols), jnp.int32)

        def clear(t, carry):
            at = pl.ds(pl.multiple_of(t * TILE, TILE), TILE)
            halo_r[far_side, at, :] = jnp.zeros((TILE, cols), jnp.float32)
            halo_u[far_side, at, :] = jnp.zeros((TILE, cols), jnp.float32)
            return carry

        lax.fori_loop(0, steps, clear, 0)

    def on(side, there):
        if side is far_side:
            pl.when(has_far)(there)
        else:
            there()

    def halo_copy(phase, side, k, raw=False):
        at = pl.multiple_of(k * chunk, chunk)
        plane = side * (depth - 1)
        if raw:
            source = r0.at[plane, pl.ds(at, chunk)]
        else:
            field = (u0, u1)[phase]
            source = field.at[plane, pl.ds(pl.multiple_of(at + PAD, PAD), chunk)]
        return pltpu.make_async_remote_copy(
            src_ref=source,
            dst_ref=(halo_r, halo_u)[phase].at[1 - side, pl.ds(at, chunk)],
            send_sem=halo_send.at[phase, side, k],
            recv_sem=halo_recv.at[phase, 1 - side, k],
            device_id=(me - 1 + 2 * side,),
            device_id_type=MESH,
        )

    def halo_arrival(phase, side, k):
        at = pl.multiple_of(k * chunk, chunk)
        target = (halo_r, halo_u)[phase].at[side, pl.ds(at, chunk)]
        return pltpu.make_async_remote_copy(
            src_ref=target,
            dst_ref=target,
            send_sem=halo_send.at[phase, side, k],
            recv_sem=halo_recv.at[phase, side, k],
            device_id=(me - 1 + 2 * side,),
            device_id_type=MESH,
        )

    def wait_halo(phase, side, k):
        on(side, lambda: halo_arrival(phase, side, k).wait_recv())

    def send_plane(phase, side, first=0, raw=False, last=chunks):
        def all_chunks():
            def one(k, carry):
                halo_copy(phase, side, k, raw).start()
                return carry

            lax.fori_loop(first, last, one, 0)

        on(side, all_chunks)

    def sent_plane(phase, side, first=0, last=chunks):
        def all_chunks():
            def one(k, carry):
                halo_copy(phase, side, k).wait_send()
                return carry

            lax.fori_loop(first, last, one, 0)

        on(side, all_chunks)

    def bit_copy(side, depth_in=0, arrival=False):
        mine_at = 2 + side * (depth - 1) + depth_in * (1 - 2 * side)
        theirs_at = 1 + (1 - side) * (depth + 1) + depth_in * (1 - 2 * side)
        halo_at = 1 + side * (depth + 1) - depth_in * (1 - 2 * side)
        return pltpu.make_async_remote_copy(
            src_ref=solid.at[halo_at if arrival else mine_at],
            dst_ref=solid.at[halo_at if arrival else theirs_at],
            send_sem=bit_send.at[side, depth_in],
            recv_sem=bit_recv.at[side if arrival else 1 - side, depth_in],
            device_id=(me - 1 + 2 * side,),
            device_id_type=MESH,
        )

    def row(k, t):
        return pl.multiple_of(k * chunk + t * TILE, TILE)

    def mask(plane, first, last):
        def tile(t, carry):
            at = pl.ds(pl.multiple_of(t * TILE, TILE), TILE)
            r0[plane, at, :] = jnp.where(flags[plane, at, :] == 1, rhs[plane, at, :], 0.0)
            return carry

        lax.fori_loop(first, last, tile, 0)

    def pack(plane):
        def one(j, found):
            at = pl.ds(pl.multiple_of(j * words, words), words)
            kinds = flags[plane, at, :]
            return tuple(
                word | jnp.left_shift(jnp.where(kinds == kind, 1, 0), j)
                for word, kind in zip(found, (2, 1))
            )

        empty = jnp.zeros((words, cols), jnp.int32)
        solid[plane + 2], fluid[plane] = lax.fori_loop(0, 32, one, (empty, empty))

    greeted = sum(len(group) for group in rounds) + near_size - 1 + (relief > 0)
    callers = 1 + has_far.astype(jnp.int32)
    reserve = jnp.where(is_first, pieces(AFTER), 0)
    load(far_plane, 0).wait()
    pack(far_plane)

    @pl.when(is_even)
    def _():
        pl.semaphore_wait(barrier, callers)
        on(far_side, lambda: bit_copy(0).start())

    load(far_plane, 1).wait()
    mask(far_plane, 0, tiles)

    @pl.when(is_even)
    def _():
        on(far_side, lambda: halo_copy(0, 0, 0, True).start())

    for plane in [near_plane] + inner_planes:
        load(plane, 0).wait()
        pack(plane)

    @pl.when(is_even)
    def _():
        on(far_side, lambda: bit_copy(0, 1).start())

    @pl.when(is_odd)
    def _():
        pl.semaphore_wait(barrier, callers + greeted)
        on(far_side, lambda: bit_copy(1).start())
        if rounds:
            tell(0)

    bit_copy(near_side).start()
    mask(far_plane, tiles, steps)

    @pl.when(is_even)
    def _():
        send_plane(0, far_side, 1, True, chunks - reserve)

    for plane in [near_plane] + inner_planes:
        load(plane, 1).wait()
        mask(plane, 0, steps)

    bit_copy(near_side, 0, True).wait_recv()
    on(far_side, lambda: bit_copy(far_side, 0, True).wait_recv())

    def classify(at, slot, known_fluid):
        word = solid[at]
        line = lax.broadcasted_iota(jnp.int32, (words, cols), 0)
        across = lax.broadcasted_iota(jnp.int32, (words, cols), 1)
        before, after = pltpu.roll(word, 1, 0), pltpu.roll(word, words - 1, 0)
        before = jnp.where(line == 0, jnp.left_shift(before, 1), before)
        after = jnp.where(line == words - 1, lax.shift_right_logical(after, 1), after)
        left = jnp.where(across == 0, 0, pltpu.roll(word, 1, 1))
        right = jnp.where(across == cols - 1, 0, pltpu.roll(word, cols - 1, 1))

        def add(a, b, c):
            return a ^ b ^ c, (a & b) | (c & (a ^ b))

        ones, twos = add(before, after, left)
        more_ones, more_twos = add(right, solid[at - 1], solid[at + 1])
        digits = [ones ^ more_ones, *add(twos, more_twos, ones & more_ones)]
        for i, digit in enumerate(digits):
            if known_fluid is not None:
                digit = digit | ~known_fluid
            code[slot, i] = digit

    def inverse(slot, j):
        bit = jnp.left_shift(1, j)
        ones, twos, fours = ((code[slot, i] & bit) != 0 for i in range(3))
        none, one, two, three, four, five, six, out = (
            jnp.float32(value) for value in (1 / 6, 1 / 5, 1 / 4, 1 / 3, 1 / 2, 1.0, 1.0, 0.0)
        )
        low = jnp.where(twos, jnp.where(ones, three, two), jnp.where(ones, one, none))
        high = jnp.where(twos, jnp.where(ones, out, six), jnp.where(ones, five, four))
        return jnp.where(fours, high, low)

    column = lax.broadcasted_iota(jnp.int32, (TILE, cols), 1)

    def inplane(ref, plane, start):
        block = ref[plane, pl.ds(start, TILE + 2 * PAD), :]
        centre = block[PAD:PAD + TILE]
        total = block[PAD - 1:PAD - 1 + TILE] + block[PAD + 1:PAD + 1 + TILE]
        total = total + jnp.where(column == 0, 0.0, pltpu.roll(centre, 1, 1))
        total = total + jnp.where(column == cols - 1, 0.0, pltpu.roll(centre, cols - 1, 1))
        return centre, total

    def centre_of(ref, plane, start):
        return ref[plane, pl.ds(pl.multiple_of(start + PAD, PAD), TILE), :]

    def put(ref, plane, start, value):
        ref[plane, pl.ds(pl.multiple_of(start + PAD, PAD), TILE), :] = value

    def fold(value):
        total = value[0:8]
        for i in range(8, value.shape[0], 8):
            total = total + value[i:i + 8]
        return total

    none = jnp.zeros((8, cols), jnp.float32)

    for plane in range(depth):
        classify(plane + 2, plane, fluid[plane])

    def first(j, moment):
        start = pl.multiple_of(j * words, words)
        at = pl.ds(start, words)
        padded = pl.ds(pl.multiple_of(start + PAD, PAD), words)
        for plane in range(depth):
            value = inverse(plane, j)
            inv[plane, at, :] = value
            residual = r0[plane, at, :]
            precond = residual * value
            u0[plane, padded, :] = precond
            moment = moment + fold(residual * precond)
        return moment

    moment0 = lax.fori_loop(0, 32, first, none)
    send_plane(0, near_side)

    @pl.when(jnp.logical_and(is_odd, is_first))
    def _():
        send_plane(0, far_side)

    @pl.when(is_even)
    def _():
        def plain(t, carry):
            at = pl.ds(pl.multiple_of(t * TILE, TILE), TILE)
            shadow[at, :] = jnp.ones((TILE, cols), jnp.float32)
            return carry

        lax.fori_loop(0, steps, plain, 0)

    @pl.when(is_odd)
    def _():
        on(far_side, lambda: bit_copy(1, 1, True).wait_recv())
        classify(depth + 2, depth, None)

        def beyond(j, carry):
            shadow[pl.ds(pl.multiple_of(j * words, words), words), :] = inverse(depth, j)
            return carry

        lax.fori_loop(0, 32, beyond, 0)
        if rounds:
            hear(0)

    def local_part(field, scaled, out, plane, start):
        at = pl.ds(start, TILE)
        _, total = inplane(field, plane, start)
        if plane > 0:
            total = total + centre_of(field, plane - 1, start)
        if plane < depth - 1:
            total = total + centre_of(field, plane + 1, start)
        image = jnp.where(inv[plane, at, :] > 0.0, scaled[plane, at, :] - total, 0.0)
        out[plane, at, :] = image
        return image

    def apply_once(plane, start, image, value, moments):
        precond = image * value
        put(u1, plane, start, precond)
        return (
            moments[0] + fold(image * centre_of(u0, plane, start)),
            moments[1] + fold(image * precond),
        )

    def second(t, moments):
        start = pl.multiple_of(t * TILE, TILE)
        for plane in range(depth):
            image = local_part(u0, r0, w0, plane, start)
            if 0 < plane < depth - 1:
                value = inv[plane, pl.ds(start, TILE), :]
                moments = apply_once(plane, start, image, value, moments)
        return moments

    moments = lax.fori_loop(0, steps, second, (none, none))

    def edge_one(side, moments):
        plane = side * (depth - 1)

        def step(k, moments):
            wait_halo(0, side, k)

            def tile(t, moments):
                start = row(k, t)
                at = pl.ds(start, TILE)
                value = inv[plane, at, :]
                beyond = halo_r[side, at, :]
                if side is far_side:
                    beyond = beyond * shadow[at, :]
                image = jnp.where(value > 0.0, w0[plane, at, :] - beyond, 0.0)
                w0[plane, at, :] = image
                return apply_once(plane, start, image, value, moments)

            moments = lax.fori_loop(0, tiles, tile, moments)
            if side is near_side:
                halo_copy(1, side, k).start()
            else:
                @pl.when(jnp.logical_and(is_odd, has_far))
                def _():
                    halo_copy(1, side, k).start()

            return moments

        return lax.fori_loop(0, chunks, step, moments)

    passing = digit == near_size - 1
    started = jnp.where(
        is_first, 0, chunks - jnp.where(passing, pieces(CHUNK), pieces(AFTER))
    )

    @pl.when(is_odd)
    def _():
        for which in range(1, len(rounds)):
            hear(which)

    @pl.when(jnp.logical_and(is_even, is_first))
    def _():
        send_plane(0, far_side, chunks - reserve, True)

    @pl.when(jnp.logical_not(is_first))
    def _():
        @pl.when(is_even)
        def _():
            sent_plane(0, far_side, 0, started)
            pl.semaphore_signal(go, inc=1, device_id=(partner,), device_id_type=MESH)

        @pl.when(is_odd)
        def _():
            pl.semaphore_wait(go, 1)

            @pl.when(jnp.logical_and(passing, chip >= near_size))
            def _():
                pl.semaphore_signal(
                    clear, inc=1, device_id=(me - 2 * near_size,), device_id_type=MESH
                )

            @pl.when(jnp.logical_and(passing, chip + near_size < count // 2))
            def _():
                pl.semaphore_wait(clear, 1)

            send_plane(0, far_side)

    moments = edge_one(near_side, moments)
    moment1, moment2 = edge_one(far_side, moments)

    def third(t, moment):
        start = pl.multiple_of(t * TILE, TILE)
        for plane in range(depth):
            image = local_part(u1, w0, w1, plane, start)
            moment = moment + fold(image * centre_of(u1, plane, start))
        return moment

    moment3 = lax.fori_loop(0, steps, third, none)

    def edge_two(side, moment, weight, after):
        plane = side * (depth - 1)

        def step(k, moment):
            wait_halo(1, side, k)
            after(k)

            def tile(t, moment):
                start = row(k, t)
                at = pl.ds(start, TILE)
                beyond = halo_u[side, at, :]
                image = jnp.where(inv[plane, at, :] > 0.0, w1[plane, at, :] - beyond, 0.0)
                w1[plane, at, :] = image
                return moment - weight * fold(beyond * centre_of(u1, plane, start))

            return lax.fori_loop(0, tiles, tile, moment)

        return lax.fori_loop(0, chunks, step, moment)

    def lanes(value):
        total = value[:, 0:128]
        for i in range(128, cols, 128):
            total = total + value[:, i:i + 128]
        return jnp.sum(total, axis=0, keepdims=True)

    for i, value in enumerate((moment0, moment1, moment2)):
        mine[0, i:i + 1, :] = lanes(value)
    mine[0, 3:8, :] = jnp.zeros((5, 128), jnp.float32)
    moment3 = edge_two(near_side, moment3, 1.0, lambda k: None)

    def pair_copy():
        return pltpu.make_async_remote_copy(
            src_ref=mine.at[0], dst_ref=pair, send_sem=pair_send, recv_sem=pair_recv,
            device_id=(partner,), device_id_type=MESH,
        )

    def sum_copy(stage, j, core, shift=0):
        slot, other = peer(stage, j)
        return pltpu.make_async_remote_copy(
            src_ref=mine.at[stage],
            dst_ref=got.at[stage, slot],
            send_sem=sum_send.at[core, stage + (shift > 0), j],
            recv_sem=sum_recv.at[stage, slot],
            device_id=(2 * (other - shift) + core,),
            device_id_type=MESH,
        )

    def across(act):
        act(sum_copy(1, 0, 0))

        def to_all(shift):
            for j in range(1, far_size):
                for core in (1, 0):
                    act(sum_copy(1, j, core, shift))

        if relief:
            pl.when(is_relief)(lambda: to_all(relief))
            pl.when(jnp.logical_not(is_first))(lambda: to_all(0))
        else:
            to_all(0)

    def sum_arrival(stage, slot):
        return pltpu.make_async_remote_copy(
            src_ref=got.at[stage, slot],
            dst_ref=got.at[stage, slot],
            send_sem=sum_send.at[0, stage, 0],
            recv_sem=sum_recv.at[stage, slot],
            device_id=(partner,),
            device_id_type=MESH,
        )

    def gathered(stage):
        total = got[stage, 0]
        for i in range(1, stages[stage][0]):
            total = total + got[stage, i]
        return total

    @pl.when(is_even)
    def _():
        def early(k):
            @pl.when(k == chunks - lag)
            def _():
                @pl.when(jnp.logical_or(jnp.logical_not(is_first), chip >= near_size))
                def _():
                    pl.semaphore_wait(go, 1)

                send_plane(1, far_side, 0, False, burst)

        pair_copy().wait_recv()
        mine[0] = mine[0] + pair[...]
        moment = edge_two(far_side, moment3, 2.0, early)
        mine[0, 3:4, :] = mine[0, 3:4, :] + lanes(moment)
        for j in range(near_size):
            sum_copy(0, j, 1).start()

        @pl.when(has_far)
        def _():
            def pace(k, carry):
                halo_copy(1, 0, k - deep).wait_send()
                halo_copy(1, 0, k).start()
                return carry

            send_plane(1, far_side, burst, False, deep)
            lax.fori_loop(deep, chunks, pace, 0)

    @pl.when(is_odd)
    def _():
        mine[0, 3:4, :] = lanes(moment3)
        pair_copy().start()
        sent_plane(1, far_side, 0, chunks - hold)

        @pl.when(jnp.logical_or(jnp.logical_not(is_first), chip + near_size < count // 2))
        def _():
            waiting = jnp.where(is_first, me - 1 + 2 * near_size, partner)
            pl.semaphore_signal(go, inc=1, device_id=(waiting,), device_id_type=MESH)

        for i in range(near_size):
            sum_arrival(0, i).wait_recv()
        total = gathered(0)
        mine[1] = total
        across(lambda copy: copy.start())
        got[1, peer(1, 0)[0]] = total

    bit_copy(near_side).wait_send()
    on(far_side, lambda: bit_copy(far_side).wait_send())
    for phase in range(2):
        sent_plane(phase, near_side)

    @pl.when(is_even)
    def _():
        on(far_side, lambda: bit_copy(0, 1).wait_send())
        sent_plane(0, far_side, started)
        for j in range(near_size):
            sum_copy(0, j, 1).wait_send()

    @pl.when(is_odd)
    def _():
        sent_plane(0, far_side)
        sent_plane(1, far_side, chunks - hold)
        pair_copy().wait_send()
        across(lambda copy: copy.wait_send())

    for j in range(1, far_size):
        sum_arrival(1, lax.rem(peer(1, 0)[0] + j, far_size)).wait_recv()
    @pl.when(is_even)
    def _():
        sum_arrival(1, peer(1, 0)[0]).wait_recv()

    everyone = gathered(1)
    s0, s1, s2, s3 = (everyone[i:i + 1] for i in range(4))

    def whole(value):
        return jnp.sum(value, axis=1, keepdims=True)

    rz_old = whole(s0)
    step_old = rz_old / whole(s1)
    rz_now = whole(s0 - 2.0 * step_old * s1 + step_old * step_old * s2)
    grown = 1.0 + rz_now / rz_old
    product = whole(grown * grown * s1 - 2.0 * step_old * grown * s2 + step_old * step_old * s3)
    step_size = rz_now / product
    lead = step_old + step_size * grown
    trail = step_size * step_old

    for plane in range(depth):
        def last(t, carry, plane=plane):
            at = pl.ds(pl.multiple_of(t * final, final), final)
            base = r0[plane, at, :]
            along = w0[plane, at, :]
            sol_ref[plane, at, :] = inv[plane, at, :] * (lead * base - trail * along)
            res_ref[plane, at, :] = base - lead * along + trail * w1[plane, at, :]
            return carry

        lax.fori_loop(0, rows // final, last, 0)

    @pl.when(jnp.logical_and(is_odd, has_far))
    def _():
        plane = depth - 1

        def late(k, carry):
            halo_arrival(1, 1, k).wait_recv()

            def tile(t, carry):
                at = pl.ds(row(k, t), TILE)
                beyond = jnp.where(inv[plane, at, :] > 0.0, halo_u[1, at, :], 0.0)
                res_ref[plane, at, :] = res_ref[plane, at, :] - trail * beyond
                return carry

            return lax.fori_loop(0, tiles, tile, carry)

        lax.fori_loop(0, chunks, late, 0)

    @pl.when(is_even)
    def _():
        sent_plane(1, far_side, chunks - deep)


def store(sol_ref, res_ref, sol_out, res_out, sem):
    copies = []
    for which, (source, target) in enumerate(((sol_ref, sol_out), (res_ref, res_out))):
        for plane in range(sol_ref.shape[0]):
            copies.append(
                pltpu.make_async_copy(source.at[plane], target.at[plane], sem.at[which, plane])
            )
    for copy in copies:
        copy.start()
    for copy in copies:
        copy.wait()


def groups(chips):
    near = math.gcd(chips, 4)
    return (near, 1), (chips // near, near)


def body(count, right_side, cell_flags):
    depth, rows, cols = right_side.shape
    assert count % 2 == 0 and depth > 1
    stages = groups(count // 2)
    widest = max(size for size, _ in stages)
    chunk = math.gcd(rows, CHUNK)
    chunks = rows // chunk
    f32 = jnp.float32
    field = pltpu.VMEM((depth, rows, cols), f32)
    padded = pltpu.VMEM((depth, rows + 2 * PAD, cols), f32)
    dma = pltpu.SemaphoreType.DMA
    grant = VMEM_BYTES - 8 * right_side.size - 2**19
    fields = pl.pallas_call(
        functools.partial(kernel, count, chunk, stages),
        out_shape=(field, field),
        in_specs=[pl.BlockSpec(memory_space=pltpu.HBM)] * 2,
        out_specs=(pl.BlockSpec(memory_space=pltpu.VMEM),) * 2,
        scratch_shapes=[
            field,
            pltpu.VMEM((depth, rows, cols), jnp.int32),
            field, field,
            pltpu.VMEM((rows, cols), f32),
            padded, padded, field, field,
            pltpu.VMEM((2, rows, cols), f32),
            pltpu.VMEM((2, rows, cols), f32),
            pltpu.VMEM((depth + 4, rows // 32, cols), jnp.int32),
            pltpu.VMEM((depth, rows // 32, cols), jnp.int32),
            pltpu.VMEM((depth + 1, 3, rows // 32, cols), jnp.int32),
            pltpu.VMEM((8, 128), f32),
            pltpu.VMEM((2, 8, 128), f32),
            pltpu.VMEM((2, widest, 8, 128), f32),
            dma((2, depth)),
            pltpu.SemaphoreType.REGULAR,
            pltpu.SemaphoreType.REGULAR,
            pltpu.SemaphoreType.REGULAR((max(stages[1][0] - 1, 1),)),
            dma((2, 2)), dma((2, 2)),
            dma((2, 2, chunks)), dma((2, 2, chunks)),
            dma, dma,
            dma((2, 3, widest)), dma((2, widest)),
        ],
        compiler_params=pltpu.CompilerParams(
            collective_id=0, has_side_effects=True, vmem_limit_bytes=grant
        ),
    )(right_side, cell_flags)
    result = jax.ShapeDtypeStruct((depth, rows, cols), f32)
    return pl.pallas_call(
        store,
        out_shape=(result, result),
        in_specs=[pl.BlockSpec(memory_space=pltpu.VMEM)] * 2,
        out_specs=(pl.BlockSpec(memory_space=pltpu.HBM),) * 2,
        scratch_shapes=[dma((2, depth))],
        compiler_params=pltpu.CompilerParams(vmem_limit_bytes=2**19),
    )(*fields)


def solution(mesh):
    placed = (P("gz", None, None), P("gz", None, None))
    return jax.shard_map(
        functools.partial(body, mesh.shape["gz"]),
        mesh=mesh,
        in_specs=placed,
        out_specs=placed,
        check_vma=False,
    )
```

```python
import functools
import math

import jax
import jax.numpy as jnp
from jax import lax
from jax.experimental import pallas as pl
from jax.experimental.pallas import tpu as pltpu
from jax.sharding import PartitionSpec as P

MESH = pl.DeviceIdType.MESH
TILE = 16
LAST = 64
LATE = (0, 2, 3, 5, 7, 8)
CHUNK = 64
PAD = 8
VMEM_BYTES = 67_043_328


def kernel(
    count, chunk, stages,
    side_hbm, flag_hbm, sol_ref, res_ref,
    rhs, flags, r0, inv, shadow, u0, u1, w0, w1, halo_r, halo_u, solid, fluid, code,
    pair, mine, got,
    in_sem, go, clear, known, bit_send, bit_recv, far_send, far_recv, near_send, near_recv,
    pair_send, pair_recv, sum_send, sum_recv,
):
    depth, rows, cols = rhs.shape
    words = rows // 32
    steps = rows // TILE
    parts = rows // chunk
    marks = sorted({0, 1, max(parts - 3, 0), max(parts - 2, 0), max(parts - 1, 0), parts})
    spans = [(a * chunk, (b - a) * chunk) for a, b in zip(marks, marks[1:])]
    most = (0, rows - spans[-1][1])
    late_marks = [rows * eighth // 8 for eighth in LATE]
    lates = [(a, b - a) for a, b in zip(late_marks, late_marks[1:])]
    final = math.gcd(rows, LAST)
    near_size, far_size = stages[0][0], stages[1][0]
    me = lax.axis_index("gz")
    chip, odd = me // 2, lax.rem(me, 2)
    is_even, is_odd = odd == 0, odd == 1
    near_side, far_side = 1 - odd, odd
    near_plane, far_plane = near_side * (depth - 1), far_side * (depth - 1)
    partner = me + 1 - 2 * odd
    has_far = jnp.where(is_even, me > 0, me < count - 1)

    digit = lax.rem(chip, near_size)
    relief = near_size // 2 if near_size > 2 else 0
    is_first, is_relief = digit == 0, digit == relief

    def load(plane, which):
        source, target = ((flag_hbm, flags), (side_hbm, rhs))[which]
        return pltpu.make_async_copy(source.at[plane], target.at[plane], in_sem.at[which, plane])

    def peer(stage, j):
        size, stride = stages[stage]
        digit = lax.rem(chip // stride, size)
        return digit, chip + (lax.rem(digit + j, size) - digit) * stride

    barrier = pltpu.get_barrier_semaphore()

    def greet(other):
        pl.semaphore_signal(barrier, inc=1, device_id=(other,), device_id_type=MESH)

    @pl.when(has_far)
    def _():
        greet(me - 1 + 2 * odd)

    greet(partner)
    inner_planes = list(range(1, depth - 1))
    load(far_plane, 0).start()
    load(far_plane, 1).start()
    for plane in [near_plane] + inner_planes:
        load(plane, 0).start()
    for plane in [near_plane] + inner_planes:
        load(plane, 1).start()
    pairs = far_size & (far_size - 1) == 0
    if pairs:
        rounds = [(far_size >> i,) for i in range(1, far_size.bit_length())]
    else:
        rounds = [tuple(range(1, far_size))]

    def far_peer(distance):
        digit = chip // near_size
        if pairs:
            step = distance * (1 - 2 * lax.rem(digit // distance, 2))
        else:
            step = lax.rem(digit + distance, far_size) - digit
        return 2 * (chip + step * near_size) + 1

    if relief:
        @pl.when(is_even)
        def _():
            greet(2 * (chip - digit + lax.rem(digit + relief, near_size)) + 1)

    @pl.when(is_odd)
    def _():
        for group in rounds:
            for distance in group:
                greet(far_peer(distance))
        for j in range(1, near_size):
            greet(2 * peer(0, j)[1] + 1)

    def tell(which):
        for distance in rounds[which]:
            pl.semaphore_signal(
                known.at[which], inc=1, device_id=(far_peer(distance),), device_id_type=MESH
            )

    def hear(which):
        pl.semaphore_wait(known.at[which], len(rounds[which]))
        if which + 1 < len(rounds):
            tell(which + 1)

    blank = jnp.zeros((PAD, cols), jnp.float32)
    for ref in (u0, u1):
        for plane in range(ref.shape[0]):
            ref[plane, 0:PAD, :] = blank
            ref[plane, rows + PAD:rows + 2 * PAD, :] = blank

    @pl.when(jnp.logical_not(has_far))
    def _():
        solid[far_side * (depth + 2)] = jnp.zeros((words, cols), jnp.int32)
        solid[far_side * (depth + 2) + 1] = jnp.zeros((words, cols), jnp.int32)

        def clear(t, carry):
            at = pl.ds(pl.multiple_of(t * TILE, TILE), TILE)
            halo_r[far_side, at, :] = jnp.zeros((TILE, cols), jnp.float32)
            halo_u[far_side, at, :] = jnp.zeros((TILE, cols), jnp.float32)
            return carry

        lax.fori_loop(0, steps, clear, 0)

    def on(side, there):
        if side is far_side:
            pl.when(has_far)(there)
        else:
            there()

    def halo_copy(phase, side, span, send, recv, raw=False):
        start, size = span
        plane = side * (depth - 1)
        if raw:
            source = r0.at[plane, pl.ds(start, size)]
        else:
            source = (u0, u1)[phase].at[plane, pl.ds(start + PAD, size)]
        return pltpu.make_async_remote_copy(
            src_ref=source,
            dst_ref=(halo_r, halo_u)[phase].at[1 - side, pl.ds(start, size)],
            send_sem=send,
            recv_sem=recv,
            device_id=(me - 1 + 2 * side,),
            device_id_type=MESH,
        )

    def halo_arrival(phase, side, span, recv):
        start, size = span
        target = (halo_r, halo_u)[phase].at[side, pl.ds(start, size)]
        return pltpu.make_async_remote_copy(
            src_ref=target,
            dst_ref=target,
            send_sem=near_send.at[phase],
            recv_sem=recv,
            device_id=(me - 1 + 2 * side,),
            device_id_type=MESH,
        )

    def far_copy(phase, i, raw=False):
        send = far_send.at[2 * phase + (i == len(spans) - 1)]
        return halo_copy(phase, far_side, spans[i], send, far_recv.at[phase, i], raw)

    def far_sent(phase):
        sender = far_send.at[2 * phase]
        on(far_side, lambda: halo_copy(
            phase, far_side, most, sender, far_recv.at[phase, 0]
        ).wait_send())

    def far_ended(phase):
        on(far_side, lambda: far_copy(phase, len(spans) - 1).wait_send())

    def late_copy(i):
        return halo_copy(1, far_side, lates[i], far_send.at[2 + i], far_recv.at[1, i])

    def near_copy(phase):
        return halo_copy(
            phase, near_side, (0, rows), near_send.at[phase], near_recv.at[phase]
        )

    def near_arrival(phase):
        return halo_arrival(phase, near_side, (0, rows), near_recv.at[phase])

    def far_pieces(first, last, phase=0, raw=False):
        def some():
            for i in range(first, last):
                far_copy(phase, i, raw).start()

        on(far_side, some)

    def bit_copy(side, depth_in=0, arrival=False):
        mine_at = 2 + side * (depth - 1) + depth_in * (1 - 2 * side)
        theirs_at = 1 + (1 - side) * (depth + 1) + depth_in * (1 - 2 * side)
        halo_at = 1 + side * (depth + 1) - depth_in * (1 - 2 * side)
        return pltpu.make_async_remote_copy(
            src_ref=solid.at[halo_at if arrival else mine_at],
            dst_ref=solid.at[halo_at if arrival else theirs_at],
            send_sem=bit_send,
            recv_sem=bit_recv.at[2 if depth_in else side if arrival else 1 - side],
            device_id=(me - 1 + 2 * side,),
            device_id_type=MESH,
        )

    def bits_sent(planes):
        several = solid.at[pl.ds(0, planes)]
        pltpu.make_async_remote_copy(
            src_ref=several,
            dst_ref=several,
            send_sem=bit_send,
            recv_sem=bit_recv.at[0],
            device_id=(partner,),
            device_id_type=MESH,
        ).wait_send()

    def mask(plane, first, last):
        def tile(t, carry):
            at = pl.ds(pl.multiple_of(t * TILE, TILE), TILE)
            r0[plane, at, :] = jnp.where(flags[plane, at, :] == 1, rhs[plane, at, :], 0.0)
            return carry

        lax.fori_loop(first, last, tile, 0)

    def pack(plane):
        def one(j, found):
            at = pl.ds(pl.multiple_of(j * words, words), words)
            kinds = flags[plane, at, :]
            return tuple(
                word | jnp.left_shift(jnp.where(kinds == kind, 1, 0), j)
                for word, kind in zip(found, (2, 1))
            )

        empty = jnp.zeros((words, cols), jnp.int32)
        solid[plane + 2], fluid[plane] = lax.fori_loop(0, 32, one, (empty, empty))

    greeted = sum(len(group) for group in rounds) + near_size - 1 + (relief > 0)
    callers = 1 + has_far.astype(jnp.int32)
    kept = max(len(spans) - 2, 1)
    load(far_plane, 0).wait()
    pack(far_plane)

    @pl.when(is_even)
    def _():
        pl.semaphore_wait(barrier, callers)
        on(far_side, lambda: bit_copy(0).start())

    load(far_plane, 1).wait()
    mask(far_plane, 0, chunk // TILE)

    @pl.when(is_even)
    def _():
        far_pieces(0, 1, raw=True)

    for plane in [near_plane] + inner_planes:
        load(plane, 0).wait()
        pack(plane)

    @pl.when(is_even)
    def _():
        on(far_side, lambda: bit_copy(0, 1).start())

    @pl.when(is_odd)
    def _():
        pl.semaphore_wait(barrier, callers + greeted)
        on(far_side, lambda: bit_copy(1).start())
        if rounds:
            tell(0)

    bit_copy(near_side).start()
    mask(far_plane, chunk // TILE, steps)

    @pl.when(is_even)
    def _():
        far_pieces(1, kept, raw=True)

        @pl.when(jnp.logical_not(is_first))
        def _():
            far_pieces(kept, len(spans), raw=True)

    for plane in [near_plane] + inner_planes:
        load(plane, 1).wait()
        mask(plane, 0, steps)

    bit_copy(near_side, 0, True).wait_recv()
    on(far_side, lambda: bit_copy(far_side, 0, True).wait_recv())

    def classify(at, slot, known_fluid):
        word = solid[at]
        line = lax.broadcasted_iota(jnp.int32, (words, cols), 0)
        across = lax.broadcasted_iota(jnp.int32, (words, cols), 1)
        before, after = pltpu.roll(word, 1, 0), pltpu.roll(word, words - 1, 0)
        before = jnp.where(line == 0, jnp.left_shift(before, 1), before)
        after = jnp.where(line == words - 1, lax.shift_right_logical(after, 1), after)
        left = jnp.where(across == 0, 0, pltpu.roll(word, 1, 1))
        right = jnp.where(across == cols - 1, 0, pltpu.roll(word, cols - 1, 1))

        def add(a, b, c):
            return a ^ b ^ c, (a & b) | (c & (a ^ b))

        ones, twos = add(before, after, left)
        more_ones, more_twos = add(right, solid[at - 1], solid[at + 1])
        digits = [ones ^ more_ones, *add(twos, more_twos, ones & more_ones)]
        for i, digit in enumerate(digits):
            if known_fluid is not None:
                digit = digit | ~known_fluid
            code[slot, i] = digit

    def inverse(slot, j):
        bit = jnp.left_shift(1, j)
        ones, twos, fours = ((code[slot, i] & bit) != 0 for i in range(3))
        none, one, two, three, four, five, six, out = (
            jnp.float32(value) for value in (1 / 6, 1 / 5, 1 / 4, 1 / 3, 1 / 2, 1.0, 1.0, 0.0)
        )
        low = jnp.where(twos, jnp.where(ones, three, two), jnp.where(ones, one, none))
        high = jnp.where(twos, jnp.where(ones, out, six), jnp.where(ones, five, four))
        return jnp.where(fours, high, low)

    column = lax.broadcasted_iota(jnp.int32, (TILE, cols), 1)

    def inplane(ref, plane, start):
        block = ref[plane, pl.ds(start, TILE + 2 * PAD), :]
        centre = block[PAD:PAD + TILE]
        total = block[PAD - 1:PAD - 1 + TILE] + block[PAD + 1:PAD + 1 + TILE]
        total = total + jnp.where(column == 0, 0.0, pltpu.roll(centre, 1, 1))
        total = total + jnp.where(column == cols - 1, 0.0, pltpu.roll(centre, cols - 1, 1))
        return centre, total

    def centre_of(ref, plane, start):
        return ref[plane, pl.ds(pl.multiple_of(start + PAD, PAD), TILE), :]

    def put(ref, plane, start, value):
        ref[plane, pl.ds(pl.multiple_of(start + PAD, PAD), TILE), :] = value

    def fold(value):
        total = value[0:8]
        for i in range(8, value.shape[0], 8):
            total = total + value[i:i + 8]
        return total

    none = jnp.zeros((8, cols), jnp.float32)

    for plane in range(depth):
        classify(plane + 2, plane, fluid[plane])

    def first(j, moment):
        start = pl.multiple_of(j * words, words)
        at = pl.ds(start, words)
        padded = pl.ds(pl.multiple_of(start + PAD, PAD), words)
        for plane in range(depth):
            value = inverse(plane, j)
            inv[plane, at, :] = value
            residual = r0[plane, at, :]
            precond = residual * value
            u0[plane, padded, :] = precond
            moment = moment + fold(residual * precond)
        return moment

    moment0 = lax.fori_loop(0, 32, first, none)
    near_copy(0).start()

    @pl.when(jnp.logical_and(is_odd, is_first))
    def _():
        far_pieces(0, len(spans))

    @pl.when(is_even)
    def _():
        def plain(t, carry):
            at = pl.ds(pl.multiple_of(t * TILE, TILE), TILE)
            shadow[at, :] = jnp.ones((TILE, cols), jnp.float32)
            return carry

        lax.fori_loop(0, steps, plain, 0)

    @pl.when(is_odd)
    def _():
        on(far_side, lambda: bit_copy(1, 1, True).wait_recv())
        classify(depth + 2, depth, None)

        def beyond(j, carry):
            shadow[pl.ds(pl.multiple_of(j * words, words), words), :] = inverse(depth, j)
            return carry

        lax.fori_loop(0, 32, beyond, 0)
        if rounds:
            hear(0)

    def local_part(field, scaled, out, plane, start):
        at = pl.ds(start, TILE)
        _, total = inplane(field, plane, start)
        if plane > 0:
            total = total + centre_of(field, plane - 1, start)
        if plane < depth - 1:
            total = total + centre_of(field, plane + 1, start)
        image = jnp.where(inv[plane, at, :] > 0.0, scaled[plane, at, :] - total, 0.0)
        out[plane, at, :] = image
        return image

    def apply_once(plane, start, image, value, moments):
        precond = image * value
        put(u1, plane, start, precond)
        return (
            moments[0] + fold(image * centre_of(u0, plane, start)),
            moments[1] + fold(image * precond),
        )

    def second(t, moments):
        start = pl.multiple_of(t * TILE, TILE)
        for plane in range(depth):
            image = local_part(u0, r0, w0, plane, start)
            if 0 < plane < depth - 1:
                value = inv[plane, pl.ds(start, TILE), :]
                moments = apply_once(plane, start, image, value, moments)
        return moments

    moments = lax.fori_loop(0, steps, second, (none, none))

    def edge_one(side, span, moments):
        plane = side * (depth - 1)

        def tile(t, moments):
            start = pl.multiple_of(span[0] + t * TILE, TILE)
            at = pl.ds(start, TILE)
            value = inv[plane, at, :]
            beyond = halo_r[side, at, :]
            if side is far_side:
                beyond = beyond * shadow[at, :]
            image = jnp.where(value > 0.0, w0[plane, at, :] - beyond, 0.0)
            w0[plane, at, :] = image
            return apply_once(plane, start, image, value, moments)

        return lax.fori_loop(0, span[1] // TILE, tile, moments)

    passing = digit == near_size - 1
    @pl.when(is_odd)
    def _():
        for which in range(1, len(rounds)):
            hear(which)

    @pl.when(jnp.logical_and(is_even, is_first))
    def _():
        far_pieces(kept, len(spans), raw=True)

    @pl.when(jnp.logical_not(is_first))
    def _():
        @pl.when(is_even)
        def _():
            far_sent(0)
            pl.semaphore_signal(go, inc=1, device_id=(partner,), device_id_type=MESH)

        @pl.when(is_odd)
        def _():
            pl.semaphore_wait(go, 1)

            @pl.when(jnp.logical_and(passing, chip >= near_size))
            def _():
                pl.semaphore_signal(
                    clear, inc=1, device_id=(me - 2 * near_size,), device_id_type=MESH
                )

            @pl.when(jnp.logical_and(passing, chip + near_size < count // 2))
            def _():
                pl.semaphore_wait(clear, 1)

            far_pieces(0, len(spans))

    near_arrival(0).wait_recv()
    moments = edge_one(near_side, (0, rows), moments)
    near_copy(1).start()
    for i, span in enumerate(spans):
        on(far_side, lambda: halo_arrival(0, far_side, span, far_recv.at[0, i]).wait_recv())
        moments = edge_one(far_side, span, moments)

        @pl.when(is_odd)
        def _():
            far_pieces(i, i + 1, 1)

    moment1, moment2 = moments

    def third(t, moment):
        start = pl.multiple_of(t * TILE, TILE)
        for plane in range(depth):
            image = local_part(u1, w0, w1, plane, start)
            moment = moment + fold(image * centre_of(u1, plane, start))
        return moment

    moment3 = lax.fori_loop(0, steps, third, none)

    def edge_two(side, span, moment, weight):
        plane = side * (depth - 1)

        def tile(t, moment):
            start = pl.multiple_of(span[0] + t * TILE, TILE)
            at = pl.ds(start, TILE)
            beyond = halo_u[side, at, :]
            image = jnp.where(inv[plane, at, :] > 0.0, w1[plane, at, :] - beyond, 0.0)
            w1[plane, at, :] = image
            return moment - weight * fold(beyond * centre_of(u1, plane, start))

        return lax.fori_loop(0, span[1] // TILE, tile, moment)

    def lanes(value):
        total = value[:, 0:128]
        for i in range(128, cols, 128):
            total = total + value[:, i:i + 128]
        return jnp.sum(total, axis=0, keepdims=True)

    for i, value in enumerate((moment0, moment1, moment2)):
        mine[0, i:i + 1, :] = lanes(value)
    mine[0, 3:8, :] = jnp.zeros((5, 128), jnp.float32)
    near_arrival(1).wait_recv()
    moment3 = edge_two(near_side, (0, rows), moment3, 1.0)

    def pair_copy():
        return pltpu.make_async_remote_copy(
            src_ref=mine.at[0], dst_ref=pair, send_sem=pair_send, recv_sem=pair_recv,
            device_id=(partner,), device_id_type=MESH,
        )

    def sum_copy(stage, j, core, shift=0):
        slot, other = peer(stage, j)
        return pltpu.make_async_remote_copy(
            src_ref=mine.at[stage],
            dst_ref=got.at[stage, slot],
            send_sem=sum_send.at[0 if stage == 0 or j == 0 else 2 if shift else 1],
            recv_sem=sum_recv.at[stage],
            device_id=(2 * (other - shift) + core,),
            device_id_type=MESH,
        )

    def sums(stage, copies, sender=0):
        several = got.at[stage, pl.ds(0, copies)]
        return pltpu.make_async_remote_copy(
            src_ref=several,
            dst_ref=several,
            send_sem=sum_send.at[sender],
            recv_sem=sum_recv.at[stage],
            device_id=(partner,),
            device_id_type=MESH,
        )

    def across():
        sum_copy(1, 0, 0).start()

        def to_all(shift):
            for j in range(1, far_size):
                for core in (1, 0):
                    sum_copy(1, j, core, shift).start()

        if relief:
            pl.when(is_relief)(lambda: to_all(relief))
            pl.when(jnp.logical_not(is_first))(lambda: to_all(0))
        else:
            to_all(0)

    def across_sent():
        sums(0, 1).wait_send()
        if far_size > 1:
            pl.when(jnp.logical_not(is_first) if relief else True)(
                lambda: sums(0, 2 * (far_size - 1), 1).wait_send()
            )
            if relief:
                pl.when(is_relief)(lambda: sums(0, 2 * (far_size - 1), 2).wait_send())

    def gathered(stage):
        total = got[stage, 0]
        for i in range(1, stages[stage][0]):
            total = total + got[stage, i]
        return total

    @pl.when(is_even)
    def _():
        pair_copy().wait_recv()
        mine[0] = mine[0] + pair[...]
        moment = moment3
        for i, span in enumerate(spans):
            on(far_side, lambda: halo_arrival(1, far_side, span, far_recv.at[1, i]).wait_recv())
            for place, after in ((is_first, 4), (jnp.logical_not(is_first), 3)):
                if i == max(len(spans) - after, 0):
                    @pl.when(place)
                    def _():
                        @pl.when(jnp.logical_or(jnp.logical_not(is_first), chip >= near_size))
                        def _():
                            pl.semaphore_wait(go, 1)

                        on(far_side, lambda: late_copy(0).start())

                        @pl.when(jnp.logical_and(is_first, has_far))
                        def _():
                            late_copy(1).start()

            moment = edge_two(far_side, span, moment, 2.0)

        mine[0, 3:4, :] = mine[0, 3:4, :] + lanes(moment)
        for j in range(near_size):
            sum_copy(0, j, 1).start()

        @pl.when(has_far)
        def _():
            pl.when(jnp.logical_not(is_first))(lambda: late_copy(1).start())
            late_copy(2).start()
            for i in range(3, len(lates)):
                late_copy(i - 3).wait_send()
                late_copy(i).start()

    @pl.when(is_odd)
    def _():
        mine[0, 3:4, :] = lanes(moment3)
        pair_copy().start()
        far_sent(1)

        @pl.when(jnp.logical_or(jnp.logical_not(is_first), chip + near_size < count // 2))
        def _():
            waiting = jnp.where(is_first, me - 1 + 2 * near_size, partner)
            pl.semaphore_signal(go, inc=1, device_id=(waiting,), device_id_type=MESH)

        sums(0, near_size).wait_recv()
        total = gathered(0)
        mine[1] = total
        across()
        got[1, peer(1, 0)[0]] = total

    near_copy(0).wait_send()
    near_copy(1).wait_send()
    far_ended(0)

    @pl.when(is_even)
    def _():
        pl.when(has_far)(lambda: bits_sent(3))
        pl.when(jnp.logical_not(has_far))(lambda: bits_sent(1))
        pl.when(is_first)(lambda: far_sent(0))
        sums(0, near_size).wait_send()
        sums(1, far_size).wait_recv()

    @pl.when(is_odd)
    def _():
        pl.when(has_far)(lambda: bits_sent(2))
        pl.when(jnp.logical_not(has_far))(lambda: bits_sent(1))
        far_sent(0)
        far_ended(1)
        pair_copy().wait_send()
        across_sent()
        if far_size > 1:
            sums(1, far_size - 1).wait_recv()

    everyone = gathered(1)
    s0, s1, s2, s3 = (everyone[i:i + 1] for i in range(4))

    def whole(value):
        return jnp.sum(value, axis=1, keepdims=True)

    rz_old = whole(s0)
    step_old = rz_old / whole(s1)
    rz_now = whole(s0 - 2.0 * step_old * s1 + step_old * step_old * s2)
    grown = 1.0 + rz_now / rz_old
    product = whole(grown * grown * s1 - 2.0 * step_old * grown * s2 + step_old * step_old * s3)
    step_size = rz_now / product
    lead = step_old + step_size * grown
    trail = step_size * step_old

    for plane in range(depth):
        def last(t, carry, plane=plane):
            at = pl.ds(pl.multiple_of(t * final, final), final)
            base = r0[plane, at, :]
            along = w0[plane, at, :]
            sol_ref[plane, at, :] = inv[plane, at, :] * (lead * base - trail * along)
            res_ref[plane, at, :] = base - lead * along + trail * w1[plane, at, :]
            return carry

        lax.fori_loop(0, rows // final, last, 0)

    @pl.when(jnp.logical_and(is_odd, has_far))
    def _():
        plane = depth - 1

        for i, span in enumerate(lates):
            halo_arrival(1, 1, span, far_recv.at[1, i]).wait_recv()

            def tile(t, carry, span=span):
                at = pl.ds(pl.multiple_of(span[0] + t * TILE, TILE), TILE)
                beyond = jnp.where(inv[plane, at, :] > 0.0, halo_u[1, at, :], 0.0)
                res_ref[plane, at, :] = res_ref[plane, at, :] - trail * beyond
                return carry

            lax.fori_loop(0, span[1] // TILE, tile, 0)

    @pl.when(jnp.logical_and(is_even, has_far))
    def _():
        for i in range(len(lates) - 3, len(lates)):
            late_copy(i).wait_send()


def store(sol_ref, res_ref, sol_out, res_out, sem):
    copies = []
    for which, (source, target) in enumerate(((sol_ref, sol_out), (res_ref, res_out))):
        for plane in range(sol_ref.shape[0]):
            copies.append(
                pltpu.make_async_copy(source.at[plane], target.at[plane], sem.at[which, plane])
            )
    for copy in copies:
        copy.start()
    for copy in copies:
        copy.wait()


def groups(chips):
    near = math.gcd(chips, 4)
    return (near, 1), (chips // near, near)


def body(count, right_side, cell_flags):
    depth, rows, cols = right_side.shape
    assert count % 2 == 0 and depth > 1
    stages = groups(count // 2)
    widest = max(stages[0][0], stages[1][0], 2 * (stages[1][0] - 1))
    chunk = math.gcd(rows, CHUNK)
    assert rows % (8 * TILE) == 0
    pieces = max(len({0, 1, *(max(rows // chunk - i, 0) for i in range(4))}), len(LATE)) - 1
    f32 = jnp.float32
    field = pltpu.VMEM((depth, rows, cols), f32)
    padded = pltpu.VMEM((depth, rows + 2 * PAD, cols), f32)
    dma = pltpu.SemaphoreType.DMA
    grant = VMEM_BYTES - 8 * right_side.size - 2**19
    fields = pl.pallas_call(
        functools.partial(kernel, count, chunk, stages),
        out_shape=(field, field),
        in_specs=[pl.BlockSpec(memory_space=pltpu.HBM)] * 2,
        out_specs=(pl.BlockSpec(memory_space=pltpu.VMEM),) * 2,
        scratch_shapes=[
            field,
            pltpu.VMEM((depth, rows, cols), jnp.int32),
            field, field,
            pltpu.VMEM((rows, cols), f32),
            padded, padded, field, field,
            pltpu.VMEM((2, rows, cols), f32),
            pltpu.VMEM((2, rows, cols), f32),
            pltpu.VMEM((depth + 4, rows // 32, cols), jnp.int32),
            pltpu.VMEM((depth, rows // 32, cols), jnp.int32),
            pltpu.VMEM((depth + 1, 3, rows // 32, cols), jnp.int32),
            pltpu.VMEM((8, 128), f32),
            pltpu.VMEM((2, 8, 128), f32),
            pltpu.VMEM((2, widest, 8, 128), f32),
            dma((2, depth)),
            pltpu.SemaphoreType.REGULAR,
            pltpu.SemaphoreType.REGULAR,
            pltpu.SemaphoreType.REGULAR((max((stages[1][0] - 1).bit_length(), 1),)),
            dma, dma((3,)),
            dma((1 + len(LATE),)), dma((2, pieces)), dma((2,)), dma((2,)),
            dma, dma,
            dma((3,)), dma((2,)),
        ],
        compiler_params=pltpu.CompilerParams(
            collective_id=0, has_side_effects=True, vmem_limit_bytes=grant
        ),
    )(right_side, cell_flags)
    result = jax.ShapeDtypeStruct((depth, rows, cols), f32)
    return pl.pallas_call(
        store,
        out_shape=(result, result),
        in_specs=[pl.BlockSpec(memory_space=pltpu.VMEM)] * 2,
        out_specs=(pl.BlockSpec(memory_space=pltpu.HBM),) * 2,
        scratch_shapes=[dma((2, depth))],
        compiler_params=pltpu.CompilerParams(vmem_limit_bytes=2**19),
    )(*fields)


def solution(mesh):
    placed = (P("gz", None, None), P("gz", None, None))
    return jax.shard_map(
        functools.partial(body, mesh.shape["gz"]),
        mesh=mesh,
        in_specs=placed,
        out_specs=placed,
        check_vma=False,
    )
```

```python
import functools
import math

import jax
import jax.numpy as jnp
from jax import lax
from jax.experimental import pallas as pl
from jax.experimental.pallas import tpu as pltpu
from jax.sharding import PartitionSpec as P

MESH = pl.DeviceIdType.MESH
TILE = 16
LAST = 64
LATE = (0, 2, 3, 5, 7, 8)
CHUNK = 64
PAD = 8
VMEM_BYTES = 67_043_328


def kernel(
    count, chunk, stages,
    side_hbm, flag_hbm, sol_ref, res_ref,
    rhs, flags, r0, inv, shadow, u0, u1, w0, w1, halo_r, halo_u, solid, halves, fluid, code,
    pair, mine, got,
    in_sem, go, clear, known, bit_send, bit_recv, far_send, far_recv, near_send, near_recv,
    pair_send, pair_recv, sum_send, sum_recv,
):
    depth, rows, cols = rhs.shape
    words = rows // 32
    steps = rows // TILE
    parts = rows // chunk
    marks = sorted({0, 1, parts // 2, max(parts - 2, 0), max(parts - 1, 0), parts})
    plain = marks.index(parts // 2)
    half = words // 2
    spans = [(a * chunk, (b - a) * chunk) for a, b in zip(marks, marks[1:])]
    most = (0, rows - spans[-1][1])
    late_marks = [rows * eighth // 8 for eighth in LATE]
    lates = [(a, b - a) for a, b in zip(late_marks, late_marks[1:])]
    final = math.gcd(rows, LAST)
    near_size, far_size = stages[0][0], stages[1][0]
    me = lax.axis_index("gz")
    chip, odd = me // 2, lax.rem(me, 2)
    is_even, is_odd = odd == 0, odd == 1
    near_side, far_side = 1 - odd, odd
    near_plane, far_plane = near_side * (depth - 1), far_side * (depth - 1)
    partner = me + 1 - 2 * odd
    has_far = jnp.where(is_even, me > 0, me < count - 1)

    digit = lax.rem(chip, near_size)
    relief = near_size // 2 if near_size > 2 else 0
    is_first, is_relief = digit == 0, digit == relief

    def load(plane, which):
        source, target = ((flag_hbm, flags), (side_hbm, rhs))[which]
        return pltpu.make_async_copy(source.at[plane], target.at[plane], in_sem.at[which, plane])

    def peer(stage, j):
        size, stride = stages[stage]
        digit = lax.rem(chip // stride, size)
        return digit, chip + (lax.rem(digit + j, size) - digit) * stride

    barrier = pltpu.get_barrier_semaphore()

    def greet(other):
        pl.semaphore_signal(barrier, inc=1, device_id=(other,), device_id_type=MESH)

    @pl.when(has_far)
    def _():
        greet(me - 1 + 2 * odd)

    greet(partner)
    inner_planes = list(range(1, depth - 1))
    load(far_plane, 0).start()
    load(far_plane, 1).start()
    for plane in [near_plane] + inner_planes:
        load(plane, 0).start()
    for plane in [near_plane] + inner_planes:
        load(plane, 1).start()
    pairs = far_size & (far_size - 1) == 0
    if pairs:
        rounds = [(far_size >> i,) for i in range(1, far_size.bit_length())]
    else:
        rounds = [tuple(range(1, far_size))]

    def far_peer(distance):
        digit = chip // near_size
        if pairs:
            step = distance * (1 - 2 * lax.rem(digit // distance, 2))
        else:
            step = lax.rem(digit + distance, far_size) - digit
        return 2 * (chip + step * near_size) + 1

    if relief:
        @pl.when(is_even)
        def _():
            greet(2 * (chip - digit + lax.rem(digit + relief, near_size)) + 1)

    @pl.when(is_odd)
    def _():
        for group in rounds:
            for distance in group:
                greet(far_peer(distance))
        for j in range(1, near_size):
            greet(2 * peer(0, j)[1] + 1)

    def tell(which):
        for distance in rounds[which]:
            pl.semaphore_signal(
                known.at[which], inc=1, device_id=(far_peer(distance),), device_id_type=MESH
            )

    def hear(which):
        pl.semaphore_wait(known.at[which], len(rounds[which]))
        if which + 1 < len(rounds):
            tell(which + 1)

    blank = jnp.zeros((PAD, cols), jnp.float32)
    for ref in (u0, u1):
        for plane in range(ref.shape[0]):
            ref[plane, 0:PAD, :] = blank
            ref[plane, rows + PAD:rows + 2 * PAD, :] = blank

    @pl.when(jnp.logical_not(has_far))
    def _():
        solid[far_side * (depth + 2)] = jnp.zeros((words, cols), jnp.int32)
        solid[far_side * (depth + 2) + 1] = jnp.zeros((words, cols), jnp.int32)
        halves[1] = jnp.zeros((half, cols), jnp.int32)

        def clear(t, carry):
            at = pl.ds(pl.multiple_of(t * TILE, TILE), TILE)
            halo_r[far_side, at, :] = jnp.zeros((TILE, cols), jnp.float32)
            halo_u[far_side, at, :] = jnp.zeros((TILE, cols), jnp.float32)
            return carry

        lax.fori_loop(0, steps, clear, 0)

    def on(side, there):
        if side is far_side:
            pl.when(has_far)(there)
        else:
            there()

    def halo_copy(phase, side, span, send, recv, raw=False):
        start, size = span
        plane = side * (depth - 1)
        if raw:
            source = r0.at[plane, pl.ds(start, size)]
        else:
            source = (u0, u1)[phase].at[plane, pl.ds(start + PAD, size)]
        return pltpu.make_async_remote_copy(
            src_ref=source,
            dst_ref=(halo_r, halo_u)[phase].at[1 - side, pl.ds(start, size)],
            send_sem=send,
            recv_sem=recv,
            device_id=(me - 1 + 2 * side,),
            device_id_type=MESH,
        )

    def halo_arrival(phase, side, span, recv):
        start, size = span
        target = (halo_r, halo_u)[phase].at[side, pl.ds(start, size)]
        return pltpu.make_async_remote_copy(
            src_ref=target,
            dst_ref=target,
            send_sem=near_send.at[phase],
            recv_sem=recv,
            device_id=(me - 1 + 2 * side,),
            device_id_type=MESH,
        )

    def far_copy(phase, i, raw=False):
        send = far_send.at[2 * phase + (i == len(spans) - 1)]
        return halo_copy(phase, far_side, spans[i], send, far_recv.at[phase, i], raw)

    def far_sent(phase):
        sender = far_send.at[2 * phase]
        on(far_side, lambda: halo_copy(
            phase, far_side, most, sender, far_recv.at[phase, 0]
        ).wait_send())

    def far_ended(phase):
        on(far_side, lambda: far_copy(phase, len(spans) - 1).wait_send())

    def late_copy(i):
        return halo_copy(1, far_side, lates[i], far_send.at[2 + i], far_recv.at[1, i])

    def near_copy(phase):
        return halo_copy(
            phase, near_side, (0, rows), near_send.at[phase], near_recv.at[phase]
        )

    def near_arrival(phase):
        return halo_arrival(phase, near_side, (0, rows), near_recv.at[phase])

    def far_pieces(first, last, phase=0, raw=False):
        def some():
            for i in range(first, last):
                far_copy(phase, i, raw).start()

        on(far_side, some)

    def bit_copy(side, arrival=False):
        halo_at = 1 + side * (depth + 1)
        source = halo_at if arrival else 2 + side * (depth - 1)
        target = halo_at if arrival else 1 + (1 - side) * (depth + 1)
        return pltpu.make_async_remote_copy(
            src_ref=solid.at[source],
            dst_ref=solid.at[target],
            send_sem=bit_send.at[0],
            recv_sem=bit_recv.at[side if arrival else 1 - side],
            device_id=(me - 1 + 2 * side,),
            device_id_type=MESH,
        )

    def half_copy(arrival=False):
        return pltpu.make_async_remote_copy(
            src_ref=halves.at[1 if arrival else 0],
            dst_ref=halves.at[1],
            send_sem=bit_send.at[1],
            recv_sem=bit_recv.at[2],
            device_id=(me - 1 + 2 * far_side,),
            device_id_type=MESH,
        )

    def bits_sent(planes):
        several = solid.at[pl.ds(0, planes)]
        pltpu.make_async_remote_copy(
            src_ref=several,
            dst_ref=several,
            send_sem=bit_send.at[0],
            recv_sem=bit_recv.at[0],
            device_id=(partner,),
            device_id_type=MESH,
        ).wait_send()

    def mask(plane, first, last):
        def tile(t, carry):
            at = pl.ds(pl.multiple_of(t * TILE, TILE), TILE)
            r0[plane, at, :] = jnp.where(flags[plane, at, :] == 1, rhs[plane, at, :], 0.0)
            return carry

        lax.fori_loop(first, last, tile, 0)

    def pack(plane):
        def one(j, found):
            at = pl.ds(pl.multiple_of(j * words, words), words)
            kinds = flags[plane, at, :]
            return tuple(
                word | jnp.left_shift(jnp.where(kinds == kind, 1, 0), j)
                for word, kind in zip(found, (2, 1))
            )

        empty = jnp.zeros((words, cols), jnp.int32)
        solid[plane + 2], fluid[plane] = lax.fori_loop(0, 32, one, (empty, empty))

    greeted = sum(len(group) for group in rounds) + near_size - 1 + (relief > 0)
    callers = 1 + has_far.astype(jnp.int32)
    kept = max(len(spans) - 2, 1)
    load(far_plane, 0).wait()
    pack(far_plane)

    @pl.when(is_even)
    def _():
        pl.semaphore_wait(barrier, callers)
        on(far_side, lambda: bit_copy(0).start())

    load(far_plane, 1).wait()
    mask(far_plane, 0, chunk // TILE)

    @pl.when(is_even)
    def _():
        far_pieces(0, 1, raw=True)

    for plane in [near_plane] + inner_planes:
        load(plane, 0).wait()
        pack(plane)

    @pl.when(is_even)
    def _():
        low, high = solid[3, 0:half, :], solid[3, half:words, :]
        halves[0] = jnp.bitwise_and(low, 0xFFFF) | jnp.left_shift(high, 16)
        on(far_side, lambda: half_copy().start())

    @pl.when(is_odd)
    def _():
        pl.semaphore_wait(barrier, callers + greeted)
        on(far_side, lambda: bit_copy(1).start())
        if rounds:
            tell(0)

    bit_copy(near_side).start()
    mask(far_plane, chunk // TILE, steps)

    @pl.when(is_even)
    def _():
        far_pieces(1, plain, raw=True)

    for plane in [near_plane] + inner_planes:
        load(plane, 1).wait()
        mask(plane, 0, steps)

    bit_copy(near_side, True).wait_recv()
    on(far_side, lambda: bit_copy(far_side, True).wait_recv())

    def classify(at, slot, known_fluid):
        word = solid[at]
        line = lax.broadcasted_iota(jnp.int32, (words, cols), 0)
        across = lax.broadcasted_iota(jnp.int32, (words, cols), 1)
        before, after = pltpu.roll(word, 1, 0), pltpu.roll(word, words - 1, 0)
        before = jnp.where(line == 0, jnp.left_shift(before, 1), before)
        after = jnp.where(line == words - 1, lax.shift_right_logical(after, 1), after)
        left = jnp.where(across == 0, 0, pltpu.roll(word, 1, 1))
        right = jnp.where(across == cols - 1, 0, pltpu.roll(word, cols - 1, 1))

        def add(a, b, c):
            return a ^ b ^ c, (a & b) | (c & (a ^ b))

        ones, twos = add(before, after, left)
        more_ones, more_twos = add(right, solid[at - 1], solid[at + 1])
        digits = [ones ^ more_ones, *add(twos, more_twos, ones & more_ones)]
        for i, digit in enumerate(digits):
            if known_fluid is not None:
                digit = digit | ~known_fluid
            code[slot, i] = digit

    def inverse(slot, j):
        bit = jnp.left_shift(1, j)
        ones, twos, fours = ((code[slot, i] & bit) != 0 for i in range(3))
        none, one, two, three, four, five, six, out = (
            jnp.float32(value) for value in (1 / 6, 1 / 5, 1 / 4, 1 / 3, 1 / 2, 1.0, 1.0, 0.0)
        )
        low = jnp.where(twos, jnp.where(ones, three, two), jnp.where(ones, one, none))
        high = jnp.where(twos, jnp.where(ones, out, six), jnp.where(ones, five, four))
        return jnp.where(fours, high, low)

    column = lax.broadcasted_iota(jnp.int32, (TILE, cols), 1)

    def inplane(ref, plane, start):
        block = ref[plane, pl.ds(start, TILE + 2 * PAD), :]
        centre = block[PAD:PAD + TILE]
        total = block[PAD - 1:PAD - 1 + TILE] + block[PAD + 1:PAD + 1 + TILE]
        total = total + jnp.where(column == 0, 0.0, pltpu.roll(centre, 1, 1))
        total = total + jnp.where(column == cols - 1, 0.0, pltpu.roll(centre, cols - 1, 1))
        return centre, total

    def centre_of(ref, plane, start):
        return ref[plane, pl.ds(pl.multiple_of(start + PAD, PAD), TILE), :]

    def put(ref, plane, start, value):
        ref[plane, pl.ds(pl.multiple_of(start + PAD, PAD), TILE), :] = value

    def fold(value):
        total = value[0:8]
        for i in range(8, value.shape[0], 8):
            total = total + value[i:i + 8]
        return total

    none = jnp.zeros((8, cols), jnp.float32)

    for plane in range(depth):
        classify(plane + 2, plane, fluid[plane])

    def first(j, moment):
        start = pl.multiple_of(j * words, words)
        at = pl.ds(start, words)
        padded = pl.ds(pl.multiple_of(start + PAD, PAD), words)
        for plane in range(depth):
            value = inverse(plane, j)
            inv[plane, at, :] = value
            residual = r0[plane, at, :]
            precond = residual * value
            u0[plane, padded, :] = precond
            moment = moment + fold(residual * precond)
        return moment

    moment0 = lax.fori_loop(0, 32, first, none)
    near_copy(0).start()

    @pl.when(is_even)
    def _():
        far_pieces(plain, kept)

        @pl.when(jnp.logical_not(is_first))
        def _():
            far_pieces(kept, len(spans))

    @pl.when(jnp.logical_and(is_odd, is_first))
    def _():
        far_pieces(0, len(spans))

    def known_scale(t, carry):
        at = pl.ds(pl.multiple_of(t * TILE, TILE), TILE)
        shadow[at, :] = jnp.ones((TILE, cols), jnp.float32)
        return carry

    lax.fori_loop(odd * (steps // 2), steps, known_scale, 0)

    @pl.when(is_odd)
    def _():
        on(far_side, lambda: half_copy(True).wait_recv())
        solid[depth + 3, 0:half, :] = jnp.bitwise_and(halves[1], 0xFFFF)
        solid[depth + 3, half:words, :] = lax.shift_right_logical(halves[1], 16)
        classify(depth + 2, depth, None)

        def beyond(j, carry):
            shadow[pl.ds(pl.multiple_of(j * words, words), words), :] = inverse(depth, j)
            return carry

        lax.fori_loop(0, 16, beyond, 0)
        if rounds:
            hear(0)

    def local_part(field, scaled, out, plane, start):
        at = pl.ds(start, TILE)
        _, total = inplane(field, plane, start)
        if plane > 0:
            total = total + centre_of(field, plane - 1, start)
        if plane < depth - 1:
            total = total + centre_of(field, plane + 1, start)
        image = jnp.where(inv[plane, at, :] > 0.0, scaled[plane, at, :] - total, 0.0)
        out[plane, at, :] = image
        return image

    def apply_once(plane, start, image, value, moments):
        precond = image * value
        put(u1, plane, start, precond)
        return (
            moments[0] + fold(image * centre_of(u0, plane, start)),
            moments[1] + fold(image * precond),
        )

    def second(t, moments):
        start = pl.multiple_of(t * TILE, TILE)
        for plane in range(depth):
            image = local_part(u0, r0, w0, plane, start)
            if 0 < plane < depth - 1:
                value = inv[plane, pl.ds(start, TILE), :]
                moments = apply_once(plane, start, image, value, moments)
        return moments

    moments = lax.fori_loop(0, steps, second, (none, none))

    def edge_one(side, span, moments):
        plane = side * (depth - 1)

        def tile(t, moments):
            start = pl.multiple_of(span[0] + t * TILE, TILE)
            at = pl.ds(start, TILE)
            value = inv[plane, at, :]
            beyond = halo_r[side, at, :]
            if side is far_side:
                beyond = beyond * shadow[at, :]
            image = jnp.where(value > 0.0, w0[plane, at, :] - beyond, 0.0)
            w0[plane, at, :] = image
            return apply_once(plane, start, image, value, moments)

        return lax.fori_loop(0, span[1] // TILE, tile, moments)

    passing = digit == near_size - 1
    @pl.when(is_odd)
    def _():
        for which in range(1, len(rounds)):
            hear(which)

    @pl.when(jnp.logical_and(is_even, is_first))
    def _():
        far_pieces(kept, len(spans))

    @pl.when(jnp.logical_not(is_first))
    def _():
        @pl.when(is_even)
        def _():
            far_sent(0)
            pl.semaphore_signal(go, inc=1, device_id=(partner,), device_id_type=MESH)

        @pl.when(is_odd)
        def _():
            pl.semaphore_wait(go, 1)

            @pl.when(jnp.logical_and(passing, chip >= near_size))
            def _():
                pl.semaphore_signal(
                    clear, inc=1, device_id=(me - 2 * near_size,), device_id_type=MESH
                )

            @pl.when(jnp.logical_and(passing, chip + near_size < count // 2))
            def _():
                pl.semaphore_wait(clear, 1)

            far_pieces(0, len(spans))

    near_arrival(0).wait_recv()
    moments = edge_one(near_side, (0, rows), moments)
    near_copy(1).start()
    for i, span in enumerate(spans):
        on(far_side, lambda: halo_arrival(0, far_side, span, far_recv.at[0, i]).wait_recv())
        moments = edge_one(far_side, span, moments)

        @pl.when(is_odd)
        def _():
            far_pieces(i, i + 1, 1)

    moment1, moment2 = moments

    def third(t, moment):
        start = pl.multiple_of(t * TILE, TILE)
        for plane in range(depth):
            image = local_part(u1, w0, w1, plane, start)
            moment = moment + fold(image * centre_of(u1, plane, start))
        return moment

    moment3 = lax.fori_loop(0, steps, third, none)

    def edge_two(side, span, moment, weight):
        plane = side * (depth - 1)

        def tile(t, moment):
            start = pl.multiple_of(span[0] + t * TILE, TILE)
            at = pl.ds(start, TILE)
            beyond = halo_u[side, at, :]
            image = jnp.where(inv[plane, at, :] > 0.0, w1[plane, at, :] - beyond, 0.0)
            w1[plane, at, :] = image
            return moment - weight * fold(beyond * centre_of(u1, plane, start))

        return lax.fori_loop(0, span[1] // TILE, tile, moment)

    def lanes(value):
        total = value[:, 0:128]
        for i in range(128, cols, 128):
            total = total + value[:, i:i + 128]
        return jnp.sum(total, axis=0, keepdims=True)

    for i, value in enumerate((moment0, moment1, moment2)):
        mine[0, i:i + 1, :] = lanes(value)
    mine[0, 3:8, :] = jnp.zeros((5, 128), jnp.float32)
    near_arrival(1).wait_recv()
    moment3 = edge_two(near_side, (0, rows), moment3, 1.0)

    def pair_copy():
        return pltpu.make_async_remote_copy(
            src_ref=mine.at[0], dst_ref=pair, send_sem=pair_send, recv_sem=pair_recv,
            device_id=(partner,), device_id_type=MESH,
        )

    def sum_copy(stage, j, core, shift=0):
        slot, other = peer(stage, j)
        return pltpu.make_async_remote_copy(
            src_ref=mine.at[stage],
            dst_ref=got.at[stage, slot],
            send_sem=sum_send.at[0 if stage == 0 or j == 0 else 2 if shift else 1],
            recv_sem=sum_recv.at[stage],
            device_id=(2 * (other - shift) + core,),
            device_id_type=MESH,
        )

    def sums(stage, copies, sender=0):
        several = got.at[stage, pl.ds(0, copies)]
        return pltpu.make_async_remote_copy(
            src_ref=several,
            dst_ref=several,
            send_sem=sum_send.at[sender],
            recv_sem=sum_recv.at[stage],
            device_id=(partner,),
            device_id_type=MESH,
        )

    def across():
        sum_copy(1, 0, 0).start()

        def to_all(shift):
            for j in range(1, far_size):
                for core in (1, 0):
                    sum_copy(1, j, core, shift).start()

        if relief:
            pl.when(is_relief)(lambda: to_all(relief))
            pl.when(jnp.logical_not(is_first))(lambda: to_all(0))
        else:
            to_all(0)

    def across_sent():
        sums(0, 1).wait_send()
        if far_size > 1:
            pl.when(jnp.logical_not(is_first) if relief else True)(
                lambda: sums(0, 2 * (far_size - 1), 1).wait_send()
            )
            if relief:
                pl.when(is_relief)(lambda: sums(0, 2 * (far_size - 1), 2).wait_send())

    def gathered(stage):
        total = got[stage, 0]
        for i in range(1, stages[stage][0]):
            total = total + got[stage, i]
        return total

    @pl.when(is_even)
    def _():
        pair_copy().wait_recv()
        mine[0] = mine[0] + pair[...]
        moment = moment3
        for i, span in enumerate(spans):
            on(far_side, lambda: halo_arrival(1, far_side, span, far_recv.at[1, i]).wait_recv())
            for place, after in ((is_first, 4), (jnp.logical_not(is_first), 3)):
                if i == max(len(spans) - after, 0):
                    @pl.when(place)
                    def _():
                        @pl.when(jnp.logical_or(jnp.logical_not(is_first), chip >= near_size))
                        def _():
                            pl.semaphore_wait(go, 1)

                        on(far_side, lambda: late_copy(0).start())

                        @pl.when(jnp.logical_and(is_first, has_far))
                        def _():
                            late_copy(1).start()

            moment = edge_two(far_side, span, moment, 2.0)

        mine[0, 3:4, :] = mine[0, 3:4, :] + lanes(moment)
        for j in range(near_size):
            sum_copy(0, j, 1).start()

        @pl.when(has_far)
        def _():
            pl.when(jnp.logical_not(is_first))(lambda: late_copy(1).start())
            late_copy(2).start()
            for i in range(3, len(lates)):
                late_copy(i - 3).wait_send()
                late_copy(i).start()

    @pl.when(is_odd)
    def _():
        mine[0, 3:4, :] = lanes(moment3)
        pair_copy().start()
        far_sent(1)

        @pl.when(jnp.logical_or(jnp.logical_not(is_first), chip + near_size < count // 2))
        def _():
            waiting = jnp.where(is_first, me - 1 + 2 * near_size, partner)
            pl.semaphore_signal(go, inc=1, device_id=(waiting,), device_id_type=MESH)

        sums(0, near_size).wait_recv()
        total = gathered(0)
        mine[1] = total
        across()
        got[1, peer(1, 0)[0]] = total

    near_copy(0).wait_send()
    near_copy(1).wait_send()
    far_ended(0)

    @pl.when(is_even)
    def _():
        pl.when(has_far)(lambda: bits_sent(2))
        pl.when(jnp.logical_not(has_far))(lambda: bits_sent(1))
        on(far_side, lambda: half_copy().wait_send())
        pl.when(is_first)(lambda: far_sent(0))
        sums(0, near_size).wait_send()
        sums(1, far_size).wait_recv()

    @pl.when(is_odd)
    def _():
        pl.when(has_far)(lambda: bits_sent(2))
        pl.when(jnp.logical_not(has_far))(lambda: bits_sent(1))
        far_sent(0)
        far_ended(1)
        pair_copy().wait_send()
        across_sent()
        if far_size > 1:
            sums(1, far_size - 1).wait_recv()

    everyone = gathered(1)
    s0, s1, s2, s3 = (everyone[i:i + 1] for i in range(4))

    def whole(value):
        return jnp.sum(value, axis=1, keepdims=True)

    rz_old = whole(s0)
    step_old = rz_old / whole(s1)
    rz_now = whole(s0 - 2.0 * step_old * s1 + step_old * step_old * s2)
    grown = 1.0 + rz_now / rz_old
    product = whole(grown * grown * s1 - 2.0 * step_old * grown * s2 + step_old * step_old * s3)
    step_size = rz_now / product
    lead = step_old + step_size * grown
    trail = step_size * step_old

    for plane in range(depth):
        def last(t, carry, plane=plane):
            at = pl.ds(pl.multiple_of(t * final, final), final)
            base = r0[plane, at, :]
            along = w0[plane, at, :]
            sol_ref[plane, at, :] = inv[plane, at, :] * (lead * base - trail * along)
            res_ref[plane, at, :] = base - lead * along + trail * w1[plane, at, :]
            return carry

        lax.fori_loop(0, rows // final, last, 0)

    @pl.when(jnp.logical_and(is_odd, has_far))
    def _():
        plane = depth - 1

        for i, span in enumerate(lates):
            halo_arrival(1, 1, span, far_recv.at[1, i]).wait_recv()

            def tile(t, carry, span=span):
                at = pl.ds(pl.multiple_of(span[0] + t * TILE, TILE), TILE)
                beyond = jnp.where(inv[plane, at, :] > 0.0, halo_u[1, at, :], 0.0)
                res_ref[plane, at, :] = res_ref[plane, at, :] - trail * beyond
                return carry

            lax.fori_loop(0, span[1] // TILE, tile, 0)

    @pl.when(jnp.logical_and(is_even, has_far))
    def _():
        for i in range(len(lates) - 3, len(lates)):
            late_copy(i).wait_send()


def store(sol_ref, res_ref, sol_out, res_out, sem):
    copies = []
    for which, (source, target) in enumerate(((sol_ref, sol_out), (res_ref, res_out))):
        for plane in range(sol_ref.shape[0]):
            copies.append(
                pltpu.make_async_copy(source.at[plane], target.at[plane], sem.at[which, plane])
            )
    for copy in copies:
        copy.start()
    for copy in copies:
        copy.wait()


def groups(chips):
    near = math.gcd(chips, 4)
    return (near, 1), (chips // near, near)


def body(count, right_side, cell_flags):
    depth, rows, cols = right_side.shape
    assert count % 2 == 0 and depth > 1
    stages = groups(count // 2)
    widest = max(stages[0][0], stages[1][0], 2 * (stages[1][0] - 1))
    chunk = math.gcd(rows, CHUNK)
    assert rows % 512 == 0
    pieces = max(6, len(LATE)) - 1
    f32 = jnp.float32
    field = pltpu.VMEM((depth, rows, cols), f32)
    padded = pltpu.VMEM((depth, rows + 2 * PAD, cols), f32)
    dma = pltpu.SemaphoreType.DMA
    grant = VMEM_BYTES - 8 * right_side.size - 2**19
    fields = pl.pallas_call(
        functools.partial(kernel, count, chunk, stages),
        out_shape=(field, field),
        in_specs=[pl.BlockSpec(memory_space=pltpu.HBM)] * 2,
        out_specs=(pl.BlockSpec(memory_space=pltpu.VMEM),) * 2,
        scratch_shapes=[
            field,
            pltpu.VMEM((depth, rows, cols), jnp.int32),
            field, field,
            pltpu.VMEM((rows, cols), f32),
            padded, padded, field, field,
            pltpu.VMEM((2, rows, cols), f32),
            pltpu.VMEM((2, rows, cols), f32),
            pltpu.VMEM((depth + 4, rows // 32, cols), jnp.int32),
            pltpu.VMEM((2, rows // 64, cols), jnp.int32),
            pltpu.VMEM((depth, rows // 32, cols), jnp.int32),
            pltpu.VMEM((depth + 1, 3, rows // 32, cols), jnp.int32),
            pltpu.VMEM((8, 128), f32),
            pltpu.VMEM((2, 8, 128), f32),
            pltpu.VMEM((2, widest, 8, 128), f32),
            dma((2, depth)),
            pltpu.SemaphoreType.REGULAR,
            pltpu.SemaphoreType.REGULAR,
            pltpu.SemaphoreType.REGULAR((max((stages[1][0] - 1).bit_length(), 1),)),
            dma((2,)), dma((3,)),
            dma((1 + len(LATE),)), dma((2, pieces)), dma((2,)), dma((2,)),
            dma, dma,
            dma((3,)), dma((2,)),
        ],
        compiler_params=pltpu.CompilerParams(
            collective_id=0, has_side_effects=True, vmem_limit_bytes=grant
        ),
    )(right_side, cell_flags)
    result = jax.ShapeDtypeStruct((depth, rows, cols), f32)
    return pl.pallas_call(
        store,
        out_shape=(result, result),
        in_specs=[pl.BlockSpec(memory_space=pltpu.VMEM)] * 2,
        out_specs=(pl.BlockSpec(memory_space=pltpu.HBM),) * 2,
        scratch_shapes=[dma((2, depth))],
        compiler_params=pltpu.CompilerParams(vmem_limit_bytes=2**19),
    )(*fields)


def solution(mesh):
    placed = (P("gz", None, None), P("gz", None, None))
    return jax.shard_map(
        functools.partial(body, mesh.shape["gz"]),
        mesh=mesh,
        in_specs=placed,
        out_specs=placed,
        check_vma=False,
    )
```

```python
import functools
import math

import jax
import jax.numpy as jnp
from jax import lax
from jax.experimental import pallas as pl
from jax.experimental.pallas import tpu as pltpu
from jax.sharding import PartitionSpec as P

MESH = pl.DeviceIdType.MESH
TILE = 16
LAST = 64
LATE = (0, 2, 3, 5, 7, 8)
CHUNK = 64
PAD = 8
VMEM_BYTES = 67_043_328


def kernel(
    count, chunk, stages,
    side_hbm, flag_hbm, sol_ref, res_ref,
    rhs, flags, r0, inv, shadow, u0, u1, w0, w1, halo_r, halo_u, solid, halves, fluid, code,
    pair, mine, got,
    in_sem, go, clear, known, bit_send, bit_recv, far_send, far_recv, near_send, near_recv,
    pair_send, pair_recv, sum_send, sum_recv,
):
    depth, rows, cols = rhs.shape
    words = rows // 32
    steps = rows // TILE
    parts = rows // chunk
    marks = sorted({0, 1, parts // 2, max(parts - 2, 0), max(parts - 1, 0), parts})
    plain = marks.index(parts // 2)
    half = words // 2
    spans = [(a * chunk, (b - a) * chunk) for a, b in zip(marks, marks[1:])]
    most = (0, rows - spans[-1][1])
    late_marks = [rows * eighth // 8 for eighth in LATE]
    lates = [(a, b - a) for a, b in zip(late_marks, late_marks[1:])]
    final = math.gcd(rows, LAST)
    near_size, far_size = stages[0][0], stages[1][0]
    me = lax.axis_index("gz")
    chip, odd = me // 2, lax.rem(me, 2)
    is_even, is_odd = odd == 0, odd == 1
    near_side, far_side = 1 - odd, odd
    near_plane, far_plane = near_side * (depth - 1), far_side * (depth - 1)
    partner = me + 1 - 2 * odd
    has_far = jnp.where(is_even, me > 0, me < count - 1)

    digit = lax.rem(chip, near_size)
    relief = near_size // 2 if near_size > 2 else 0
    is_first, is_relief = digit == 0, digit == relief

    def load(plane, which):
        source, target = ((flag_hbm, flags), (side_hbm, rhs))[which]
        return pltpu.make_async_copy(source.at[plane], target.at[plane], in_sem.at[which, plane])

    def peer(stage, j):
        size, stride = stages[stage]
        digit = lax.rem(chip // stride, size)
        return digit, chip + (lax.rem(digit + j, size) - digit) * stride

    barrier = pltpu.get_barrier_semaphore()

    def greet(other):
        pl.semaphore_signal(barrier, inc=1, device_id=(other,), device_id_type=MESH)

    @pl.when(has_far)
    def _():
        greet(me - 1 + 2 * odd)

    greet(partner)
    inner_planes = list(range(1, depth - 1))
    load(far_plane, 0).start()
    load(far_plane, 1).start()
    for plane in [near_plane] + inner_planes:
        load(plane, 0).start()
    for plane in [near_plane] + inner_planes:
        load(plane, 1).start()
    pairs = far_size & (far_size - 1) == 0
    if pairs:
        rounds = [(far_size >> i,) for i in range(1, far_size.bit_length())]
    else:
        rounds = [tuple(range(1, far_size))]

    def far_peer(distance):
        digit = chip // near_size
        if pairs:
            step = distance * (1 - 2 * lax.rem(digit // distance, 2))
        else:
            step = lax.rem(digit + distance, far_size) - digit
        return 2 * (chip + step * near_size) + 1

    if relief:
        @pl.when(is_even)
        def _():
            greet(2 * (chip - digit + lax.rem(digit + relief, near_size)) + 1)

    @pl.when(is_odd)
    def _():
        for group in rounds:
            for distance in group:
                greet(far_peer(distance))
        for j in range(1, near_size):
            greet(2 * peer(0, j)[1] + 1)

    def tell(which):
        for distance in rounds[which]:
            pl.semaphore_signal(
                known.at[which], inc=1, device_id=(far_peer(distance),), device_id_type=MESH
            )

    def hear(which):
        pl.semaphore_wait(known.at[which], len(rounds[which]))
        if which + 1 < len(rounds):
            tell(which + 1)

    blank = jnp.zeros((PAD, cols), jnp.float32)
    for ref in (u0, u1):
        for plane in range(ref.shape[0]):
            ref[plane, 0:PAD, :] = blank
            ref[plane, rows + PAD:rows + 2 * PAD, :] = blank

    @pl.when(jnp.logical_not(has_far))
    def _():
        solid[far_side * (depth + 2)] = jnp.zeros((words, cols), jnp.int32)
        solid[far_side * (depth + 2) + 1] = jnp.zeros((words, cols), jnp.int32)
        halves[1] = jnp.zeros((half, cols), jnp.int32)

        def clear(t, carry):
            at = pl.ds(pl.multiple_of(t * TILE, TILE), TILE)
            halo_r[far_side, at, :] = jnp.zeros((TILE, cols), jnp.float32)
            halo_u[far_side, at, :] = jnp.zeros((TILE, cols), jnp.float32)
            return carry

        lax.fori_loop(0, steps, clear, 0)

    def on(side, there):
        if side is far_side:
            pl.when(has_far)(there)
        else:
            there()

    def halo_copy(phase, side, span, send, recv, raw=False):
        start, size = span
        plane = side * (depth - 1)
        if raw:
            source = r0.at[plane, pl.ds(start, size)]
        else:
            source = (u0, u1)[phase].at[plane, pl.ds(start + PAD, size)]
        return pltpu.make_async_remote_copy(
            src_ref=source,
            dst_ref=(halo_r, halo_u)[phase].at[1 - side, pl.ds(start, size)],
            send_sem=send,
            recv_sem=recv,
            device_id=(me - 1 + 2 * side,),
            device_id_type=MESH,
        )

    def halo_arrival(phase, side, span, recv):
        start, size = span
        target = (halo_r, halo_u)[phase].at[side, pl.ds(start, size)]
        return pltpu.make_async_remote_copy(
            src_ref=target,
            dst_ref=target,
            send_sem=near_send.at[phase],
            recv_sem=recv,
            device_id=(me - 1 + 2 * side,),
            device_id_type=MESH,
        )

    def far_copy(phase, i, raw=False):
        send = far_send.at[2 * phase + (i == len(spans) - 1)]
        return halo_copy(phase, far_side, spans[i], send, far_recv.at[phase, i], raw)

    def far_sent(phase):
        sender = far_send.at[2 * phase]
        on(far_side, lambda: halo_copy(
            phase, far_side, most, sender, far_recv.at[phase, 0]
        ).wait_send())

    def far_ended(phase):
        on(far_side, lambda: far_copy(phase, len(spans) - 1).wait_send())

    def late_copy(i):
        return halo_copy(1, far_side, lates[i], far_send.at[2 + i], far_recv.at[1, i])

    def near_copy(phase):
        return halo_copy(
            phase, near_side, (0, rows), near_send.at[phase], near_recv.at[phase]
        )

    def near_arrival(phase):
        return halo_arrival(phase, near_side, (0, rows), near_recv.at[phase])

    def far_pieces(first, last, phase=0, raw=False):
        def some():
            for i in range(first, last):
                far_copy(phase, i, raw).start()

        on(far_side, some)

    def bit_copy(side, arrival=False):
        halo_at = 1 + side * (depth + 1)
        source = halo_at if arrival else 2 + side * (depth - 1)
        target = halo_at if arrival else 1 + (1 - side) * (depth + 1)
        return pltpu.make_async_remote_copy(
            src_ref=solid.at[source],
            dst_ref=solid.at[target],
            send_sem=bit_send.at[0],
            recv_sem=bit_recv.at[side if arrival else 1 - side],
            device_id=(me - 1 + 2 * side,),
            device_id_type=MESH,
        )

    def half_copy(arrival=False):
        return pltpu.make_async_remote_copy(
            src_ref=halves.at[1 if arrival else 0],
            dst_ref=halves.at[1],
            send_sem=bit_send.at[1],
            recv_sem=bit_recv.at[2],
            device_id=(me - 1 + 2 * far_side,),
            device_id_type=MESH,
        )

    def bits_sent(planes):
        several = solid.at[pl.ds(0, planes)]
        pltpu.make_async_remote_copy(
            src_ref=several,
            dst_ref=several,
            send_sem=bit_send.at[0],
            recv_sem=bit_recv.at[0],
            device_id=(partner,),
            device_id_type=MESH,
        ).wait_send()

    def mask(plane, first, last):
        def tile(t, carry):
            at = pl.ds(pl.multiple_of(t * TILE, TILE), TILE)
            r0[plane, at, :] = jnp.where(flags[plane, at, :] == 1, rhs[plane, at, :], 0.0)
            return carry

        lax.fori_loop(first, last, tile, 0)

    def pack(plane):
        def one(j, found):
            at = pl.ds(pl.multiple_of(j * words, words), words)
            kinds = flags[plane, at, :]
            return tuple(
                word | jnp.left_shift(jnp.where(kinds == kind, 1, 0), j)
                for word, kind in zip(found, (2, 1))
            )

        empty = jnp.zeros((words, cols), jnp.int32)
        solid[plane + 2], fluid[plane] = lax.fori_loop(0, 32, one, (empty, empty))

    greeted = sum(len(group) for group in rounds) + near_size - 1 + (relief > 0)
    callers = 1 + has_far.astype(jnp.int32)
    kept = max(len(spans) - 2, 1)
    load(far_plane, 0).wait()
    pack(far_plane)

    @pl.when(is_even)
    def _():
        pl.semaphore_wait(barrier, callers)
        on(far_side, lambda: bit_copy(0).start())

    load(far_plane, 1).wait()
    mask(far_plane, 0, chunk // TILE)

    @pl.when(is_even)
    def _():
        far_pieces(0, 1, raw=True)

    for plane in [near_plane] + inner_planes:
        load(plane, 0).wait()
        pack(plane)

    @pl.when(is_even)
    def _():
        low, high = solid[3, 0:half, :], solid[3, half:words, :]
        halves[0] = jnp.bitwise_and(low, 0xFFFF) | jnp.left_shift(high, 16)
        on(far_side, lambda: half_copy().start())

    @pl.when(is_odd)
    def _():
        pl.semaphore_wait(barrier, callers + greeted)
        on(far_side, lambda: bit_copy(1).start())
        if rounds:
            tell(0)

    bit_copy(near_side).start()
    mask(far_plane, chunk // TILE, steps)

    @pl.when(is_even)
    def _():
        far_pieces(1, plain, raw=True)

    for plane in [near_plane] + inner_planes:
        load(plane, 1).wait()
        mask(plane, 0, steps)

    bit_copy(near_side, True).wait_recv()
    on(far_side, lambda: bit_copy(far_side, True).wait_recv())

    def classify(at, slot, known_fluid):
        word = solid[at]
        line = lax.broadcasted_iota(jnp.int32, (words, cols), 0)
        across = lax.broadcasted_iota(jnp.int32, (words, cols), 1)
        before, after = pltpu.roll(word, 1, 0), pltpu.roll(word, words - 1, 0)
        before = jnp.where(line == 0, jnp.left_shift(before, 1), before)
        after = jnp.where(line == words - 1, lax.shift_right_logical(after, 1), after)
        left = jnp.where(across == 0, 0, pltpu.roll(word, 1, 1))
        right = jnp.where(across == cols - 1, 0, pltpu.roll(word, cols - 1, 1))

        def add(a, b, c):
            return a ^ b ^ c, (a & b) | (c & (a ^ b))

        ones, twos = add(before, after, left)
        more_ones, more_twos = add(right, solid[at - 1], solid[at + 1])
        digits = [ones ^ more_ones, *add(twos, more_twos, ones & more_ones)]
        for i, digit in enumerate(digits):
            if known_fluid is not None:
                digit = digit | ~known_fluid
            code[slot, i] = digit

    def inverse(slot, j):
        bit = jnp.left_shift(1, j)
        ones, twos, fours = ((code[slot, i] & bit) != 0 for i in range(3))
        none, one, two, three, four, five, six, out = (
            jnp.float32(value) for value in (1 / 6, 1 / 5, 1 / 4, 1 / 3, 1 / 2, 1.0, 1.0, 0.0)
        )
        low = jnp.where(twos, jnp.where(ones, three, two), jnp.where(ones, one, none))
        high = jnp.where(twos, jnp.where(ones, out, six), jnp.where(ones, five, four))
        return jnp.where(fours, high, low)

    column = lax.broadcasted_iota(jnp.int32, (TILE, cols), 1)

    def inplane(ref, plane, start):
        block = ref[plane, pl.ds(start, TILE + 2 * PAD), :]
        centre = block[PAD:PAD + TILE]
        total = block[PAD - 1:PAD - 1 + TILE] + block[PAD + 1:PAD + 1 + TILE]
        total = total + jnp.where(column == 0, 0.0, pltpu.roll(centre, 1, 1))
        total = total + jnp.where(column == cols - 1, 0.0, pltpu.roll(centre, cols - 1, 1))
        return centre, total

    def centre_of(ref, plane, start):
        return ref[plane, pl.ds(pl.multiple_of(start + PAD, PAD), TILE), :]

    def put(ref, plane, start, value):
        ref[plane, pl.ds(pl.multiple_of(start + PAD, PAD), TILE), :] = value

    def fold(value):
        total = value[0:8]
        for i in range(8, value.shape[0], 8):
            total = total + value[i:i + 8]
        return total

    none = jnp.zeros((8, cols), jnp.float32)

    for plane in range(depth):
        classify(plane + 2, plane, fluid[plane])

    def first(j, moment):
        start = pl.multiple_of(j * words, words)
        at = pl.ds(start, words)
        padded = pl.ds(pl.multiple_of(start + PAD, PAD), words)
        for plane in range(depth):
            value = inverse(plane, j)
            inv[plane, at, :] = value
            residual = r0[plane, at, :]
            precond = residual * value
            u0[plane, padded, :] = precond
            moment = moment + fold(residual * precond)
        return moment

    moment0 = lax.fori_loop(0, 32, first, none)
    near_copy(0).start()

    @pl.when(is_even)
    def _():
        far_pieces(plain, kept)

        @pl.when(jnp.logical_not(is_first))
        def _():
            far_pieces(kept, len(spans))

    @pl.when(jnp.logical_and(is_odd, is_first))
    def _():
        far_pieces(0, len(spans))

    def known_scale(t, carry):
        at = pl.ds(pl.multiple_of(t * TILE, TILE), TILE)
        shadow[at, :] = jnp.ones((TILE, cols), jnp.float32)
        return carry

    lax.fori_loop(odd * (steps // 2), steps, known_scale, 0)

    @pl.when(is_odd)
    def _():
        on(far_side, lambda: half_copy(True).wait_recv())
        solid[depth + 3, 0:half, :] = jnp.bitwise_and(halves[1], 0xFFFF)
        solid[depth + 3, half:words, :] = lax.shift_right_logical(halves[1], 16)
        classify(depth + 2, depth, None)

        def beyond(j, carry):
            shadow[pl.ds(pl.multiple_of(j * words, words), words), :] = inverse(depth, j)
            return carry

        lax.fori_loop(0, 16, beyond, 0)
        if rounds:
            hear(0)

    def local_part(field, scaled, out, plane, start):
        at = pl.ds(start, TILE)
        _, total = inplane(field, plane, start)
        if plane > 0:
            total = total + centre_of(field, plane - 1, start)
        if plane < depth - 1:
            total = total + centre_of(field, plane + 1, start)
        image = jnp.where(inv[plane, at, :] > 0.0, scaled[plane, at, :] - total, 0.0)
        out[plane, at, :] = image
        return image

    def apply_once(plane, start, image, value, moments):
        precond = image * value
        put(u1, plane, start, precond)
        return (
            moments[0] + fold(image * centre_of(u0, plane, start)),
            moments[1] + fold(image * precond),
        )

    def second(t, moments):
        start = pl.multiple_of(t * TILE, TILE)
        for plane in range(depth):
            image = local_part(u0, r0, w0, plane, start)
            if 0 < plane < depth - 1:
                value = inv[plane, pl.ds(start, TILE), :]
                moments = apply_once(plane, start, image, value, moments)
        return moments

    moments = lax.fori_loop(0, steps, second, (none, none))

    def edge_one(side, span, moments):
        plane = side * (depth - 1)

        def tile(t, moments):
            start = pl.multiple_of(span[0] + t * TILE, TILE)
            at = pl.ds(start, TILE)
            value = inv[plane, at, :]
            beyond = halo_r[side, at, :]
            if side is far_side:
                beyond = beyond * shadow[at, :]
            image = jnp.where(value > 0.0, w0[plane, at, :] - beyond, 0.0)
            w0[plane, at, :] = image
            return apply_once(plane, start, image, value, moments)

        return lax.fori_loop(0, span[1] // TILE, tile, moments)

    passing = digit == near_size - 1
    @pl.when(is_odd)
    def _():
        for which in range(1, len(rounds)):
            hear(which)

    @pl.when(jnp.logical_and(is_even, is_first))
    def _():
        far_pieces(kept, len(spans))

    @pl.when(jnp.logical_not(is_first))
    def _():
        @pl.when(is_even)
        def _():
            far_sent(0)
            pl.semaphore_signal(go, inc=1, device_id=(partner,), device_id_type=MESH)

        @pl.when(is_odd)
        def _():
            pl.semaphore_wait(go, 1)

            @pl.when(jnp.logical_and(passing, chip >= near_size))
            def _():
                pl.semaphore_signal(
                    clear, inc=1, device_id=(me - 2 * near_size,), device_id_type=MESH
                )

            @pl.when(jnp.logical_and(passing, chip + near_size < count // 2))
            def _():
                pl.semaphore_wait(clear, 1)

            far_pieces(0, len(spans))

    near_arrival(0).wait_recv()
    moments = edge_one(near_side, (0, rows), moments)
    near_copy(1).start()
    for i, span in enumerate(spans):
        on(far_side, lambda: halo_arrival(0, far_side, span, far_recv.at[0, i]).wait_recv())
        moments = edge_one(far_side, span, moments)

        @pl.when(is_odd)
        def _():
            far_pieces(i, i + 1, 1)

    moment1, moment2 = moments

    def third(t, moment):
        start = pl.multiple_of(t * TILE, TILE)
        for plane in range(depth):
            image = local_part(u1, w0, w1, plane, start)
            moment = moment + fold(image * centre_of(u1, plane, start))
        return moment

    moment3 = lax.fori_loop(0, steps, third, none)

    def edge_two(side, span, moment, weight):
        plane = side * (depth - 1)

        def tile(t, moment):
            start = pl.multiple_of(span[0] + t * TILE, TILE)
            at = pl.ds(start, TILE)
            beyond = halo_u[side, at, :]
            image = jnp.where(inv[plane, at, :] > 0.0, w1[plane, at, :] - beyond, 0.0)
            w1[plane, at, :] = image
            return moment - weight * fold(beyond * centre_of(u1, plane, start))

        return lax.fori_loop(0, span[1] // TILE, tile, moment)

    def lanes(value):
        total = value[:, 0:128]
        for i in range(128, cols, 128):
            total = total + value[:, i:i + 128]
        return jnp.sum(total, axis=0, keepdims=True)

    for i, value in enumerate((moment0, moment1, moment2)):
        mine[0, i:i + 1, :] = lanes(value)
    mine[0, 3:8, :] = jnp.zeros((5, 128), jnp.float32)
    near_arrival(1).wait_recv()
    moment3 = edge_two(near_side, (0, rows), moment3, 1.0)

    def pair_copy():
        return pltpu.make_async_remote_copy(
            src_ref=mine.at[0], dst_ref=pair, send_sem=pair_send, recv_sem=pair_recv,
            device_id=(partner,), device_id_type=MESH,
        )

    def sum_copy(stage, j, core, shift=0):
        slot, other = peer(stage, j)
        return pltpu.make_async_remote_copy(
            src_ref=mine.at[stage],
            dst_ref=got.at[stage, slot],
            send_sem=sum_send.at[0 if stage == 0 or j == 0 else 2 if shift else 1],
            recv_sem=sum_recv.at[stage],
            device_id=(2 * (other - shift) + core,),
            device_id_type=MESH,
        )

    def sums(stage, copies, sender=0):
        several = got.at[stage, pl.ds(0, copies)]
        return pltpu.make_async_remote_copy(
            src_ref=several,
            dst_ref=several,
            send_sem=sum_send.at[sender],
            recv_sem=sum_recv.at[stage],
            device_id=(partner,),
            device_id_type=MESH,
        )

    def across():
        sum_copy(1, 0, 0).start()

        def to_all(shift):
            for j in range(1, far_size):
                for core in (1, 0):
                    sum_copy(1, j, core, shift).start()

        if relief:
            pl.when(is_relief)(lambda: to_all(relief))
            pl.when(jnp.logical_not(is_first))(lambda: to_all(0))
        else:
            to_all(0)

    def across_sent():
        sums(0, 1).wait_send()
        if far_size > 1:
            pl.when(jnp.logical_not(is_first) if relief else True)(
                lambda: sums(0, 2 * (far_size - 1), 1).wait_send()
            )
            if relief:
                pl.when(is_relief)(lambda: sums(0, 2 * (far_size - 1), 2).wait_send())

    def gathered(stage):
        total = got[stage, 0]
        for i in range(1, stages[stage][0]):
            total = total + got[stage, i]
        return total

    @pl.when(is_even)
    def _():
        pair_copy().wait_recv()
        mine[0] = mine[0] + pair[...]
        moment = moment3
        for i, span in enumerate(spans):
            on(far_side, lambda: halo_arrival(1, far_side, span, far_recv.at[1, i]).wait_recv())
            for place, after in ((is_first, 4), (jnp.logical_not(is_first), 3)):
                if i == max(len(spans) - after, 0):
                    @pl.when(place)
                    def _():
                        @pl.when(jnp.logical_or(jnp.logical_not(is_first), chip >= near_size))
                        def _():
                            pl.semaphore_wait(go, 1)

                        on(far_side, lambda: late_copy(0).start())

                        @pl.when(jnp.logical_and(is_first, has_far))
                        def _():
                            late_copy(1).start()

            moment = edge_two(far_side, span, moment, 2.0)

        mine[0, 3:4, :] = mine[0, 3:4, :] + lanes(moment)
        for j in range(near_size):
            sum_copy(0, j, 1).start()

        @pl.when(has_far)
        def _():
            pl.when(jnp.logical_not(is_first))(lambda: late_copy(1).start())
            late_copy(2).start()
            for i in range(3, len(lates)):
                late_copy(i - 3).wait_send()
                late_copy(i).start()

    @pl.when(is_odd)
    def _():
        mine[0, 3:4, :] = lanes(moment3)
        pair_copy().start()
        far_sent(1)

        @pl.when(jnp.logical_or(jnp.logical_not(is_first), chip + near_size < count // 2))
        def _():
            waiting = jnp.where(is_first, me - 1 + 2 * near_size, partner)
            pl.semaphore_signal(go, inc=1, device_id=(waiting,), device_id_type=MESH)

        sums(0, near_size).wait_recv()
        total = gathered(0)
        mine[1] = total
        across()
        got[1, peer(1, 0)[0]] = total

    near_copy(0).wait_send()
    near_copy(1).wait_send()
    far_ended(0)

    @pl.when(is_even)
    def _():
        pl.when(has_far)(lambda: bits_sent(2))
        pl.when(jnp.logical_not(has_far))(lambda: bits_sent(1))
        on(far_side, lambda: half_copy().wait_send())
        pl.when(is_first)(lambda: far_sent(0))
        sums(0, near_size).wait_send()
        sums(1, far_size).wait_recv()

    @pl.when(is_odd)
    def _():
        pl.when(has_far)(lambda: bits_sent(2))
        pl.when(jnp.logical_not(has_far))(lambda: bits_sent(1))
        far_sent(0)
        far_ended(1)
        pair_copy().wait_send()
        across_sent()
        if far_size > 1:
            sums(1, far_size - 1).wait_recv()

    everyone = gathered(1)
    s0, s1, s2, s3 = (everyone[i:i + 1] for i in range(4))

    def whole(value):
        return jnp.sum(value, axis=1, keepdims=True)

    rz_old = whole(s0)
    step_old = rz_old / whole(s1)
    rz_now = whole(s0 - 2.0 * step_old * s1 + step_old * step_old * s2)
    grown = 1.0 + rz_now / rz_old
    product = whole(grown * grown * s1 - 2.0 * step_old * grown * s2 + step_old * step_old * s3)
    step_size = rz_now / product
    lead = step_old + step_size * grown
    trail = step_size * step_old

    for plane in range(depth):
        def last(t, carry, plane=plane):
            at = pl.ds(pl.multiple_of(t * final, final), final)
            base = r0[plane, at, :]
            along = w0[plane, at, :]
            sol_ref[plane, at, :] = inv[plane, at, :] * (lead * base - trail * along)
            res_ref[plane, at, :] = base - lead * along + trail * w1[plane, at, :]
            return carry

        lax.fori_loop(0, rows // final, last, 0)

    @pl.when(jnp.logical_and(is_odd, has_far))
    def _():
        plane = depth - 1

        for i, span in enumerate(lates):
            halo_arrival(1, 1, span, far_recv.at[1, i]).wait_recv()

            def tile(t, carry, span=span):
                at = pl.ds(pl.multiple_of(span[0] + t * final, final), final)
                beyond = jnp.where(inv[plane, at, :] > 0.0, halo_u[1, at, :], 0.0)
                res_ref[plane, at, :] = res_ref[plane, at, :] - trail * beyond
                return carry

            lax.fori_loop(0, span[1] // final, tile, 0)

    @pl.when(jnp.logical_and(is_even, has_far))
    def _():
        for i in range(len(lates) - 3, len(lates)):
            late_copy(i).wait_send()


def store(sol_ref, res_ref, sol_out, res_out, sem):
    copies = []
    for which, (source, target) in enumerate(((sol_ref, sol_out), (res_ref, res_out))):
        for plane in range(sol_ref.shape[0]):
            copies.append(
                pltpu.make_async_copy(source.at[plane], target.at[plane], sem.at[which])
            )
    for copy in copies:
        copy.start()
    for which, (source, target) in enumerate(((sol_ref, sol_out), (res_ref, res_out))):
        pltpu.make_async_copy(source, target, sem.at[which]).wait()


def groups(chips):
    near = math.gcd(chips, 4)
    return (near, 1), (chips // near, near)


def body(count, right_side, cell_flags):
    depth, rows, cols = right_side.shape
    assert count % 2 == 0 and depth > 1
    stages = groups(count // 2)
    widest = max(stages[0][0], stages[1][0], 2 * (stages[1][0] - 1))
    chunk = math.gcd(rows, CHUNK)
    assert rows % 512 == 0
    pieces = max(6, len(LATE)) - 1
    f32 = jnp.float32
    field = pltpu.VMEM((depth, rows, cols), f32)
    padded = pltpu.VMEM((depth, rows + 2 * PAD, cols), f32)
    dma = pltpu.SemaphoreType.DMA
    grant = VMEM_BYTES - 8 * right_side.size - 2**19
    fields = pl.pallas_call(
        functools.partial(kernel, count, chunk, stages),
        out_shape=(field, field),
        in_specs=[pl.BlockSpec(memory_space=pltpu.HBM)] * 2,
        out_specs=(pl.BlockSpec(memory_space=pltpu.VMEM),) * 2,
        scratch_shapes=[
            field,
            pltpu.VMEM((depth, rows, cols), jnp.int32),
            field, field,
            pltpu.VMEM((rows, cols), f32),
            padded, padded, field, field,
            pltpu.VMEM((2, rows, cols), f32),
            pltpu.VMEM((2, rows, cols), f32),
            pltpu.VMEM((depth + 4, rows // 32, cols), jnp.int32),
            pltpu.VMEM((2, rows // 64, cols), jnp.int32),
            pltpu.VMEM((depth, rows // 32, cols), jnp.int32),
            pltpu.VMEM((depth + 1, 3, rows // 32, cols), jnp.int32),
            pltpu.VMEM((8, 128), f32),
            pltpu.VMEM((2, 8, 128), f32),
            pltpu.VMEM((2, widest, 8, 128), f32),
            dma((2, depth)),
            pltpu.SemaphoreType.REGULAR,
            pltpu.SemaphoreType.REGULAR,
            pltpu.SemaphoreType.REGULAR((max((stages[1][0] - 1).bit_length(), 1),)),
            dma((2,)), dma((3,)),
            dma((1 + len(LATE),)), dma((2, pieces)), dma((2,)), dma((2,)),
            dma, dma,
            dma((3,)), dma((2,)),
        ],
        compiler_params=pltpu.CompilerParams(
            collective_id=0, has_side_effects=True, vmem_limit_bytes=grant
        ),
    )(right_side, cell_flags)
    result = jax.ShapeDtypeStruct((depth, rows, cols), f32)
    return pl.pallas_call(
        store,
        out_shape=(result, result),
        in_specs=[pl.BlockSpec(memory_space=pltpu.VMEM)] * 2,
        out_specs=(pl.BlockSpec(memory_space=pltpu.HBM),) * 2,
        scratch_shapes=[dma((2,))],
        compiler_params=pltpu.CompilerParams(vmem_limit_bytes=2**19),
    )(*fields)


def solution(mesh):
    placed = (P("gz", None, None), P("gz", None, None))
    return jax.shard_map(
        functools.partial(body, mesh.shape["gz"]),
        mesh=mesh,
        in_specs=placed,
        out_specs=placed,
        check_vma=False,
    )
```

```python
import functools
import math

import jax
import jax.numpy as jnp
from jax import lax
from jax.experimental import pallas as pl
from jax.experimental.pallas import tpu as pltpu
from jax.sharding import PartitionSpec as P

MESH = pl.DeviceIdType.MESH
TILE = 16
LAST = 128
LATE = (0, 2, 3, 5, 7, 8)
CHUNK = 64
PAD = 8
VMEM_BYTES = 67_043_328


def kernel(
    count, chunk, stages,
    side_hbm, flag_hbm, sol_ref, res_ref,
    rhs, flags, r0, inv, shadow, u0, u1, w0, w1, halo_r, halo_u, solid, halves, fluid, code,
    pair, mine, got,
    in_sem, go, clear, known, bit_send, bit_recv, far_send, far_recv, near_send, near_recv,
    pair_send, pair_recv, sum_send, sum_recv,
):
    depth, rows, cols = rhs.shape
    words = rows // 32
    steps = rows // TILE
    parts = rows // chunk
    marks = sorted({0, 1, parts // 2, max(parts - 2, 0), max(parts - 1, 0), parts})
    plain = marks.index(parts // 2)
    half = words // 2
    spans = [(a * chunk, (b - a) * chunk) for a, b in zip(marks, marks[1:])]
    most = (0, rows - spans[-1][1])
    late_marks = [rows * eighth // 8 for eighth in LATE]
    lates = [(a, b - a) for a, b in zip(late_marks, late_marks[1:])]
    final = math.gcd(rows, LAST)
    late_rows = math.gcd(chunk, LAST)
    near_size, far_size = stages[0][0], stages[1][0]
    me = lax.axis_index("gz")
    chip, odd = me // 2, lax.rem(me, 2)
    is_even, is_odd = odd == 0, odd == 1
    near_side, far_side = 1 - odd, odd
    near_plane, far_plane = near_side * (depth - 1), far_side * (depth - 1)
    partner = me + 1 - 2 * odd
    has_far = jnp.where(is_even, me > 0, me < count - 1)

    digit = lax.rem(chip, near_size)
    relief = near_size // 2 if near_size > 2 else 0
    is_first, is_relief = digit == 0, digit == relief

    def load(plane, which):
        source, target = ((flag_hbm, flags), (side_hbm, rhs))[which]
        return pltpu.make_async_copy(source.at[plane], target.at[plane], in_sem.at[which, plane])

    def peer(stage, j):
        size, stride = stages[stage]
        digit = lax.rem(chip // stride, size)
        return digit, chip + (lax.rem(digit + j, size) - digit) * stride

    barrier = pltpu.get_barrier_semaphore()

    def greet(other):
        pl.semaphore_signal(barrier, inc=1, device_id=(other,), device_id_type=MESH)

    @pl.when(has_far)
    def _():
        greet(me - 1 + 2 * odd)

    greet(partner)
    inner_planes = list(range(1, depth - 1))
    load(far_plane, 0).start()
    load(far_plane, 1).start()
    for plane in [near_plane] + inner_planes:
        load(plane, 0).start()
    for plane in [near_plane] + inner_planes:
        load(plane, 1).start()
    pairs = far_size & (far_size - 1) == 0
    if pairs:
        rounds = [(far_size >> i,) for i in range(1, far_size.bit_length())]
    else:
        rounds = [tuple(range(1, far_size))]

    def far_peer(distance):
        digit = chip // near_size
        if pairs:
            step = distance * (1 - 2 * lax.rem(digit // distance, 2))
        else:
            step = lax.rem(digit + distance, far_size) - digit
        return 2 * (chip + step * near_size) + 1

    if relief:
        @pl.when(is_even)
        def _():
            greet(2 * (chip - digit + lax.rem(digit + relief, near_size)) + 1)

    @pl.when(is_odd)
    def _():
        for group in rounds:
            for distance in group:
                greet(far_peer(distance))
        for j in range(1, near_size):
            greet(2 * peer(0, j)[1] + 1)

    def tell(which):
        for distance in rounds[which]:
            pl.semaphore_signal(
                known.at[which], inc=1, device_id=(far_peer(distance),), device_id_type=MESH
            )

    def hear(which):
        pl.semaphore_wait(known.at[which], len(rounds[which]))
        if which + 1 < len(rounds):
            tell(which + 1)

    blank = jnp.zeros((PAD, cols), jnp.float32)
    for ref in (u0, u1):
        for plane in range(ref.shape[0]):
            ref[plane, 0:PAD, :] = blank
            ref[plane, rows + PAD:rows + 2 * PAD, :] = blank

    @pl.when(jnp.logical_not(has_far))
    def _():
        solid[far_side * (depth + 2)] = jnp.zeros((words, cols), jnp.int32)
        solid[far_side * (depth + 2) + 1] = jnp.zeros((words, cols), jnp.int32)
        halves[1] = jnp.zeros((half, cols), jnp.int32)

        def clear(t, carry):
            at = pl.ds(pl.multiple_of(t * TILE, TILE), TILE)
            halo_r[far_side, at, :] = jnp.zeros((TILE, cols), jnp.float32)
            halo_u[far_side, at, :] = jnp.zeros((TILE, cols), jnp.float32)
            return carry

        lax.fori_loop(0, steps, clear, 0)

    def on(side, there):
        if side is far_side:
            pl.when(has_far)(there)
        else:
            there()

    def halo_copy(phase, side, span, send, recv, raw=False):
        start, size = span
        plane = side * (depth - 1)
        if raw:
            source = r0.at[plane, pl.ds(start, size)]
        else:
            source = (u0, u1)[phase].at[plane, pl.ds(start + PAD, size)]
        return pltpu.make_async_remote_copy(
            src_ref=source,
            dst_ref=(halo_r, halo_u)[phase].at[1 - side, pl.ds(start, size)],
            send_sem=send,
            recv_sem=recv,
            device_id=(me - 1 + 2 * side,),
            device_id_type=MESH,
        )

    def halo_arrival(phase, side, span, recv):
        start, size = span
        target = (halo_r, halo_u)[phase].at[side, pl.ds(start, size)]
        return pltpu.make_async_remote_copy(
            src_ref=target,
            dst_ref=target,
            send_sem=near_send.at[phase],
            recv_sem=recv,
            device_id=(me - 1 + 2 * side,),
            device_id_type=MESH,
        )

    def far_copy(phase, i, raw=False):
        send = far_send.at[2 * phase + (i == len(spans) - 1)]
        return halo_copy(phase, far_side, spans[i], send, far_recv.at[phase, i], raw)

    def far_sent(phase):
        sender = far_send.at[2 * phase]
        on(far_side, lambda: halo_copy(
            phase, far_side, most, sender, far_recv.at[phase, 0]
        ).wait_send())

    def far_ended(phase):
        on(far_side, lambda: far_copy(phase, len(spans) - 1).wait_send())

    def late_copy(i):
        return halo_copy(1, far_side, lates[i], far_send.at[2 + i], far_recv.at[1, i])

    def near_copy(phase):
        return halo_copy(
            phase, near_side, (0, rows), near_send.at[phase], near_recv.at[phase]
        )

    def near_arrival(phase):
        return halo_arrival(phase, near_side, (0, rows), near_recv.at[phase])

    def far_pieces(first, last, phase=0, raw=False):
        def some():
            for i in range(first, last):
                far_copy(phase, i, raw).start()

        on(far_side, some)

    def bit_copy(side, arrival=False):
        halo_at = 1 + side * (depth + 1)
        source = halo_at if arrival else 2 + side * (depth - 1)
        target = halo_at if arrival else 1 + (1 - side) * (depth + 1)
        return pltpu.make_async_remote_copy(
            src_ref=solid.at[source],
            dst_ref=solid.at[target],
            send_sem=bit_send.at[0],
            recv_sem=bit_recv.at[side if arrival else 1 - side],
            device_id=(me - 1 + 2 * side,),
            device_id_type=MESH,
        )

    def half_copy(arrival=False):
        return pltpu.make_async_remote_copy(
            src_ref=halves.at[1 if arrival else 0],
            dst_ref=halves.at[1],
            send_sem=bit_send.at[1],
            recv_sem=bit_recv.at[2],
            device_id=(me - 1 + 2 * far_side,),
            device_id_type=MESH,
        )

    def bits_sent(planes):
        several = solid.at[pl.ds(0, planes)]
        pltpu.make_async_remote_copy(
            src_ref=several,
            dst_ref=several,
            send_sem=bit_send.at[0],
            recv_sem=bit_recv.at[0],
            device_id=(partner,),
            device_id_type=MESH,
        ).wait_send()

    def mask(plane, first, last):
        def tile(t, carry):
            at = pl.ds(pl.multiple_of(t * TILE, TILE), TILE)
            r0[plane, at, :] = jnp.where(flags[plane, at, :] == 1, rhs[plane, at, :], 0.0)
            return carry

        lax.fori_loop(first, last, tile, 0)

    def pack(plane):
        def one(j, found):
            at = pl.ds(pl.multiple_of(j * words, words), words)
            kinds = flags[plane, at, :]
            return tuple(
                word | jnp.left_shift(jnp.where(kinds == kind, 1, 0), j)
                for word, kind in zip(found, (2, 1))
            )

        empty = jnp.zeros((words, cols), jnp.int32)
        solid[plane + 2], fluid[plane] = lax.fori_loop(0, 32, one, (empty, empty))

    greeted = sum(len(group) for group in rounds) + near_size - 1 + (relief > 0)
    callers = 1 + has_far.astype(jnp.int32)
    kept = max(len(spans) - 2, 1)
    load(far_plane, 0).wait()
    pack(far_plane)

    @pl.when(is_even)
    def _():
        pl.semaphore_wait(barrier, callers)
        on(far_side, lambda: bit_copy(0).start())

    load(far_plane, 1).wait()
    mask(far_plane, 0, chunk // TILE)

    @pl.when(is_even)
    def _():
        far_pieces(0, 1, raw=True)

    for plane in [near_plane] + inner_planes:
        load(plane, 0).wait()
        pack(plane)

    @pl.when(is_even)
    def _():
        low, high = solid[3, 0:half, :], solid[3, half:words, :]
        halves[0] = jnp.bitwise_and(low, 0xFFFF) | jnp.left_shift(high, 16)
        on(far_side, lambda: half_copy().start())

    @pl.when(is_odd)
    def _():
        pl.semaphore_wait(barrier, callers + greeted)
        on(far_side, lambda: bit_copy(1).start())
        if rounds:
            tell(0)

    bit_copy(near_side).start()
    mask(far_plane, chunk // TILE, steps)

    @pl.when(is_even)
    def _():
        far_pieces(1, plain, raw=True)

    for plane in [near_plane] + inner_planes:
        load(plane, 1).wait()
        mask(plane, 0, steps)

    bit_copy(near_side, True).wait_recv()
    on(far_side, lambda: bit_copy(far_side, True).wait_recv())

    def classify(at, slot, known_fluid):
        word = solid[at]
        line = lax.broadcasted_iota(jnp.int32, (words, cols), 0)
        across = lax.broadcasted_iota(jnp.int32, (words, cols), 1)
        before, after = pltpu.roll(word, 1, 0), pltpu.roll(word, words - 1, 0)
        before = jnp.where(line == 0, jnp.left_shift(before, 1), before)
        after = jnp.where(line == words - 1, lax.shift_right_logical(after, 1), after)
        left = jnp.where(across == 0, 0, pltpu.roll(word, 1, 1))
        right = jnp.where(across == cols - 1, 0, pltpu.roll(word, cols - 1, 1))

        def add(a, b, c):
            return a ^ b ^ c, (a & b) | (c & (a ^ b))

        ones, twos = add(before, after, left)
        more_ones, more_twos = add(right, solid[at - 1], solid[at + 1])
        digits = [ones ^ more_ones, *add(twos, more_twos, ones & more_ones)]
        for i, digit in enumerate(digits):
            if known_fluid is not None:
                digit = digit | ~known_fluid
            code[slot, i] = digit

    def inverse(slot, j):
        bit = jnp.left_shift(1, j)
        ones, twos, fours = ((code[slot, i] & bit) != 0 for i in range(3))
        none, one, two, three, four, five, six, out = (
            jnp.float32(value) for value in (1 / 6, 1 / 5, 1 / 4, 1 / 3, 1 / 2, 1.0, 1.0, 0.0)
        )
        low = jnp.where(twos, jnp.where(ones, three, two), jnp.where(ones, one, none))
        high = jnp.where(twos, jnp.where(ones, out, six), jnp.where(ones, five, four))
        return jnp.where(fours, high, low)

    column = lax.broadcasted_iota(jnp.int32, (TILE, cols), 1)

    def inplane(ref, plane, start):
        block = ref[plane, pl.ds(start, TILE + 2 * PAD), :]
        centre = block[PAD:PAD + TILE]
        total = block[PAD - 1:PAD - 1 + TILE] + block[PAD + 1:PAD + 1 + TILE]
        total = total + jnp.where(column == 0, 0.0, pltpu.roll(centre, 1, 1))
        total = total + jnp.where(column == cols - 1, 0.0, pltpu.roll(centre, cols - 1, 1))
        return centre, total

    def centre_of(ref, plane, start):
        return ref[plane, pl.ds(pl.multiple_of(start + PAD, PAD), TILE), :]

    def put(ref, plane, start, value):
        ref[plane, pl.ds(pl.multiple_of(start + PAD, PAD), TILE), :] = value

    def fold(value):
        total = value[0:8]
        for i in range(8, value.shape[0], 8):
            total = total + value[i:i + 8]
        return total

    none = jnp.zeros((8, cols), jnp.float32)

    for plane in range(depth):
        classify(plane + 2, plane, fluid[plane])

    def first(j, moment):
        start = pl.multiple_of(j * words, words)
        at = pl.ds(start, words)
        padded = pl.ds(pl.multiple_of(start + PAD, PAD), words)
        for plane in range(depth):
            value = inverse(plane, j)
            inv[plane, at, :] = value
            residual = r0[plane, at, :]
            precond = residual * value
            u0[plane, padded, :] = precond
            moment = moment + fold(residual * precond)
        return moment

    moment0 = lax.fori_loop(0, 32, first, none)
    near_copy(0).start()

    @pl.when(is_even)
    def _():
        far_pieces(plain, kept)

        @pl.when(jnp.logical_not(is_first))
        def _():
            far_pieces(kept, len(spans))

    @pl.when(jnp.logical_and(is_odd, is_first))
    def _():
        far_pieces(0, len(spans))

    def known_scale(t, carry):
        at = pl.ds(pl.multiple_of(t * TILE, TILE), TILE)
        shadow[at, :] = jnp.ones((TILE, cols), jnp.float32)
        return carry

    lax.fori_loop(odd * (steps // 2), steps, known_scale, 0)

    @pl.when(is_odd)
    def _():
        on(far_side, lambda: half_copy(True).wait_recv())
        solid[depth + 3, 0:half, :] = jnp.bitwise_and(halves[1], 0xFFFF)
        solid[depth + 3, half:words, :] = lax.shift_right_logical(halves[1], 16)
        classify(depth + 2, depth, None)

        def beyond(j, carry):
            shadow[pl.ds(pl.multiple_of(j * words, words), words), :] = inverse(depth, j)
            return carry

        lax.fori_loop(0, 16, beyond, 0)
        if rounds:
            hear(0)

    def local_part(field, scaled, out, plane, start):
        at = pl.ds(start, TILE)
        _, total = inplane(field, plane, start)
        if plane > 0:
            total = total + centre_of(field, plane - 1, start)
        if plane < depth - 1:
            total = total + centre_of(field, plane + 1, start)
        image = jnp.where(inv[plane, at, :] > 0.0, scaled[plane, at, :] - total, 0.0)
        out[plane, at, :] = image
        return image

    def apply_once(plane, start, image, value, moments):
        precond = image * value
        put(u1, plane, start, precond)
        return (
            moments[0] + fold(image * centre_of(u0, plane, start)),
            moments[1] + fold(image * precond),
        )

    def second(t, moments):
        start = pl.multiple_of(t * TILE, TILE)
        for plane in range(depth):
            image = local_part(u0, r0, w0, plane, start)
            if 0 < plane < depth - 1:
                value = inv[plane, pl.ds(start, TILE), :]
                moments = apply_once(plane, start, image, value, moments)
        return moments

    moments = lax.fori_loop(0, steps, second, (none, none))

    def edge_one(side, span, moments):
        plane = side * (depth - 1)

        def tile(t, moments):
            start = pl.multiple_of(span[0] + t * TILE, TILE)
            at = pl.ds(start, TILE)
            value = inv[plane, at, :]
            beyond = halo_r[side, at, :]
            if side is far_side:
                beyond = beyond * shadow[at, :]
            image = jnp.where(value > 0.0, w0[plane, at, :] - beyond, 0.0)
            w0[plane, at, :] = image
            return apply_once(plane, start, image, value, moments)

        return lax.fori_loop(0, span[1] // TILE, tile, moments)

    passing = digit == near_size - 1
    @pl.when(is_odd)
    def _():
        for which in range(1, len(rounds)):
            hear(which)

    @pl.when(jnp.logical_and(is_even, is_first))
    def _():
        far_pieces(kept, len(spans))

    @pl.when(jnp.logical_not(is_first))
    def _():
        @pl.when(is_even)
        def _():
            far_sent(0)
            pl.semaphore_signal(go, inc=1, device_id=(partner,), device_id_type=MESH)

        @pl.when(is_odd)
        def _():
            pl.semaphore_wait(go, 1)

            @pl.when(jnp.logical_and(passing, chip >= near_size))
            def _():
                pl.semaphore_signal(
                    clear, inc=1, device_id=(me - 2 * near_size,), device_id_type=MESH
                )

            @pl.when(jnp.logical_and(passing, chip + near_size < count // 2))
            def _():
                pl.semaphore_wait(clear, 1)

            far_pieces(0, len(spans))

    near_arrival(0).wait_recv()
    moments = edge_one(near_side, (0, rows), moments)
    near_copy(1).start()
    for i, span in enumerate(spans):
        on(far_side, lambda: halo_arrival(0, far_side, span, far_recv.at[0, i]).wait_recv())
        moments = edge_one(far_side, span, moments)

        @pl.when(is_odd)
        def _():
            far_pieces(i, i + 1, 1)

    moment1, moment2 = moments

    def third(t, moment):
        start = pl.multiple_of(t * TILE, TILE)
        for plane in range(depth):
            image = local_part(u1, w0, w1, plane, start)
            moment = moment + fold(image * centre_of(u1, plane, start))
        return moment

    moment3 = lax.fori_loop(0, steps, third, none)

    def edge_two(side, span, moment, weight):
        plane = side * (depth - 1)

        def tile(t, moment):
            start = pl.multiple_of(span[0] + t * TILE, TILE)
            at = pl.ds(start, TILE)
            beyond = halo_u[side, at, :]
            image = jnp.where(inv[plane, at, :] > 0.0, w1[plane, at, :] - beyond, 0.0)
            w1[plane, at, :] = image
            return moment - weight * fold(beyond * centre_of(u1, plane, start))

        return lax.fori_loop(0, span[1] // TILE, tile, moment)

    def lanes(value):
        total = value[:, 0:128]
        for i in range(128, cols, 128):
            total = total + value[:, i:i + 128]
        return jnp.sum(total, axis=0, keepdims=True)

    for i, value in enumerate((moment0, moment1, moment2)):
        mine[0, i:i + 1, :] = lanes(value)
    mine[0, 3:8, :] = jnp.zeros((5, 128), jnp.float32)
    near_arrival(1).wait_recv()
    moment3 = edge_two(near_side, (0, rows), moment3, 1.0)

    def pair_copy():
        return pltpu.make_async_remote_copy(
            src_ref=mine.at[0], dst_ref=pair, send_sem=pair_send, recv_sem=pair_recv,
            device_id=(partner,), device_id_type=MESH,
        )

    def sum_copy(stage, j, core, shift=0):
        slot, other = peer(stage, j)
        return pltpu.make_async_remote_copy(
            src_ref=mine.at[stage],
            dst_ref=got.at[stage, slot],
            send_sem=sum_send.at[0 if stage == 0 or j == 0 else 2 if shift else 1],
            recv_sem=sum_recv.at[stage],
            device_id=(2 * (other - shift) + core,),
            device_id_type=MESH,
        )

    def sums(stage, copies, sender=0):
        several = got.at[stage, pl.ds(0, copies)]
        return pltpu.make_async_remote_copy(
            src_ref=several,
            dst_ref=several,
            send_sem=sum_send.at[sender],
            recv_sem=sum_recv.at[stage],
            device_id=(partner,),
            device_id_type=MESH,
        )

    def across():
        sum_copy(1, 0, 0).start()

        def to_all(shift):
            for j in range(1, far_size):
                for core in (1, 0):
                    sum_copy(1, j, core, shift).start()

        if relief:
            pl.when(is_relief)(lambda: to_all(relief))
            pl.when(jnp.logical_not(is_first))(lambda: to_all(0))
        else:
            to_all(0)

    def across_sent():
        sums(0, 1).wait_send()
        if far_size > 1:
            pl.when(jnp.logical_not(is_first) if relief else True)(
                lambda: sums(0, 2 * (far_size - 1), 1).wait_send()
            )
            if relief:
                pl.when(is_relief)(lambda: sums(0, 2 * (far_size - 1), 2).wait_send())

    def gathered(stage):
        total = got[stage, 0]
        for i in range(1, stages[stage][0]):
            total = total + got[stage, i]
        return total

    @pl.when(is_even)
    def _():
        pair_copy().wait_recv()
        mine[0] = mine[0] + pair[...]
        moment = moment3
        for i, span in enumerate(spans):
            on(far_side, lambda: halo_arrival(1, far_side, span, far_recv.at[1, i]).wait_recv())
            for place, after in ((is_first, 4), (jnp.logical_not(is_first), 3)):
                if i == max(len(spans) - after, 0):
                    @pl.when(place)
                    def _():
                        @pl.when(jnp.logical_or(jnp.logical_not(is_first), chip >= near_size))
                        def _():
                            pl.semaphore_wait(go, 1)

                        on(far_side, lambda: late_copy(0).start())

                        @pl.when(jnp.logical_and(is_first, has_far))
                        def _():
                            late_copy(1).start()

            moment = edge_two(far_side, span, moment, 2.0)

        mine[0, 3:4, :] = mine[0, 3:4, :] + lanes(moment)
        for j in range(near_size):
            sum_copy(0, j, 1).start()

        @pl.when(has_far)
        def _():
            pl.when(jnp.logical_not(is_first))(lambda: late_copy(1).start())
            late_copy(2).start()
            for i in range(3, len(lates)):
                late_copy(i - 3).wait_send()
                late_copy(i).start()

    @pl.when(is_odd)
    def _():
        mine[0, 3:4, :] = lanes(moment3)
        pair_copy().start()
        far_sent(1)

        @pl.when(jnp.logical_or(jnp.logical_not(is_first), chip + near_size < count // 2))
        def _():
            waiting = jnp.where(is_first, me - 1 + 2 * near_size, partner)
            pl.semaphore_signal(go, inc=1, device_id=(waiting,), device_id_type=MESH)

        sums(0, near_size).wait_recv()
        total = gathered(0)
        mine[1] = total
        across()
        got[1, peer(1, 0)[0]] = total

    near_copy(0).wait_send()
    near_copy(1).wait_send()
    far_ended(0)

    @pl.when(is_even)
    def _():
        pl.when(has_far)(lambda: bits_sent(2))
        pl.when(jnp.logical_not(has_far))(lambda: bits_sent(1))
        on(far_side, lambda: half_copy().wait_send())
        pl.when(is_first)(lambda: far_sent(0))
        sums(0, near_size).wait_send()
        sums(1, far_size).wait_recv()

    @pl.when(is_odd)
    def _():
        pl.when(has_far)(lambda: bits_sent(2))
        pl.when(jnp.logical_not(has_far))(lambda: bits_sent(1))
        far_sent(0)
        far_ended(1)
        pair_copy().wait_send()
        across_sent()
        if far_size > 1:
            sums(1, far_size - 1).wait_recv()

    everyone = gathered(1)
    s0, s1, s2, s3 = (everyone[i:i + 1] for i in range(4))

    def whole(value):
        return jnp.sum(value, axis=1, keepdims=True)

    rz_old = whole(s0)
    step_old = rz_old / whole(s1)
    rz_now = whole(s0 - 2.0 * step_old * s1 + step_old * step_old * s2)
    grown = 1.0 + rz_now / rz_old
    product = whole(grown * grown * s1 - 2.0 * step_old * grown * s2 + step_old * step_old * s3)
    step_size = rz_now / product
    lead = step_old + step_size * grown
    trail = step_size * step_old

    for plane in range(depth):
        def last(t, carry, plane=plane):
            at = pl.ds(pl.multiple_of(t * final, final), final)
            base = r0[plane, at, :]
            along = w0[plane, at, :]
            sol_ref[plane, at, :] = inv[plane, at, :] * (lead * base - trail * along)
            res_ref[plane, at, :] = base - lead * along + trail * w1[plane, at, :]
            return carry

        lax.fori_loop(0, rows // final, last, 0)

    @pl.when(jnp.logical_and(is_odd, has_far))
    def _():
        plane = depth - 1

        for i, span in enumerate(lates):
            halo_arrival(1, 1, span, far_recv.at[1, i]).wait_recv()

            def tile(t, carry, span=span):
                at = pl.ds(pl.multiple_of(span[0] + t * late_rows, late_rows), late_rows)
                beyond = jnp.where(inv[plane, at, :] > 0.0, halo_u[1, at, :], 0.0)
                res_ref[plane, at, :] = res_ref[plane, at, :] - trail * beyond
                return carry

            lax.fori_loop(0, span[1] // late_rows, tile, 0)

    @pl.when(jnp.logical_and(is_even, has_far))
    def _():
        for i in range(len(lates) - 3, len(lates)):
            late_copy(i).wait_send()


def store(sol_ref, res_ref, sol_out, res_out, sem):
    copies = []
    for which, (source, target) in enumerate(((sol_ref, sol_out), (res_ref, res_out))):
        for plane in range(sol_ref.shape[0]):
            copies.append(
                pltpu.make_async_copy(source.at[plane], target.at[plane], sem.at[which])
            )
    for copy in copies:
        copy.start()
    for which, (source, target) in enumerate(((sol_ref, sol_out), (res_ref, res_out))):
        pltpu.make_async_copy(source, target, sem.at[which]).wait()


def groups(chips):
    near = math.gcd(chips, 4)
    return (near, 1), (chips // near, near)


def body(count, right_side, cell_flags):
    depth, rows, cols = right_side.shape
    assert count % 2 == 0 and depth > 1
    stages = groups(count // 2)
    widest = max(stages[0][0], stages[1][0], 2 * (stages[1][0] - 1))
    chunk = math.gcd(rows, CHUNK)
    assert rows % 512 == 0
    pieces = max(6, len(LATE)) - 1
    f32 = jnp.float32
    field = pltpu.VMEM((depth, rows, cols), f32)
    padded = pltpu.VMEM((depth, rows + 2 * PAD, cols), f32)
    dma = pltpu.SemaphoreType.DMA
    grant = VMEM_BYTES - 8 * right_side.size - 2**19
    fields = pl.pallas_call(
        functools.partial(kernel, count, chunk, stages),
        out_shape=(field, field),
        in_specs=[pl.BlockSpec(memory_space=pltpu.HBM)] * 2,
        out_specs=(pl.BlockSpec(memory_space=pltpu.VMEM),) * 2,
        scratch_shapes=[
            field,
            pltpu.VMEM((depth, rows, cols), jnp.int32),
            field, field,
            pltpu.VMEM((rows, cols), f32),
            padded, padded, field, field,
            pltpu.VMEM((2, rows, cols), f32),
            pltpu.VMEM((2, rows, cols), f32),
            pltpu.VMEM((depth + 4, rows // 32, cols), jnp.int32),
            pltpu.VMEM((2, rows // 64, cols), jnp.int32),
            pltpu.VMEM((depth, rows // 32, cols), jnp.int32),
            pltpu.VMEM((depth + 1, 3, rows // 32, cols), jnp.int32),
            pltpu.VMEM((8, 128), f32),
            pltpu.VMEM((2, 8, 128), f32),
            pltpu.VMEM((2, widest, 8, 128), f32),
            dma((2, depth)),
            pltpu.SemaphoreType.REGULAR,
            pltpu.SemaphoreType.REGULAR,
            pltpu.SemaphoreType.REGULAR((max((stages[1][0] - 1).bit_length(), 1),)),
            dma((2,)), dma((3,)),
            dma((1 + len(LATE),)), dma((2, pieces)), dma((2,)), dma((2,)),
            dma, dma,
            dma((3,)), dma((2,)),
        ],
        compiler_params=pltpu.CompilerParams(
            collective_id=0, has_side_effects=True, vmem_limit_bytes=grant
        ),
    )(right_side, cell_flags)
    result = jax.ShapeDtypeStruct((depth, rows, cols), f32)
    return pl.pallas_call(
        store,
        out_shape=(result, result),
        in_specs=[pl.BlockSpec(memory_space=pltpu.VMEM)] * 2,
        out_specs=(pl.BlockSpec(memory_space=pltpu.HBM),) * 2,
        scratch_shapes=[dma((2,))],
        compiler_params=pltpu.CompilerParams(vmem_limit_bytes=2**19),
    )(*fields)


def solution(mesh):
    placed = (P("gz", None, None), P("gz", None, None))
    return jax.shard_map(
        functools.partial(body, mesh.shape["gz"]),
        mesh=mesh,
        in_specs=placed,
        out_specs=placed,
        check_vma=False,
    )
```
